512 devices in a mesh: gx: 32 (over y, x), gy: 16 (over z, core).
Axes of the slice: x: 4, y: 8, z: 8, core: 2. Of those that a mesh axis runs over, the one named last changes fastest.
Arguments:
- terminal: float32 [512, 8192], P('gx', 'gy'), may hold values from -15 to 15
- initial_density: float32 [512, 8192], P('gx', 'gy'), may hold values from 0.1 to 1
- density_guess: float32 [2, 512, 8192], P(None, 'gx', 'gy'), may hold values from 0.1 to 1
- diagonal: float32 [512, 8192], P('gx', 'gy'), may hold values from 0.1 to 2
Outputs:
- value_field: float32 [512, 8192], P('gx', 'gy')
- density_field: float32 [512, 8192], P('gx', 'gy')
The draws below stay inside these ranges and needn't reach their ends.
All inputs are finite; a program needn't handle non-finite values.
Results may differ from the reference program's by a relative error of at most 0.00011.
Values sent between devices are 32-bit elements; how exact they have to be, the bound alone decides.
No kernel may reach another device: no remote copies, remote signals or barrier semaphores. Data moves between devices by JAX's collectives and lax.ppermute only.
A program may use at most 64 MiB of HBM per device.

```python
import math
import jax
import jax.numpy as jnp

LEVELS = 2
STEPS = 3
NX = 512
NY = 8192


def draw_terminal(key, part):
    rows = jnp.arange(NX, dtype=jnp.float32)[:, None]
    scale = jnp.exp(jnp.log(3.0) * rows / max(NX - 1, 1))
    noise = jnp.clip(jax.random.normal(key, (NX, NY), jnp.float32), -5.0, 5.0)
    return scale * noise


def block_levels(rng, dims, pieces, low, largest):
    def one(position, shards_of):
        heights = jax.random.uniform(jax.random.fold_in(jax.random.fold_in(rng, 6), position), (shards_of,), jnp.float32, low / len(pieces), largest / len(pieces))
        return jnp.repeat(jnp.exp(heights), dims[position] // shards_of).reshape((-1,) + (1,) * (len(dims) - position - 1))

    gain = one(*pieces[0])
    for cut in pieces[1:]:
        gain = gain * one(*cut)
    return gain


def setup_inputs(seed: int = 0) -> dict:
    splits = jax.random.split(jax.random.key(seed), 5)
    terminal = draw_terminal(jax.random.fold_in(splits[4], 71), 0)
    initial_density = jnp.clip(jnp.exp(math.log(1.0) - 2.3025851 * jax.random.uniform(splits[1], (NX, NY), jnp.float32) ** block_levels(splits[1], (NX, NY), ((0, 32), (1, 16)), -0.2, 0.2)), 0.1, 1.0)
    density_guess = jnp.clip(jnp.exp(math.log(1.0) - 2.3025851 * jax.random.uniform(splits[2], (LEVELS, NX, NY), jnp.float32) ** block_levels(splits[2], (LEVELS, NX, NY), ((1, 32), (2, 16)), -0.2, 0.2)), 0.1, 1.0)
    diagonal = jnp.clip(jnp.exp(math.log(2.0) - 2.9957323 * jax.random.uniform(splits[3], (NX, NY), jnp.float32) ** block_levels(splits[3], (NX, NY), ((0, 32), (1, 16)), -0.2, 0.2)), 0.1, 2.0)
    return {"terminal": terminal, "initial_density": initial_density, "density_guess": density_guess, "diagonal": diagonal}


inv_step = 0.5
coupling = 0.5


def apply_padded(padded, center, diagonal):
    beside = padded[2:, 1:-1] + padded[:-2, 1:-1] + padded[1:-1, 2:] + padded[1:-1, :-2]
    return (inv_step + diagonal) * center + (4.0 * center - beside)


def hamiltonian(padded):
    center = padded[1:-1, 1:-1]
    back_x = center - padded[:-2, 1:-1]
    ahead_x = padded[2:, 1:-1] - center
    back_y = center - padded[1:-1, :-2]
    ahead_y = padded[1:-1, 2:] - center
    return 0.5 * (jnp.maximum(back_x, 0.0) ** 2 + jnp.minimum(ahead_x, 0.0) ** 2
                  + jnp.maximum(back_y, 0.0) ** 2 + jnp.minimum(ahead_y, 0.0) ** 2)


def divergence(pad_m, pad_u):
    m_mid = pad_m[1:-1, 1:-1]
    u_mid = pad_u[1:-1, 1:-1]
    speed_ahead = -(pad_u[2:, 1:-1] - u_mid)
    speed_back = -(u_mid - pad_u[:-2, 1:-1])
    flux_ahead = jnp.maximum(speed_ahead, 0.0) * m_mid + jnp.minimum(speed_ahead, 0.0) * pad_m[2:, 1:-1]
    flux_back = jnp.maximum(speed_back, 0.0) * pad_m[:-2, 1:-1] + jnp.minimum(speed_back, 0.0) * m_mid
    total = flux_ahead - flux_back
    speed_ahead = -(pad_u[1:-1, 2:] - u_mid)
    speed_back = -(u_mid - pad_u[1:-1, :-2])
    flux_ahead = jnp.maximum(speed_ahead, 0.0) * m_mid + jnp.minimum(speed_ahead, 0.0) * pad_m[1:-1, 2:]
    flux_back = jnp.maximum(speed_back, 0.0) * pad_m[1:-1, :-2] + jnp.minimum(speed_back, 0.0) * m_mid
    return total + flux_ahead - flux_back


def solve(rhs, diagonal):
    answer = jnp.zeros_like(rhs)
    resid = rhs
    direction = rhs
    norm_now = jnp.sum(resid * resid)
    for step in range(STEPS):
        image = apply_padded(jnp.pad(direction, 1), direction, diagonal)
        alpha = norm_now / jnp.sum(direction * image)
        answer = answer + alpha * direction
        resid = resid - alpha * image
        norm_next = jnp.sum(resid * resid)
        direction = resid + (norm_next / norm_now) * direction
        norm_now = norm_next
    return answer


def reference(terminal, initial_density, density_guess, diagonal):
    levels = [None] * LEVELS
    later = terminal
    for level in reversed(range(LEVELS)):
        rhs = inv_step * later - hamiltonian(jnp.pad(later, 1)) + coupling * density_guess[level]
        later = solve(rhs, diagonal)
        levels[level] = later
    density = initial_density
    for level in range(LEVELS):
        rhs = inv_step * density - divergence(jnp.pad(density, 1), jnp.pad(levels[level], 1))
        density = solve(rhs, diagonal)
    return levels[0], density
```

```python
import functools

import jax
import jax.numpy as jnp
from jax import lax
from jax.experimental import pallas as pl
from jax.experimental.pallas import tpu as pltpu
from jax.sharding import Mesh
from jax.sharding import PartitionSpec as P

GX = ("gx_0", "gx_1")
GY = ("gy_0", "gy_1")
FIRST = ("gx_1", "gy_1")
SECOND = ("gx_0", "gy_0")

inv_step = 0.5
coupling = 0.5

LOW = 0.6
HIGH = 10.5
S1 = 2.0
S2 = 6.0
S3 = 4.0
PAIRS = ((0, 0), (0, 1), (0, 2), (1, 1), (1, 2), (2, 2), (2, 3))
MIXED = ((0, 0), (1, 1), (2, 2), (0, 1), (0, 2), (1, 2))

HALF = 64
EDGE = 128


def before(v, dim):
    return pltpu.roll(v, 1, dim)


def after(v, dim):
    return pltpu.roll(v, v.shape[dim] - 1, dim)


def inside(rows, wide, first_row, own, grid):
    nx, ny, local_x, local_y = grid
    row = lax.broadcasted_iota(jnp.int32, (rows, wide), 0) + (lax.axis_index(GX) * local_x + first_row)
    lane = lax.broadcasted_iota(jnp.int32, (rows, wide), 1)
    column = jnp.where(lane < own + HALF, lane, lane - wide) + lax.axis_index(GY) * local_y
    return (row >= 0) & (row < nx) & (column >= 0) & (column < ny)


def shifted(v, center, shift, keep):
    beside = (before(v, 0) + after(v, 0)) + (before(v, 1) + after(v, 1))
    return jnp.where(keep, (center - shift) * v - beside, 0.0)


def basis(v0, center, keep):
    v1 = shifted(v0, center, S1, keep)
    v2 = shifted(v1, center, S2, keep)
    return [v0, v1, v2, shifted(v2, center, S3, keep)]


def hamiltonian(u):
    ahead_x = after(u, 0) - u
    back_x = u - before(u, 0)
    ahead_y = after(u, 1) - u
    back_y = u - before(u, 1)
    return 0.5 * (
        jnp.maximum(back_x, 0.0) ** 2
        + jnp.minimum(ahead_x, 0.0) ** 2
        + jnp.maximum(back_y, 0.0) ** 2
        + jnp.minimum(ahead_y, 0.0) ** 2
    )


def drift(u):
    speed_x = u - after(u, 0)
    speed_y = u - after(u, 1)
    return (
        jnp.maximum(speed_x, 0.0),
        jnp.minimum(speed_x, 0.0),
        jnp.maximum(speed_y, 0.0),
        jnp.minimum(speed_y, 0.0),
    )


def density_rhs(m, speeds, keep):
    out_x, in_x, out_y, in_y = speeds
    flux_x = out_x * m + in_x * after(m, 0)
    flux_y = out_y * m + in_y * after(m, 1)
    div = (flux_x - before(flux_x, 0)) + (flux_y - before(flux_y, 1))
    return jnp.where(keep, inv_step * m - div, 0.0)


def dot(a, b):
    return jnp.sum(jnp.sum(a * b, axis=0, keepdims=True), axis=1, keepdims=True)


def row_of(values):
    lane = lax.broadcasted_iota(jnp.int32, (1, 128), 1)
    row = jnp.zeros((1, 128), jnp.float32)
    for place, value in values:
        row = jnp.where(lane == place, value, row)
    return row


def entry(row, place):
    lane = lax.broadcasted_iota(jnp.int32, row.shape, 1)
    return jnp.sum(jnp.where(lane == place, row, 0.0), axis=1, keepdims=True)


def form(matrix, vector):
    total = None
    for i, a in enumerate(vector):
        for j, b in enumerate(vector[: i + 1]):
            term = a * b * matrix[j][i]
            term = term if i == j else 2.0 * term
            total = term if total is None else total + term
    return total


def alpha_of(squared, energy):
    return jnp.clip(squared / jnp.maximum(energy, 1e-36), 0.999 / HIGH, 1.001 / LOW)


def beta_of(new, old):
    return jnp.clip(new / jnp.maximum(old, 1e-36), 0.0, 1.001 * HIGH / LOW)


def coefficients(products):
    g = dict(zip(PAIRS, products))
    gram = [[g[0, 0], g[0, 1], g[0, 2]], [None, g[1, 1], g[1, 2]], [None, None, g[2, 2]]]
    energy = [
        [g[0, 1] + S1 * g[0, 0], g[1, 1] + S1 * g[0, 1], g[1, 2] + S1 * g[0, 2]],
        [None, g[1, 2] + S2 * g[1, 1], g[2, 2] + S2 * g[1, 2]],
        [None, None, g[2, 3] + S3 * g[2, 2]],
    ]
    norm0 = g[0, 0]
    alpha0 = alpha_of(norm0, energy[0][0])
    resid1 = (1.0 - alpha0 * S1, -alpha0)
    norm1 = jnp.maximum(form(gram, resid1), 0.0)
    beta0 = beta_of(norm1, norm0)
    direct1 = (resid1[0] + beta0, resid1[1])
    alpha1 = alpha_of(norm1, form(energy, direct1))
    resid2 = (
        resid1[0] - alpha1 * (S1 * direct1[0]),
        resid1[1] - alpha1 * (direct1[0] + S2 * direct1[1]),
        -alpha1 * direct1[1],
    )
    norm2 = jnp.maximum(form(gram, resid2), 0.0)
    beta1 = beta_of(norm2, norm1)
    direct2 = (resid2[0] + beta1 * direct1[0], resid2[1] + beta1 * direct1[1], resid2[2])
    alpha2 = alpha_of(norm2, form(energy, direct2))
    return (
        alpha0 + alpha1 * direct1[0] + alpha2 * direct2[0],
        alpha1 * direct1[1] + alpha2 * direct2[1],
        alpha2 * direct2[2],
    )


def combined(coefs, vectors):
    total = coefs[0] * vectors[0]
    for c, v in zip(coefs[1:], vectors[1:]):
        total = total + c * v
    return total


def middle(v, x, own):
    return v[(v.shape[0] - x) // 2 : (v.shape[0] + x) // 2, :own]


def gathered_products(parts_ref):
    parts = parts_ref[...]
    return jnp.sum(parts.reshape(parts.shape[0], 128), axis=0, keepdims=True)


def first_kernel(grid, own_ref, above_ref, below_ref, left_ref, right_ref, basis_ref, fields_ref, sums_ref):
    x, own = own_ref.shape[1:]
    wide = own + EDGE
    keep = inside(3 * x, wide, -x, own, grid)
    half = lax.broadcasted_iota(jnp.int32, (3 * x, EDGE), 1) < HALF

    def extended(k):
        middle_part = jnp.concatenate([above_ref[k], own_ref[k], below_ref[k]], axis=0)
        edge = jnp.where(half, right_ref[k], left_ref[k])
        return jnp.concatenate([middle_part, edge], axis=1)

    later = extended(0)
    center = extended(1) + (inv_step + 4.0)
    rhs = inv_step * later - hamiltonian(later) + coupling * extended(2)
    vs = basis(jnp.where(keep, rhs, 0.0), center, keep)
    for k in range(3):
        basis_ref[k] = vs[k]
    fields_ref[0] = center
    fields_ref[1] = extended(3)
    fields_ref[2] = extended(4)
    mine = [middle(v, x, own) for v in vs]
    sums_ref[...] = row_of([(k, dot(mine[i], mine[j])) for k, (i, j) in enumerate(PAIRS)])


def second_kernel(grid, parts_ref, last_ref, fields_ref, later_ref, basis_ref, sums_ref):
    _, _, x, own = grid
    rows, wide = last_ref.shape[1:]
    keep = inside(rows, wide, -x, own, grid)
    row = gathered_products(parts_ref)
    coefs = coefficients([entry(row, k) for k in range(len(PAIRS))])
    later = combined(coefs, [last_ref[k] for k in range(3)])
    later_ref[...] = later
    rhs = inv_step * later - hamiltonian(later) + coupling * fields_ref[1]
    vs = basis(jnp.where(keep, rhs, 0.0), fields_ref[0], keep)
    for k in range(3):
        basis_ref[k] = vs[k]
    mine = [middle(v, x, own) for v in vs]
    sums_ref[...] = row_of([(k, dot(mine[i], mine[j])) for k, (i, j) in enumerate(PAIRS)])


def third_kernel(grid, parts_ref, last_ref, fields_ref, later_ref, value_ref, images_ref, sums_ref):
    _, _, x, own = grid
    rows, wide = last_ref.shape[1:]
    cut = x // 2
    some = pl.ds(cut, rows - 2 * cut)
    keep = inside(rows - 2 * cut, wide, cut - x, own, grid)
    row = gathered_products(parts_ref)
    coefs = coefficients([entry(row, k) for k in range(len(PAIRS))])
    value = combined(coefs, [last_ref[k, some, :] for k in range(3)])
    value_ref[...] = middle(value, x, own)
    center = fields_ref[0, some, :]
    firsts = basis(density_rhs(fields_ref[2, some, :], drift(value), keep), center, keep)
    mine = [middle(v, x, own) for v in firsts]
    values = [(6 * 8 + k, dot(mine[i], mine[j])) for k, (i, j) in enumerate(PAIRS)]
    speeds = drift(later_ref[some, :])
    images = []
    for v in firsts[:3]:
        chain = basis(density_rhs(v, speeds, keep), center, keep)
        images.append([middle(w, x, own) for w in chain])
    for i in range(3):
        for k in range(3):
            images_ref[3 * i + k] = images[i][k]
    for place, (a, b) in enumerate(MIXED):
        for k, (i, j) in enumerate(PAIRS):
            values.append((8 * place + k, dot(images[a][i], images[b][j])))
    sums_ref[...] = row_of(values)


def fourth_kernel(parts_ref, images_ref, density_ref):
    row = gathered_products(parts_ref)
    first = coefficients([entry(row, 6 * 8 + k) for k in range(len(PAIRS))])
    products = []
    for k in range(len(PAIRS)):
        total = None
        for place, (a, b) in enumerate(MIXED):
            term = first[a] * first[b] * entry(row, 8 * place + k)
            term = term if a == b else 2.0 * term
            total = term if total is None else total + term
        products.append(total)
    second = coefficients(products)
    total = None
    for i in range(3):
        for k in range(3):
            term = (first[i] * second[k]) * images_ref[3 * i + k]
            total = term if total is None else total + term
    density_ref[...] = total


def spread(row, axes):
    size = lax.axis_size(axes)
    copies = jnp.broadcast_to(row, (size, 1, 128))
    return lax.all_to_all(copies, axes, split_axis=0, concat_axis=0, tiled=True)


def everywhere(row):
    nearer = spread(row, FIRST).sum(axis=0)
    return spread(nearer, SECOND)


def neighbours(shard, axis):
    peers = lax.axis_size(axis)
    up = [(i, i + 1) for i in range(peers - 1)]
    return up, [(b, a) for a, b in up]


def call(kernel, out_shape, *args):
    vmem = pl.BlockSpec(memory_space=pltpu.VMEM)
    return pl.pallas_call(
        kernel,
        out_shape=[jax.ShapeDtypeStruct(s, jnp.float32) for s in out_shape],
        in_specs=[vmem] * len(args),
        out_specs=[vmem] * len(out_shape),
    )(*args)


def shards(terminal, initial_density, density_guess, diagonal):
    x, own = terminal.shape
    grid = (x * lax.axis_size(GX), own * lax.axis_size(GY), x, own)
    fields = jnp.stack([terminal, diagonal, density_guess[1], density_guess[0], initial_density])
    up, down = neighbours(fields, GX)
    above = lax.ppermute(fields, GX, up)
    below = lax.ppermute(fields, GX, down)
    tall = [above, fields, below]
    up, down = neighbours(fields, GY)
    left = lax.ppermute(jnp.concatenate([f[:, :, own - EDGE :] for f in tall], axis=1), GY, up)
    right = lax.ppermute(jnp.concatenate([f[:, :, :EDGE] for f in tall], axis=1), GY, down)
    full = (3 * x, own + EDGE)
    basis1, kept, sums = call(
        functools.partial(first_kernel, grid),
        [(3, *full), (3, *full), (1, 128)],
        fields, above, below, left, right,
    )
    later, basis0, sums = call(
        functools.partial(second_kernel, grid),
        [full, (3, *full), (1, 128)],
        everywhere(sums), basis1, kept,
    )
    value, images, sums = call(
        functools.partial(third_kernel, grid),
        [(x, own), (9, x, own), (1, 128)],
        everywhere(sums), basis0, kept, later,
    )
    (density,) = call(fourth_kernel, [(x, own)], everywhere(sums), images)
    return value, density


def solution(mesh):
    torus = Mesh(mesh.devices.reshape(8, 4, 8, 2), ("gx_0", "gx_1", "gy_0", "gy_1"))
    in_specs = (P(GX, GY), P(GX, GY), P(None, GX, GY), P(GX, GY))
    out_specs = (P(GX, GY), P(GX, GY))
    return jax.shard_map(
        shards, mesh=torus, in_specs=in_specs, out_specs=out_specs, check_vma=False
    )
```

```python
import functools

import jax
import jax.numpy as jnp
from jax import lax
from jax.experimental import pallas as pl
from jax.experimental.pallas import tpu as pltpu
from jax.sharding import Mesh
from jax.sharding import PartitionSpec as P

GX = ("gx_0", "gx_1")
GY = ("gy_0", "gy_1")
FIRST = ("gx_0", "gy_1")
SECOND = ("gx_1", "gy_0")

inv_step = 0.5
coupling = 0.5

LOW = 0.6
HIGH = 10.5
S1 = 2.0
S2 = 6.0
S3 = 4.0
PAIRS = ((0, 0), (0, 1), (0, 2), (1, 1), (1, 2), (2, 2), (2, 3))
MIXED = ((0, 0), (1, 1), (2, 2), (0, 1), (0, 2), (1, 2))

HALF = 64
EDGE = 128
TERMINAL, DIAGONAL, GUESS, INITIAL = 0, 1, 2, 4


def before(v, dim):
    return pltpu.roll(v, 1, dim)


def after(v, dim):
    return pltpu.roll(v, v.shape[dim] - 1, dim)


def inside(rows, wide, first_row, own, grid):
    nx, ny, local_x, local_y = grid
    row = lax.broadcasted_iota(jnp.int32, (rows, wide), 0) + (lax.axis_index(GX) * local_x + first_row)
    lane = lax.broadcasted_iota(jnp.int32, (rows, wide), 1)
    column = jnp.where(lane < own + HALF, lane, lane - wide) + lax.axis_index(GY) * local_y
    return (row >= 0) & (row < nx) & (column >= 0) & (column < ny)


def shifted(v, center, shift, keep):
    beside = (before(v, 0) + after(v, 0)) + (before(v, 1) + after(v, 1))
    return jnp.where(keep, (center - shift) * v - beside, 0.0)


def basis(v0, center, keep):
    v1 = shifted(v0, center, S1, keep)
    v2 = shifted(v1, center, S2, keep)
    return [v0, v1, v2, shifted(v2, center, S3, keep)]


def hamiltonian(u):
    ahead_x = after(u, 0) - u
    back_x = u - before(u, 0)
    ahead_y = after(u, 1) - u
    back_y = u - before(u, 1)
    return 0.5 * (
        jnp.maximum(back_x, 0.0) ** 2
        + jnp.minimum(ahead_x, 0.0) ** 2
        + jnp.maximum(back_y, 0.0) ** 2
        + jnp.minimum(ahead_y, 0.0) ** 2
    )


def drift(u):
    speed_x = u - after(u, 0)
    speed_y = u - after(u, 1)
    return (
        jnp.maximum(speed_x, 0.0),
        jnp.minimum(speed_x, 0.0),
        jnp.maximum(speed_y, 0.0),
        jnp.minimum(speed_y, 0.0),
    )


def density_rhs(m, speeds, keep):
    out_x, in_x, out_y, in_y = speeds
    flux_x = out_x * m + in_x * after(m, 0)
    flux_y = out_y * m + in_y * after(m, 1)
    div = (flux_x - before(flux_x, 0)) + (flux_y - before(flux_y, 1))
    return jnp.where(keep, inv_step * m - div, 0.0)


def dot(a, b):
    return jnp.sum(jnp.sum(a * b, axis=0, keepdims=True), axis=1, keepdims=True)


def row_of(values):
    lane = lax.broadcasted_iota(jnp.int32, (1, 128), 1)
    row = jnp.zeros((1, 128), jnp.float32)
    for place, value in values:
        row = jnp.where(lane == place, value, row)
    return row


def entry(row, place):
    lane = lax.broadcasted_iota(jnp.int32, row.shape, 1)
    return jnp.sum(jnp.where(lane == place, row, 0.0), axis=1, keepdims=True)


def form(matrix, vector):
    total = None
    for i, a in enumerate(vector):
        for j, b in enumerate(vector[: i + 1]):
            term = a * b * matrix[j][i]
            term = term if i == j else 2.0 * term
            total = term if total is None else total + term
    return total


def alpha_of(squared, energy):
    return jnp.clip(squared / jnp.maximum(energy, 1e-36), 0.999 / HIGH, 1.001 / LOW)


def beta_of(new, old):
    return jnp.clip(new / jnp.maximum(old, 1e-36), 0.0, 1.001 * HIGH / LOW)


def coefficients(products):
    g = dict(zip(PAIRS, products))
    gram = [[g[0, 0], g[0, 1], g[0, 2]], [None, g[1, 1], g[1, 2]], [None, None, g[2, 2]]]
    energy = [
        [g[0, 1] + S1 * g[0, 0], g[1, 1] + S1 * g[0, 1], g[1, 2] + S1 * g[0, 2]],
        [None, g[1, 2] + S2 * g[1, 1], g[2, 2] + S2 * g[1, 2]],
        [None, None, g[2, 3] + S3 * g[2, 2]],
    ]
    norm0 = g[0, 0]
    alpha0 = alpha_of(norm0, energy[0][0])
    resid1 = (1.0 - alpha0 * S1, -alpha0)
    norm1 = jnp.maximum(form(gram, resid1), 0.0)
    beta0 = beta_of(norm1, norm0)
    direct1 = (resid1[0] + beta0, resid1[1])
    alpha1 = alpha_of(norm1, form(energy, direct1))
    resid2 = (
        resid1[0] - alpha1 * (S1 * direct1[0]),
        resid1[1] - alpha1 * (direct1[0] + S2 * direct1[1]),
        -alpha1 * direct1[1],
    )
    norm2 = jnp.maximum(form(gram, resid2), 0.0)
    beta1 = beta_of(norm2, norm1)
    direct2 = (resid2[0] + beta1 * direct1[0], resid2[1] + beta1 * direct1[1], resid2[2])
    alpha2 = alpha_of(norm2, form(energy, direct2))
    return (
        alpha0 + alpha1 * direct1[0] + alpha2 * direct2[0],
        alpha1 * direct1[1] + alpha2 * direct2[1],
        alpha2 * direct2[2],
    )


def combined(coefs, vectors):
    total = coefs[0] * vectors[0]
    for c, v in zip(coefs[1:], vectors[1:]):
        total = total + c * v
    return total


def middle(v, x, own):
    return v[(v.shape[0] - x) // 2 : (v.shape[0] + x) // 2, :own]


def gathered_products(parts_ref):
    parts = parts_ref[...]
    return jnp.sum(parts.reshape(parts.shape[0], 128), axis=0, keepdims=True)


def stack_kernel(terminal, diagonal, guess, initial, fields_ref, sems):
    copies = [
        pltpu.make_async_copy(terminal, fields_ref.at[TERMINAL], sems.at[0]),
        pltpu.make_async_copy(diagonal, fields_ref.at[DIAGONAL], sems.at[1]),
        pltpu.make_async_copy(guess, fields_ref.at[pl.ds(GUESS, 2)], sems.at[2]),
        pltpu.make_async_copy(initial, fields_ref.at[INITIAL], sems.at[3]),
    ]
    for copy in copies:
        copy.start()
    for copy in copies:
        copy.wait()


def first_kernel(grid, own_ref, above_ref, below_ref, own_edge, above_edge, below_edge, basis_ref, fields_ref, sums_ref):
    x, own = own_ref.shape[1:]
    wide = own + EDGE
    keep = inside(3 * x, wide, -x, own, grid)

    def extended(k):
        rows = [(above_ref, above_edge), (own_ref, own_edge), (below_ref, below_edge)]
        return jnp.concatenate([jnp.concatenate([r[k], e[k]], axis=1) for r, e in rows], axis=0)

    later = extended(TERMINAL)
    center = extended(DIAGONAL) + (inv_step + 4.0)
    rhs = inv_step * later - hamiltonian(later) + coupling * extended(GUESS + 1)
    vs = basis(jnp.where(keep, rhs, 0.0), center, keep)
    for k in range(3):
        basis_ref[k] = vs[k]
    fields_ref[0] = center
    fields_ref[1] = extended(GUESS)
    fields_ref[2] = extended(INITIAL)
    mine = [middle(v, x, own) for v in vs]
    sums_ref[...] = row_of([(k, dot(mine[i], mine[j])) for k, (i, j) in enumerate(PAIRS)])


def second_kernel(grid, parts_ref, last_ref, fields_ref, later_ref, basis_ref, sums_ref):
    _, _, x, own = grid
    rows, wide = last_ref.shape[1:]
    keep = inside(rows, wide, -x, own, grid)
    row = gathered_products(parts_ref)
    coefs = coefficients([entry(row, k) for k in range(len(PAIRS))])
    later = combined(coefs, [last_ref[k] for k in range(3)])
    later_ref[...] = later
    rhs = inv_step * later - hamiltonian(later) + coupling * fields_ref[1]
    vs = basis(jnp.where(keep, rhs, 0.0), fields_ref[0], keep)
    for k in range(3):
        basis_ref[k] = vs[k]
    mine = [middle(v, x, own) for v in vs]
    sums_ref[...] = row_of([(k, dot(mine[i], mine[j])) for k, (i, j) in enumerate(PAIRS)])


def third_kernel(grid, parts_ref, last_ref, fields_ref, later_ref, value_ref, images_ref, sums_ref):
    _, _, x, own = grid
    rows, wide = last_ref.shape[1:]
    cut = x // 2
    some = pl.ds(cut, rows - 2 * cut)
    keep = inside(rows - 2 * cut, wide, cut - x, own, grid)
    row = gathered_products(parts_ref)
    coefs = coefficients([entry(row, k) for k in range(len(PAIRS))])
    value = combined(coefs, [last_ref[k, some, :] for k in range(3)])
    value_ref[...] = middle(value, x, own)
    center = fields_ref[0, some, :]
    firsts = basis(density_rhs(fields_ref[2, some, :], drift(value), keep), center, keep)
    mine = [middle(v, x, own) for v in firsts]
    values = [(6 * 8 + k, dot(mine[i], mine[j])) for k, (i, j) in enumerate(PAIRS)]
    speeds = drift(later_ref[some, :])
    images = []
    for v in firsts[:3]:
        chain = basis(density_rhs(v, speeds, keep), center, keep)
        images.append([middle(w, x, own) for w in chain])
    for i in range(3):
        for k in range(3):
            images_ref[3 * i + k] = images[i][k]
    for place, (a, b) in enumerate(MIXED):
        for k, (i, j) in enumerate(PAIRS):
            values.append((8 * place + k, dot(images[a][i], images[b][j])))
    sums_ref[...] = row_of(values)


def fourth_kernel(parts_ref, images_ref, density_ref):
    row = gathered_products(parts_ref)
    first = coefficients([entry(row, 6 * 8 + k) for k in range(len(PAIRS))])
    products = []
    for k in range(len(PAIRS)):
        total = None
        for place, (a, b) in enumerate(MIXED):
            term = first[a] * first[b] * entry(row, 8 * place + k)
            term = term if a == b else 2.0 * term
            total = term if total is None else total + term
        products.append(total)
    second = coefficients(products)
    total = None
    for i in range(3):
        for k in range(3):
            term = (first[i] * second[k]) * images_ref[3 * i + k]
            total = term if total is None else total + term
    density_ref[...] = total


def spread(row, axes):
    size = lax.axis_size(axes)
    copies = jnp.broadcast_to(row, (size, 1, 128))
    return lax.all_to_all(copies, axes, split_axis=0, concat_axis=0, tiled=True)


def everywhere(row):
    nearer = spread(row, FIRST).sum(axis=0)
    return spread(nearer, SECOND)


def neighbours(shard, axis):
    peers = lax.axis_size(axis)
    up = [(i, i + 1) for i in range(peers - 1)]
    return up, [(b, a) for a, b in up]


def call(kernel, out_shape, *args):
    vmem = pl.BlockSpec(memory_space=pltpu.VMEM)
    return pl.pallas_call(
        kernel,
        out_shape=[pltpu.VMEM(s, jnp.float32) for s in out_shape],
        in_specs=[vmem] * len(args),
        out_specs=[vmem] * len(out_shape),
    )(*[pltpu.with_memory_space_constraint(a, pltpu.VMEM) for a in args])


def shards(terminal, initial_density, density_guess, diagonal):
    x, own = terminal.shape
    grid = (x * lax.axis_size(GX), own * lax.axis_size(GY), x, own)
    fields = pl.pallas_call(
        stack_kernel,
        out_shape=pltpu.VMEM((5, x, own), jnp.float32),
        in_specs=[pl.BlockSpec(memory_space=pltpu.HBM)] * 4,
        out_specs=pl.BlockSpec(memory_space=pltpu.VMEM),
        scratch_shapes=[pltpu.SemaphoreType.DMA((4,))],
    )(terminal, diagonal, density_guess, initial_density)
    down, up = neighbours(fields, GX)
    above = lax.ppermute(fields, GX, down)
    below = lax.ppermute(fields, GX, up)
    ahead, back = neighbours(fields, GY)
    left = lax.ppermute(fields[:, :, own - EDGE :], GY, ahead)
    right = lax.ppermute(fields[:, :, :EDGE], GY, back)
    lane = lax.broadcasted_iota(jnp.int32, left.shape, 2)
    edge = jnp.where(lane < HALF, right, left)
    above_edge = lax.ppermute(edge, GX, down)
    below_edge = lax.ppermute(edge, GX, up)
    full = (3 * x, own + EDGE)
    basis1, kept, sums = call(
        functools.partial(first_kernel, grid),
        [(3, *full), (3, *full), (1, 128)],
        fields, above, below, edge, above_edge, below_edge,
    )
    later, basis0, sums = call(
        functools.partial(second_kernel, grid),
        [full, (3, *full), (1, 128)],
        everywhere(sums), basis1, kept,
    )
    value, images, sums = call(
        functools.partial(third_kernel, grid),
        [(x, own), (9, x, own), (1, 128)],
        everywhere(sums), basis0, kept, later,
    )
    (density,) = call(fourth_kernel, [(x, own)], everywhere(sums), images)
    return value, density


def solution(mesh):
    torus = Mesh(mesh.devices.reshape(8, 4, 8, 2), ("gx_0", "gx_1", "gy_0", "gy_1"))
    in_specs = (P(GX, GY), P(GX, GY), P(None, GX, GY), P(GX, GY))
    out_specs = (P(GX, GY), P(GX, GY))
    return jax.shard_map(
        shards, mesh=torus, in_specs=in_specs, out_specs=out_specs, check_vma=False
    )
```

```python
import functools

import jax
import jax.numpy as jnp
from jax import lax
from jax.experimental import pallas as pl
from jax.experimental.pallas import tpu as pltpu
from jax.sharding import Mesh
from jax.sharding import PartitionSpec as P

GX = ("gx_0", "gx_1")
GY = ("gy_0", "gy_1")
FIRST = ("gx_0", "gy_1")
SECOND = ("gx_1", "gy_0")

inv_step = 0.5
coupling = 0.5

LOW = 0.6
HIGH = 10.5
S1 = 2.0
S2 = 6.0
S3 = 4.0
PAIRS = ((0, 0), (0, 1), (0, 2), (1, 1), (1, 2), (2, 2), (2, 3))
MIXED = ((0, 0), (1, 1), (2, 2), (0, 1), (0, 2), (1, 2))

HALF = 64
EDGE = 128
TERMINAL, DIAGONAL, GUESS, INITIAL = 0, 1, 2, 4
FIELDS = 5
STRIP = 16


def before(v, dim):
    return pltpu.roll(v, 1, dim)


def after(v, dim):
    return pltpu.roll(v, v.shape[dim] - 1, dim)


def inside(rows, wide, first_row, own, grid):
    nx, ny, local_x, local_y = grid
    row = lax.broadcasted_iota(jnp.int32, (rows, wide), 0) + (lax.axis_index(GX) * local_x + first_row)
    lane = lax.broadcasted_iota(jnp.int32, (rows, wide), 1)
    column = jnp.where(lane < own + HALF, lane, lane - wide) + lax.axis_index(GY) * local_y
    return (row >= 0) & (row < nx) & (column >= 0) & (column < ny)


def shifted(v, center, shift, keep):
    beside = (before(v, 0) + after(v, 0)) + (before(v, 1) + after(v, 1))
    return jnp.where(keep, (center - shift) * v - beside, 0.0)


def basis(v0, center, keep):
    v1 = shifted(v0, center, S1, keep)
    v2 = shifted(v1, center, S2, keep)
    return [v0, v1, v2, shifted(v2, center, S3, keep)]


def hamiltonian(u):
    ahead_x = after(u, 0) - u
    back_x = u - before(u, 0)
    ahead_y = after(u, 1) - u
    back_y = u - before(u, 1)
    return 0.5 * (
        jnp.maximum(back_x, 0.0) ** 2
        + jnp.minimum(ahead_x, 0.0) ** 2
        + jnp.maximum(back_y, 0.0) ** 2
        + jnp.minimum(ahead_y, 0.0) ** 2
    )


def drift(u):
    speed_x = u - after(u, 0)
    speed_y = u - after(u, 1)
    return (
        jnp.maximum(speed_x, 0.0),
        jnp.minimum(speed_x, 0.0),
        jnp.maximum(speed_y, 0.0),
        jnp.minimum(speed_y, 0.0),
    )


def density_rhs(m, speeds, keep):
    out_x, in_x, out_y, in_y = speeds
    flux_x = out_x * m + in_x * after(m, 0)
    flux_y = out_y * m + in_y * after(m, 1)
    div = (flux_x - before(flux_x, 0)) + (flux_y - before(flux_y, 1))
    return jnp.where(keep, inv_step * m - div, 0.0)


def dot(a, b):
    return jnp.sum(jnp.sum(a * b, axis=0, keepdims=True), axis=1, keepdims=True)


def row_of(values):
    lane = lax.broadcasted_iota(jnp.int32, (1, 128), 1)
    row = jnp.zeros((1, 128), jnp.float32)
    for place, value in values:
        row = jnp.where(lane == place, value, row)
    return row


def entry(row, place):
    lane = lax.broadcasted_iota(jnp.int32, row.shape, 1)
    return jnp.sum(jnp.where(lane == place, row, 0.0), axis=1, keepdims=True)


def form(matrix, vector):
    total = None
    for i, a in enumerate(vector):
        for j, b in enumerate(vector[: i + 1]):
            term = a * b * matrix[j][i]
            term = term if i == j else 2.0 * term
            total = term if total is None else total + term
    return total


def alpha_of(squared, energy):
    return jnp.clip(squared / jnp.maximum(energy, 1e-36), 0.999 / HIGH, 1.001 / LOW)


def beta_of(new, old):
    return jnp.clip(new / jnp.maximum(old, 1e-36), 0.0, 1.001 * HIGH / LOW)


def coefficients(products):
    g = dict(zip(PAIRS, products))
    gram = [[g[0, 0], g[0, 1], g[0, 2]], [None, g[1, 1], g[1, 2]], [None, None, g[2, 2]]]
    energy = [
        [g[0, 1] + S1 * g[0, 0], g[1, 1] + S1 * g[0, 1], g[1, 2] + S1 * g[0, 2]],
        [None, g[1, 2] + S2 * g[1, 1], g[2, 2] + S2 * g[1, 2]],
        [None, None, g[2, 3] + S3 * g[2, 2]],
    ]
    norm0 = g[0, 0]
    alpha0 = alpha_of(norm0, energy[0][0])
    resid1 = (1.0 - alpha0 * S1, -alpha0)
    norm1 = jnp.maximum(form(gram, resid1), 0.0)
    beta0 = beta_of(norm1, norm0)
    direct1 = (resid1[0] + beta0, resid1[1])
    alpha1 = alpha_of(norm1, form(energy, direct1))
    resid2 = (
        resid1[0] - alpha1 * (S1 * direct1[0]),
        resid1[1] - alpha1 * (direct1[0] + S2 * direct1[1]),
        -alpha1 * direct1[1],
    )
    norm2 = jnp.maximum(form(gram, resid2), 0.0)
    beta1 = beta_of(norm2, norm1)
    direct2 = (resid2[0] + beta1 * direct1[0], resid2[1] + beta1 * direct1[1], resid2[2])
    alpha2 = alpha_of(norm2, form(energy, direct2))
    return (
        alpha0 + alpha1 * direct1[0] + alpha2 * direct2[0],
        alpha1 * direct1[1] + alpha2 * direct2[1],
        alpha2 * direct2[2],
    )


def combined(coefs, vectors):
    total = coefs[0] * vectors[0]
    for c, v in zip(coefs[1:], vectors[1:]):
        total = total + c * v
    return total


def middle(v, x, own):
    return v[(v.shape[0] - x) // 2 : (v.shape[0] + x) // 2, :own]


def gathered_products(parts_ref):
    parts = parts_ref[...]
    return jnp.sum(parts.reshape(parts.shape[0], 128), axis=0, keepdims=True)


def odd_index(axis, shape):
    place = lax.rem(lax.axis_index(axis), 2)
    return (lax.broadcasted_iota(jnp.int32, shape, 0) * 0 + place) == 1


def stack_kernel(terminal, diagonal, guess, initial, fields_ref, far_ref, near_ref, sems):
    copies = [
        pltpu.make_async_copy(terminal, fields_ref.at[TERMINAL], sems.at[0]),
        pltpu.make_async_copy(diagonal, fields_ref.at[DIAGONAL], sems.at[1]),
        pltpu.make_async_copy(guess, fields_ref.at[pl.ds(GUESS, 2)], sems.at[2]),
        pltpu.make_async_copy(initial, fields_ref.at[INITIAL], sems.at[3]),
    ]
    for copy in copies:
        copy.start()
    for copy in copies:
        copy.wait()
    fields = fields_ref[...]
    shape = (8, fields.shape[2])
    row = lax.broadcasted_iota(jnp.int32, shape, 0)
    first, second = fields[:, :8], fields[:, 8:]
    top = [first[k] for k in range(FIELDS)] + [
        jnp.where(row < 5, second[TERMINAL], pltpu.roll(second[DIAGONAL], 5, 0)),
        jnp.where(row < 4, second[GUESS + 1], pltpu.roll(second[GUESS], 4, 0)),
    ]
    bottom = [second[k] for k in range(FIELDS)] + [
        jnp.where(row >= 3, first[TERMINAL], pltpu.roll(first[DIAGONAL], 3, 0)),
        jnp.where(row >= 4, first[GUESS + 1], pltpu.roll(first[GUESS], 4, 0)),
    ]
    odd = odd_index(GX, shape)
    for k, (t, b) in enumerate(zip(top, bottom)):
        far_ref[8 * k : 8 * k + 8, :] = jnp.where(odd, b, t)
        near_ref[8 * k : 8 * k + 8, :] = jnp.where(odd, t, b)


def column_kernel(own_ref, far_ref, near_ref, tall_ref, far_edge, near_edge):
    x, own = own_ref.shape[1:]
    odd = odd_index(GX, (8, own))

    def tile(k, odd_from, even_from):
        here = pl.ds(8 * k, 8)
        return jnp.where(odd, odd_from[here, :], even_from[here, :])

    above = [tile(k, near_ref, far_ref) for k in range(FIELDS + 2)]
    below = [tile(k, far_ref, near_ref) for k in range(FIELDS + 2)]
    rest_above = {
        TERMINAL: above[FIELDS],
        DIAGONAL: pltpu.roll(above[FIELDS], 5, 0),
        GUESS + 1: above[FIELDS + 1],
        GUESS: pltpu.roll(above[FIELDS + 1], 4, 0),
    }
    rest_below = {
        TERMINAL: below[FIELDS],
        DIAGONAL: pltpu.roll(below[FIELDS], 3, 0),
        GUESS + 1: below[FIELDS + 1],
        GUESS: pltpu.roll(below[FIELDS + 1], 4, 0),
    }
    nothing = jnp.zeros((8, own), jnp.float32)
    shape = (3 * x, 128)
    strip = lax.broadcasted_iota(jnp.int32, shape, 1) // STRIP
    firsts = lasts = jnp.zeros(shape, jnp.float32)
    for k in range(FIELDS):
        parts = [rest_above.get(k, nothing), above[k], own_ref[k], below[k], rest_below.get(k, nothing)]
        whole = jnp.concatenate(parts, axis=0)
        tall_ref[k] = whole
        first, last = whole[:, :128], whole[:, own - 128 :]
        firsts = jnp.where(strip == k, pltpu.roll(first, STRIP * k, 1) if k else first, firsts)
        lasts = jnp.where(strip == k, pltpu.roll(last, STRIP * (k + 1), 1), lasts)
    odd = odd_index(GY, shape)
    far_edge[...] = jnp.where(odd, lasts, firsts)
    near_edge[...] = jnp.where(odd, firsts, lasts)


def first_kernel(grid, tall_ref, far_edge, near_edge, basis_ref, fields_ref, sums_ref):
    _, _, x, own = grid
    wide = own + EDGE
    keep = inside(3 * x, wide, -x, own, grid)
    odd = odd_index(GY, (3 * x, EDGE))
    left = jnp.where(odd, near_edge[...], far_edge[...])
    right = jnp.where(odd, far_edge[...], near_edge[...])
    half = lax.broadcasted_iota(jnp.int32, (3 * x, EDGE), 1) < HALF

    def extended(k):
        from_right = pltpu.roll(right, 128 - STRIP * k, 1) if k else right
        from_left = pltpu.roll(left, 128 - STRIP * (k + 1), 1)
        return jnp.concatenate([tall_ref[k], jnp.where(half, from_right, from_left)], axis=1)

    later = extended(TERMINAL)
    center = extended(DIAGONAL) + (inv_step + 4.0)
    rhs = inv_step * later - hamiltonian(later) + coupling * extended(GUESS + 1)
    vs = basis(jnp.where(keep, rhs, 0.0), center, keep)
    for k in range(3):
        basis_ref[k] = vs[k]
    fields_ref[0] = center
    fields_ref[1] = extended(GUESS)
    fields_ref[2] = extended(INITIAL)
    mine = [middle(v, x, own) for v in vs]
    sums_ref[...] = row_of([(k, dot(mine[i], mine[j])) for k, (i, j) in enumerate(PAIRS)])


def second_kernel(grid, parts_ref, last_ref, fields_ref, later_ref, basis_ref, sums_ref):
    _, _, x, own = grid
    rows, wide = last_ref.shape[1:]
    keep = inside(rows, wide, -x, own, grid)
    row = gathered_products(parts_ref)
    coefs = coefficients([entry(row, k) for k in range(len(PAIRS))])
    later = combined(coefs, [last_ref[k] for k in range(3)])
    later_ref[...] = later
    rhs = inv_step * later - hamiltonian(later) + coupling * fields_ref[1]
    vs = basis(jnp.where(keep, rhs, 0.0), fields_ref[0], keep)
    for k in range(3):
        basis_ref[k] = vs[k]
    mine = [middle(v, x, own) for v in vs]
    sums_ref[...] = row_of([(k, dot(mine[i], mine[j])) for k, (i, j) in enumerate(PAIRS)])


def third_kernel(grid, parts_ref, last_ref, fields_ref, later_ref, value_ref, images_ref, sums_ref):
    _, _, x, own = grid
    rows, wide = last_ref.shape[1:]
    cut = x // 2
    some = pl.ds(cut, rows - 2 * cut)
    keep = inside(rows - 2 * cut, wide, cut - x, own, grid)
    row = gathered_products(parts_ref)
    coefs = coefficients([entry(row, k) for k in range(len(PAIRS))])
    value = combined(coefs, [last_ref[k, some, :] for k in range(3)])
    value_ref[...] = middle(value, x, own)
    center = fields_ref[0, some, :]
    firsts = basis(density_rhs(fields_ref[2, some, :], drift(value), keep), center, keep)
    mine = [middle(v, x, own) for v in firsts]
    values = [(6 * 8 + k, dot(mine[i], mine[j])) for k, (i, j) in enumerate(PAIRS)]
    speeds = drift(later_ref[some, :])
    images = []
    for v in firsts[:3]:
        chain = basis(density_rhs(v, speeds, keep), center, keep)
        images.append([middle(w, x, own) for w in chain])
    for i in range(3):
        for k in range(3):
            images_ref[3 * i + k] = images[i][k]
    for place, (a, b) in enumerate(MIXED):
        for k, (i, j) in enumerate(PAIRS):
            values.append((8 * place + k, dot(images[a][i], images[b][j])))
    sums_ref[...] = row_of(values)


def fourth_kernel(parts_ref, images_ref, value_ref, value_out, density_ref):
    value_out[...] = value_ref[...]
    row = gathered_products(parts_ref)
    first = coefficients([entry(row, 6 * 8 + k) for k in range(len(PAIRS))])
    products = []
    for k in range(len(PAIRS)):
        total = None
        for place, (a, b) in enumerate(MIXED):
            term = first[a] * first[b] * entry(row, 8 * place + k)
            term = term if a == b else 2.0 * term
            total = term if total is None else total + term
        products.append(total)
    second = coefficients(products)
    total = None
    for i in range(3):
        for k in range(3):
            term = (first[i] * second[k]) * images_ref[3 * i + k]
            total = term if total is None else total + term
    density_ref[...] = total


def spread(row, axes):
    size = lax.axis_size(axes)
    copies = jnp.broadcast_to(row, (size, 1, 128))
    return lax.all_to_all(copies, axes, split_axis=0, concat_axis=0, tiled=True)


def everywhere(row):
    nearer = spread(row, FIRST).sum(axis=0)
    return spread(nearer, SECOND)


def swapped(far, near, axis):
    peers = lax.axis_size(axis)

    def swap(array, start):
        pairs = [(i, i + 1) for i in range(start, peers - 1, 2)]
        return lax.ppermute(array, axis, pairs + [(b, a) for a, b in pairs])

    return swap(far, 1), swap(near, 0)


def call(kernel, out_shape, *args, results=pltpu.VMEM):
    vmem = pl.BlockSpec(memory_space=pltpu.VMEM)
    return pl.pallas_call(
        kernel,
        out_shape=[results(s, jnp.float32) for s in out_shape],
        in_specs=[vmem] * len(args),
        out_specs=[vmem] * len(out_shape),
    )(*[pltpu.with_memory_space_constraint(a, pltpu.VMEM) for a in args])


def shards(terminal, initial_density, density_guess, diagonal):
    x, own = terminal.shape
    grid = (x * lax.axis_size(GX), own * lax.axis_size(GY), x, own)
    packed = (8 * (FIELDS + 2), own)
    fields, far, near = pl.pallas_call(
        stack_kernel,
        out_shape=[pltpu.VMEM(s, jnp.float32) for s in [(FIELDS, x, own), packed, packed]],
        in_specs=[pl.BlockSpec(memory_space=pltpu.HBM)] * 4,
        out_specs=[pl.BlockSpec(memory_space=pltpu.VMEM)] * 3,
        scratch_shapes=[pltpu.SemaphoreType.DMA((4,))],
    )(terminal, diagonal, density_guess, initial_density)
    strips = (3 * x, 128)
    tall, far, near = call(
        column_kernel, [(FIELDS, 3 * x, own), strips, strips], fields, *swapped(far, near, GX)
    )
    full = (3 * x, own + EDGE)
    basis1, kept, sums = call(
        functools.partial(first_kernel, grid),
        [(3, *full), (3, *full), (1, 128)],
        tall, *swapped(far, near, GY),
    )
    later, basis0, sums = call(
        functools.partial(second_kernel, grid),
        [full, (3, *full), (1, 128)],
        everywhere(sums), basis1, kept,
    )
    value, images, sums = call(
        functools.partial(third_kernel, grid),
        [(x, own), (9, x, own), (1, 128)],
        everywhere(sums), basis0, kept, later,
    )
    return tuple(
        call(
            fourth_kernel, [(x, own)] * 2, everywhere(sums), images, value,
            results=jax.ShapeDtypeStruct,
        )
    )


def solution(mesh):
    torus = Mesh(mesh.devices.reshape(8, 4, 8, 2), ("gx_0", "gx_1", "gy_0", "gy_1"))
    in_specs = (P(GX, GY), P(GX, GY), P(None, GX, GY), P(GX, GY))
    out_specs = (P(GX, GY), P(GX, GY))
    return jax.shard_map(
        shards, mesh=torus, in_specs=in_specs, out_specs=out_specs, check_vma=False
    )
```

```python
import functools

import jax
import jax.numpy as jnp
from jax import lax
from jax.experimental import pallas as pl
from jax.experimental.pallas import tpu as pltpu
from jax.sharding import Mesh
from jax.sharding import PartitionSpec as P

GX = ("gx_0", "gx_1", "gx_2")
GY = ("gy_0", "gy_1")
FIRST = ("gx_0", "gy_1")
SECOND = ("gx_1", "gx_2", "gy_0")

inv_step = 0.5
coupling = 0.5

LOW = 0.6
HIGH = 10.5
S1 = 2.0
S2 = 6.0
S3 = 4.0
PAIRS = ((0, 0), (0, 1), (0, 2), (1, 1), (1, 2), (2, 2), (2, 3))
MIXED = ((0, 0), (1, 1), (2, 2), (0, 1), (0, 2), (1, 2))

HALF = 64
EDGE = 128
TERMINAL, DIAGONAL, GUESS, INITIAL = 0, 1, 2, 4
FIELDS = 5
STRIP = 16


def before(v, dim):
    return pltpu.roll(v, 1, dim)


def after(v, dim):
    return pltpu.roll(v, v.shape[dim] - 1, dim)


def inside(rows, wide, first_row, own, grid):
    nx, ny, local_x, local_y = grid
    row = lax.broadcasted_iota(jnp.int32, (rows, wide), 0) + (lax.axis_index(GX) * local_x + first_row)
    lane = lax.broadcasted_iota(jnp.int32, (rows, wide), 1)
    column = jnp.where(lane < own + HALF, lane, lane - wide) + lax.axis_index(GY) * local_y
    return (row >= 0) & (row < nx) & (column >= 0) & (column < ny)


def shifted(v, center, shift, keep):
    beside = (before(v, 0) + after(v, 0)) + (before(v, 1) + after(v, 1))
    return jnp.where(keep, (center - shift) * v - beside, 0.0)


def basis(v0, center, keep):
    v1 = shifted(v0, center, S1, keep)
    v2 = shifted(v1, center, S2, keep)
    return [v0, v1, v2, shifted(v2, center, S3, keep)]


def hamiltonian(u):
    ahead_x = after(u, 0) - u
    back_x = u - before(u, 0)
    ahead_y = after(u, 1) - u
    back_y = u - before(u, 1)
    return 0.5 * (
        jnp.maximum(back_x, 0.0) ** 2
        + jnp.minimum(ahead_x, 0.0) ** 2
        + jnp.maximum(back_y, 0.0) ** 2
        + jnp.minimum(ahead_y, 0.0) ** 2
    )


def drift(u):
    speed_x = u - after(u, 0)
    speed_y = u - after(u, 1)
    return (
        jnp.maximum(speed_x, 0.0),
        jnp.minimum(speed_x, 0.0),
        jnp.maximum(speed_y, 0.0),
        jnp.minimum(speed_y, 0.0),
    )


def density_rhs(m, speeds, keep):
    out_x, in_x, out_y, in_y = speeds
    flux_x = out_x * m + in_x * after(m, 0)
    flux_y = out_y * m + in_y * after(m, 1)
    div = (flux_x - before(flux_x, 0)) + (flux_y - before(flux_y, 1))
    return jnp.where(keep, inv_step * m - div, 0.0)


def dot(a, b):
    return jnp.sum(jnp.sum(a * b, axis=0, keepdims=True), axis=1, keepdims=True)


def row_of(values):
    lane = lax.broadcasted_iota(jnp.int32, (1, 128), 1)
    row = jnp.zeros((1, 128), jnp.float32)
    for place, value in values:
        row = jnp.where(lane == place, value, row)
    return row


def entry(row, place):
    lane = lax.broadcasted_iota(jnp.int32, row.shape, 1)
    return jnp.sum(jnp.where(lane == place, row, 0.0), axis=1, keepdims=True)


def form(matrix, vector):
    total = None
    for i, a in enumerate(vector):
        for j, b in enumerate(vector[: i + 1]):
            term = a * b * matrix[j][i]
            term = term if i == j else 2.0 * term
            total = term if total is None else total + term
    return total


def alpha_of(squared, energy):
    return jnp.clip(squared / jnp.maximum(energy, 1e-36), 0.999 / HIGH, 1.001 / LOW)


def beta_of(new, old):
    return jnp.clip(new / jnp.maximum(old, 1e-36), 0.0, 1.001 * HIGH / LOW)


def coefficients(products):
    g = dict(zip(PAIRS, products))
    gram = [[g[0, 0], g[0, 1], g[0, 2]], [None, g[1, 1], g[1, 2]], [None, None, g[2, 2]]]
    energy = [
        [g[0, 1] + S1 * g[0, 0], g[1, 1] + S1 * g[0, 1], g[1, 2] + S1 * g[0, 2]],
        [None, g[1, 2] + S2 * g[1, 1], g[2, 2] + S2 * g[1, 2]],
        [None, None, g[2, 3] + S3 * g[2, 2]],
    ]
    norm0 = g[0, 0]
    alpha0 = alpha_of(norm0, energy[0][0])
    resid1 = (1.0 - alpha0 * S1, -alpha0)
    norm1 = jnp.maximum(form(gram, resid1), 0.0)
    beta0 = beta_of(norm1, norm0)
    direct1 = (resid1[0] + beta0, resid1[1])
    alpha1 = alpha_of(norm1, form(energy, direct1))
    resid2 = (
        resid1[0] - alpha1 * (S1 * direct1[0]),
        resid1[1] - alpha1 * (direct1[0] + S2 * direct1[1]),
        -alpha1 * direct1[1],
    )
    norm2 = jnp.maximum(form(gram, resid2), 0.0)
    beta1 = beta_of(norm2, norm1)
    direct2 = (resid2[0] + beta1 * direct1[0], resid2[1] + beta1 * direct1[1], resid2[2])
    alpha2 = alpha_of(norm2, form(energy, direct2))
    return (
        alpha0 + alpha1 * direct1[0] + alpha2 * direct2[0],
        alpha1 * direct1[1] + alpha2 * direct2[1],
        alpha2 * direct2[2],
    )


def combined(coefs, vectors):
    total = coefs[0] * vectors[0]
    for c, v in zip(coefs[1:], vectors[1:]):
        total = total + c * v
    return total


def middle(v, x, own):
    return v[(v.shape[0] - x) // 2 : (v.shape[0] + x) // 2, :own]


def gathered_products(parts_ref):
    parts = parts_ref[...]
    return jnp.sum(parts.reshape(parts.shape[0], 128), axis=0, keepdims=True)


def odd_index(axis, shape):
    place = lax.rem(lax.axis_index(axis), 2)
    return (lax.broadcasted_iota(jnp.int32, shape, 0) * 0 + place) == 1


def stack_kernel(terminal, diagonal, guess, initial, fields_ref, far_ref, near_ref, sems):
    copies = [
        pltpu.make_async_copy(terminal, fields_ref.at[TERMINAL], sems.at[0]),
        pltpu.make_async_copy(diagonal, fields_ref.at[DIAGONAL], sems.at[1]),
        pltpu.make_async_copy(guess, fields_ref.at[pl.ds(GUESS, 2)], sems.at[2]),
        pltpu.make_async_copy(initial, fields_ref.at[INITIAL], sems.at[3]),
    ]
    for copy in copies:
        copy.start()
    for copy in copies:
        copy.wait()
    fields = fields_ref[...]
    shape = (8, fields.shape[2])
    row = lax.broadcasted_iota(jnp.int32, shape, 0)
    first, second = fields[:, :8], fields[:, 8:]
    top = [first[k] for k in range(FIELDS)] + [
        jnp.where(row < 5, second[TERMINAL], pltpu.roll(second[DIAGONAL], 5, 0)),
        jnp.where(row < 4, second[GUESS + 1], pltpu.roll(second[GUESS], 4, 0)),
    ]
    bottom = [second[k] for k in range(FIELDS)] + [
        jnp.where(row >= 3, first[TERMINAL], pltpu.roll(first[DIAGONAL], 3, 0)),
        jnp.where(row >= 4, first[GUESS + 1], pltpu.roll(first[GUESS], 4, 0)),
    ]
    odd = odd_index(GX, shape)
    for k, (t, b) in enumerate(zip(top, bottom)):
        far_ref[8 * k : 8 * k + 8, :] = jnp.where(odd, b, t)
        near_ref[8 * k : 8 * k + 8, :] = jnp.where(odd, t, b)


def column_kernel(own_ref, far_ref, near_ref, tall_ref, far_edge, near_edge):
    x, own = own_ref.shape[1:]
    odd = odd_index(GX, (8, own))

    sent = FIELDS + 2

    def tile(k, odd_from, odd_start, even_from, even_start):
        odd_tile = odd_from[8 * (odd_start + k) : 8 * (odd_start + k) + 8, :]
        return jnp.where(odd, odd_tile, even_from[8 * (even_start + k) : 8 * (even_start + k) + 8, :])

    above = [tile(k, near_ref, 0, far_ref, 0) for k in range(sent)]
    below = [tile(k, far_ref, 0, near_ref, sent) for k in range(sent)]
    rest_above = {
        TERMINAL: above[FIELDS],
        DIAGONAL: pltpu.roll(above[FIELDS], 5, 0),
        GUESS + 1: above[FIELDS + 1],
        GUESS: pltpu.roll(above[FIELDS + 1], 4, 0),
    }
    rest_below = {
        TERMINAL: below[FIELDS],
        DIAGONAL: pltpu.roll(below[FIELDS], 3, 0),
        GUESS + 1: below[FIELDS + 1],
        GUESS: pltpu.roll(below[FIELDS + 1], 4, 0),
    }
    nothing = jnp.zeros((8, own), jnp.float32)
    shape = (3 * x, 128)
    strip = lax.broadcasted_iota(jnp.int32, shape, 1) // STRIP
    firsts = lasts = jnp.zeros(shape, jnp.float32)
    for k in range(FIELDS):
        parts = [rest_above.get(k, nothing), above[k], own_ref[k], below[k], rest_below.get(k, nothing)]
        whole = jnp.concatenate(parts, axis=0)
        tall_ref[k] = whole
        first, last = whole[:, :128], whole[:, own - 128 :]
        firsts = jnp.where(strip == k, pltpu.roll(first, STRIP * k, 1) if k else first, firsts)
        lasts = jnp.where(strip == k, pltpu.roll(last, STRIP * (k + 1), 1), lasts)
    odd = odd_index(GY, shape)
    far_edge[...] = jnp.where(odd, lasts, firsts)
    near_edge[...] = jnp.where(odd, firsts, lasts)


def first_kernel(grid, tall_ref, far_edge, near_edge, basis_ref, fields_ref, sums_ref):
    _, _, x, own = grid
    wide = own + EDGE
    keep = inside(3 * x, wide, -x, own, grid)
    odd = odd_index(GY, (3 * x, EDGE))
    left = jnp.where(odd, near_edge[: 3 * x, :], far_edge[...])
    right = jnp.where(odd, far_edge[...], near_edge[3 * x :, :])
    half = lax.broadcasted_iota(jnp.int32, (3 * x, EDGE), 1) < HALF

    def extended(k):
        from_right = pltpu.roll(right, 128 - STRIP * k, 1) if k else right
        from_left = pltpu.roll(left, 128 - STRIP * (k + 1), 1)
        return jnp.concatenate([tall_ref[k], jnp.where(half, from_right, from_left)], axis=1)

    later = extended(TERMINAL)
    center = extended(DIAGONAL) + (inv_step + 4.0)
    rhs = inv_step * later - hamiltonian(later) + coupling * extended(GUESS + 1)
    vs = basis(jnp.where(keep, rhs, 0.0), center, keep)
    for k in range(3):
        basis_ref[k] = vs[k]
    fields_ref[0] = center
    fields_ref[1] = extended(GUESS)
    fields_ref[2] = extended(INITIAL)
    mine = [middle(v, x, own) for v in vs]
    sums_ref[...] = row_of([(k, dot(mine[i], mine[j])) for k, (i, j) in enumerate(PAIRS)])


def second_kernel(grid, parts_ref, last_ref, fields_ref, later_ref, basis_ref, sums_ref):
    _, _, x, own = grid
    rows, wide = last_ref.shape[1:]
    keep = inside(rows, wide, -x, own, grid)
    row = gathered_products(parts_ref)
    coefs = coefficients([entry(row, k) for k in range(len(PAIRS))])
    later = combined(coefs, [last_ref[k] for k in range(3)])
    later_ref[...] = later
    rhs = inv_step * later - hamiltonian(later) + coupling * fields_ref[1]
    vs = basis(jnp.where(keep, rhs, 0.0), fields_ref[0], keep)
    for k in range(3):
        basis_ref[k] = vs[k]
    mine = [middle(v, x, own) for v in vs]
    sums_ref[...] = row_of([(k, dot(mine[i], mine[j])) for k, (i, j) in enumerate(PAIRS)])


def third_kernel(grid, parts_ref, last_ref, fields_ref, later_ref, value_ref, images_ref, sums_ref):
    _, _, x, own = grid
    rows, wide = last_ref.shape[1:]
    cut = x // 2
    some = pl.ds(cut, rows - 2 * cut)
    keep = inside(rows - 2 * cut, wide, cut - x, own, grid)
    row = gathered_products(parts_ref)
    coefs = coefficients([entry(row, k) for k in range(len(PAIRS))])
    value = combined(coefs, [last_ref[k, some, :] for k in range(3)])
    value_ref[...] = middle(value, x, own)
    center = fields_ref[0, some, :]
    firsts = basis(density_rhs(fields_ref[2, some, :], drift(value), keep), center, keep)
    mine = [middle(v, x, own) for v in firsts]
    values = [(6 * 8 + k, dot(mine[i], mine[j])) for k, (i, j) in enumerate(PAIRS)]
    speeds = drift(later_ref[some, :])
    images = []
    for v in firsts[:3]:
        chain = basis(density_rhs(v, speeds, keep), center, keep)
        images.append([middle(w, x, own) for w in chain])
    for i in range(3):
        for k in range(3):
            images_ref[3 * i + k] = images[i][k]
    for place, (a, b) in enumerate(MIXED):
        for k, (i, j) in enumerate(PAIRS):
            values.append((8 * place + k, dot(images[a][i], images[b][j])))
    sums_ref[...] = row_of(values)


def fourth_kernel(parts_ref, images_ref, value_ref, value_out, density_ref):
    value_out[...] = value_ref[...]
    row = gathered_products(parts_ref)
    first = coefficients([entry(row, 6 * 8 + k) for k in range(len(PAIRS))])
    products = []
    for k in range(len(PAIRS)):
        total = None
        for place, (a, b) in enumerate(MIXED):
            term = first[a] * first[b] * entry(row, 8 * place + k)
            term = term if a == b else 2.0 * term
            total = term if total is None else total + term
        products.append(total)
    second = coefficients(products)
    total = None
    for i in range(3):
        for k in range(3):
            term = (first[i] * second[k]) * images_ref[3 * i + k]
            total = term if total is None else total + term
    density_ref[...] = total


def spread(row, axes):
    size = lax.axis_size(axes)
    copies = jnp.broadcast_to(row, (size, 1, 128))
    return lax.all_to_all(copies, axes, split_axis=0, concat_axis=0, tiled=True)


def everywhere(row):
    nearer = spread(row, FIRST).sum(axis=0)
    return spread(nearer, SECOND)


def swapped(far, near, axis):
    peers = lax.axis_size(axis)
    pairs = [(i, i + 1) for i in range(1, peers - 1, 2)]
    return (
        lax.ppermute(far, axis, pairs + [(b, a) for a, b in pairs]),
        lax.all_gather(near, axis[-1], tiled=True),
    )


def call(kernel, out_shape, *args, results=pltpu.VMEM):
    vmem = pl.BlockSpec(memory_space=pltpu.VMEM)
    return pl.pallas_call(
        kernel,
        out_shape=[results(s, jnp.float32) for s in out_shape],
        in_specs=[vmem] * len(args),
        out_specs=[vmem] * len(out_shape),
    )(*[pltpu.with_memory_space_constraint(a, pltpu.VMEM) for a in args])


def shards(terminal, initial_density, density_guess, diagonal):
    x, own = terminal.shape
    grid = (x * lax.axis_size(GX), own * lax.axis_size(GY), x, own)
    packed = (8 * (FIELDS + 2), own)
    fields, far, near = pl.pallas_call(
        stack_kernel,
        out_shape=[pltpu.VMEM(s, jnp.float32) for s in [(FIELDS, x, own), packed, packed]],
        in_specs=[pl.BlockSpec(memory_space=pltpu.HBM)] * 4,
        out_specs=[pl.BlockSpec(memory_space=pltpu.VMEM)] * 3,
        scratch_shapes=[pltpu.SemaphoreType.DMA((4,))],
    )(terminal, diagonal, density_guess, initial_density)
    strips = (3 * x, 128)
    tall, far, near = call(
        column_kernel, [(FIELDS, 3 * x, own), strips, strips], fields, *swapped(far, near, GX)
    )
    full = (3 * x, own + EDGE)
    basis1, kept, sums = call(
        functools.partial(first_kernel, grid),
        [(3, *full), (3, *full), (1, 128)],
        tall, *swapped(far, near, GY),
    )
    later, basis0, sums = call(
        functools.partial(second_kernel, grid),
        [full, (3, *full), (1, 128)],
        everywhere(sums), basis1, kept,
    )
    value, images, sums = call(
        functools.partial(third_kernel, grid),
        [(x, own), (9, x, own), (1, 128)],
        everywhere(sums), basis0, kept, later,
    )
    return tuple(
        call(
            fourth_kernel, [(x, own)] * 2, everywhere(sums), images, value,
            results=jax.ShapeDtypeStruct,
        )
    )


def solution(mesh):
    torus = Mesh(mesh.devices.reshape(8, 2, 2, 8, 2), GX + GY)
    in_specs = (P(GX, GY), P(GX, GY), P(None, GX, GY), P(GX, GY))
    out_specs = (P(GX, GY), P(GX, GY))
    return jax.shard_map(
        shards, mesh=torus, in_specs=in_specs, out_specs=out_specs, check_vma=False
    )
```

```python
import functools

import jax
import jax.numpy as jnp
from jax import lax
from jax.experimental import pallas as pl
from jax.experimental.pallas import tpu as pltpu
from jax.sharding import Mesh
from jax.sharding import PartitionSpec as P

BAND = ("band_0", "band_1")
PART = "part"
GX = (*BAND, PART)
GY = ("gy_0", "gy_1")

inv_step = 0.5
coupling = 0.5

LOW = 0.6
HIGH = 10.5
S1 = 2.0
S2 = 6.0
S3 = 4.0
PAIRS = ((0, 0), (0, 1), (0, 2), (1, 1), (1, 2), (2, 2), (2, 3))
MIXED = ((0, 0), (1, 1), (2, 2), (0, 1), (0, 2), (1, 2))

HALF = 64
EDGE = 128
TERMINAL, DIAGONAL, GUESS, INITIAL = 0, 1, 2, 4
FIELDS = 5
VMEM_LIMIT = 24 * 2**20
STRIP = 16
HALO = 16
INNER = 8


def before(v, dim):
    return pltpu.roll(v, 1, dim)


def after(v, dim):
    return pltpu.roll(v, v.shape[dim] - 1, dim)


def inside(rows, wide, first_row, own, grid):
    nx, ny, local_x, local_y = grid
    row = lax.broadcasted_iota(jnp.int32, (rows, wide), 0) + (lax.axis_index(BAND) * local_x + first_row)
    lane = lax.broadcasted_iota(jnp.int32, (rows, wide), 1)
    column = jnp.where(lane < own + HALF, lane, lane - wide) + lax.axis_index(GY) * local_y
    return (row >= 0) & (row < nx) & (column >= 0) & (column < ny)


def shifted(v, center, shift, keep):
    beside = (before(v, 0) + after(v, 0)) + (before(v, 1) + after(v, 1))
    return jnp.where(keep, (center - shift) * v - beside, 0.0)


def basis(v0, center, keep):
    v1 = shifted(v0, center, S1, keep)
    v2 = shifted(v1, center, S2, keep)
    return [v0, v1, v2, shifted(v2, center, S3, keep)]


def hamiltonian(u):
    ahead_x = after(u, 0) - u
    back_x = u - before(u, 0)
    ahead_y = after(u, 1) - u
    back_y = u - before(u, 1)
    return 0.5 * (
        jnp.maximum(back_x, 0.0) ** 2
        + jnp.minimum(ahead_x, 0.0) ** 2
        + jnp.maximum(back_y, 0.0) ** 2
        + jnp.minimum(ahead_y, 0.0) ** 2
    )


def drift(u):
    speed_x = u - after(u, 0)
    speed_y = u - after(u, 1)
    return (
        jnp.maximum(speed_x, 0.0),
        jnp.minimum(speed_x, 0.0),
        jnp.maximum(speed_y, 0.0),
        jnp.minimum(speed_y, 0.0),
    )


def density_rhs(m, speeds, keep):
    out_x, in_x, out_y, in_y = speeds
    flux_x = out_x * m + in_x * after(m, 0)
    flux_y = out_y * m + in_y * after(m, 1)
    div = (flux_x - before(flux_x, 0)) + (flux_y - before(flux_y, 1))
    return jnp.where(keep, inv_step * m - div, 0.0)


def dot(a, b):
    return jnp.sum(jnp.sum(a * b, axis=0, keepdims=True), axis=1, keepdims=True)


def row_of(values):
    lane = lax.broadcasted_iota(jnp.int32, (1, 128), 1)
    row = jnp.zeros((1, 128), jnp.float32)
    for place, value in values:
        row = jnp.where(lane == place, value, row)
    return row


def entry(row, place):
    lane = lax.broadcasted_iota(jnp.int32, row.shape, 1)
    return jnp.sum(jnp.where(lane == place, row, 0.0), axis=1, keepdims=True)


def form(matrix, vector):
    total = None
    for i, a in enumerate(vector):
        for j, b in enumerate(vector[: i + 1]):
            term = a * b * matrix[j][i]
            term = term if i == j else 2.0 * term
            total = term if total is None else total + term
    return total


def alpha_of(squared, energy):
    return jnp.clip(squared / jnp.maximum(energy, 1e-36), 0.999 / HIGH, 1.001 / LOW)


def beta_of(new, old):
    return jnp.clip(new / jnp.maximum(old, 1e-36), 0.0, 1.001 * HIGH / LOW)


def coefficients(products):
    g = dict(zip(PAIRS, products))
    gram = [[g[0, 0], g[0, 1], g[0, 2]], [None, g[1, 1], g[1, 2]], [None, None, g[2, 2]]]
    energy = [
        [g[0, 1] + S1 * g[0, 0], g[1, 1] + S1 * g[0, 1], g[1, 2] + S1 * g[0, 2]],
        [None, g[1, 2] + S2 * g[1, 1], g[2, 2] + S2 * g[1, 2]],
        [None, None, g[2, 3] + S3 * g[2, 2]],
    ]
    norm0 = g[0, 0]
    alpha0 = alpha_of(norm0, energy[0][0])
    resid1 = (1.0 - alpha0 * S1, -alpha0)
    norm1 = jnp.maximum(form(gram, resid1), 0.0)
    beta0 = beta_of(norm1, norm0)
    direct1 = (resid1[0] + beta0, resid1[1])
    alpha1 = alpha_of(norm1, form(energy, direct1))
    resid2 = (
        resid1[0] - alpha1 * (S1 * direct1[0]),
        resid1[1] - alpha1 * (direct1[0] + S2 * direct1[1]),
        -alpha1 * direct1[1],
    )
    norm2 = jnp.maximum(form(gram, resid2), 0.0)
    beta1 = beta_of(norm2, norm1)
    direct2 = (resid2[0] + beta1 * direct1[0], resid2[1] + beta1 * direct1[1], resid2[2])
    alpha2 = alpha_of(norm2, form(energy, direct2))
    return (
        alpha0 + alpha1 * direct1[0] + alpha2 * direct2[0],
        alpha1 * direct1[1] + alpha2 * direct2[1],
        alpha2 * direct2[2],
    )


def combined(coefs, vectors):
    total = coefs[0] * vectors[0]
    for c, v in zip(coefs[1:], vectors[1:]):
        total = total + c * v
    return total


def middle(v, x, own):
    return v[(v.shape[0] - x) // 2 : (v.shape[0] + x) // 2, :own]


def inner(v):
    return v[HALO - INNER : v.shape[0] - (HALO - INNER)]


def gathered_products(parts_ref):
    return jnp.sum(parts_ref[...], axis=0, keepdims=True)


def odd_index(axis, shape):
    place = lax.rem(lax.axis_index(axis), 2)
    return (lax.broadcasted_iota(jnp.int32, shape, 0) * 0 + place) == 1


def stack_kernel(terminal, diagonal, guess, initial, fields_ref, sems):
    copies = [
        pltpu.make_async_copy(terminal, fields_ref.at[TERMINAL], sems.at[0]),
        pltpu.make_async_copy(diagonal, fields_ref.at[DIAGONAL], sems.at[1]),
        pltpu.make_async_copy(guess, fields_ref.at[pl.ds(GUESS, 2)], sems.at[2]),
        pltpu.make_async_copy(initial, fields_ref.at[INITIAL], sems.at[3]),
    ]
    for copy in copies:
        copy.start()
    for copy in copies:
        copy.wait()


def row_kernel(band_ref, far_ref, near_ref):
    parts, _, _, own = band_ref.shape
    shape = (8, own)
    row = lax.broadcasted_iota(jnp.int32, shape, 0)
    first, second = ([band_ref[0, k, half] for k in range(FIELDS)] for half in (pl.ds(0, 8), pl.ds(8, 8)))
    top = first + [
        jnp.where(row < 5, second[TERMINAL], pltpu.roll(second[DIAGONAL], 5, 0)),
        jnp.where(row < 4, second[GUESS + 1], pltpu.roll(second[GUESS], 4, 0)),
    ]
    first, second = ([band_ref[parts - 1, k, half] for k in range(FIELDS)] for half in (pl.ds(0, 8), pl.ds(8, 8)))
    bottom = second + [
        jnp.where(row >= 3, first[TERMINAL], pltpu.roll(first[DIAGONAL], 3, 0)),
        jnp.where(row >= 4, first[GUESS + 1], pltpu.roll(first[GUESS], 4, 0)),
    ]
    odd = odd_index(BAND, shape)
    for k, (t, b) in enumerate(zip(top, bottom)):
        far_ref[8 * k : 8 * k + 8, :] = jnp.where(odd, b, t)
        near_ref[8 * k : 8 * k + 8, :] = jnp.where(odd, t, b)


def column_kernel(band_ref, far_ref, near_ref, tall_ref, far_edge, near_edge):
    parts, _, x, own = band_ref.shape
    odd = odd_index(BAND, (8, own))

    sent = FIELDS + 2

    def tile(k, odd_from, odd_start, even_from, even_start):
        odd_tile = odd_from[8 * (odd_start + k) : 8 * (odd_start + k) + 8, :]
        return jnp.where(odd, odd_tile, even_from[8 * (even_start + k) : 8 * (even_start + k) + 8, :])

    above = [tile(k, near_ref, 0, far_ref, 0) for k in range(sent)]
    below = [tile(k, far_ref, 0, near_ref, sent) for k in range(sent)]
    rest_above = {
        TERMINAL: above[FIELDS],
        DIAGONAL: pltpu.roll(above[FIELDS], 5, 0),
        GUESS + 1: above[FIELDS + 1],
        GUESS: pltpu.roll(above[FIELDS + 1], 4, 0),
    }
    rest_below = {
        TERMINAL: below[FIELDS],
        DIAGONAL: pltpu.roll(below[FIELDS], 3, 0),
        GUESS + 1: below[FIELDS + 1],
        GUESS: pltpu.roll(below[FIELDS + 1], 4, 0),
    }
    nothing = jnp.zeros((8, own), jnp.float32)
    shape = (parts * x + 2 * HALO, 128)
    strip = lax.broadcasted_iota(jnp.int32, shape, 1) // STRIP
    firsts = lasts = jnp.zeros(shape, jnp.float32)
    for k in range(FIELDS):
        blocks = [band_ref[part, k] for part in range(parts)]
        whole = jnp.concatenate(
            [rest_above.get(k, nothing), above[k], *blocks, below[k], rest_below.get(k, nothing)], axis=0
        )
        tall_ref[k] = whole
        first, last = whole[:, :128], whole[:, own - 128 :]
        firsts = jnp.where(strip == k, pltpu.roll(first, STRIP * k, 1) if k else first, firsts)
        lasts = jnp.where(strip == k, pltpu.roll(last, STRIP * (k + 1), 1), lasts)
    odd = odd_index(GY, shape)
    far_edge[...] = jnp.where(odd, lasts, firsts)
    near_edge[...] = jnp.where(odd, firsts, lasts)


def first_kernel(grid, tall_ref, far_edge, near_edge, basis_ref, center_ref, guess_ref, initial_ref, sums_ref):
    _, _, x, own = grid
    wide = own + EDGE
    rows = tall_ref.shape[1]
    keep = inside(rows, wide, -HALO, own, grid)
    odd = odd_index(GY, (rows, EDGE))
    left = jnp.where(odd, near_edge[:rows, :], far_edge[...])
    right = jnp.where(odd, far_edge[...], near_edge[rows:, :])
    half = lax.broadcasted_iota(jnp.int32, (rows, EDGE), 1) < HALF

    def extended(k):
        from_right = pltpu.roll(right, 128 - STRIP * k, 1) if k else right
        from_left = pltpu.roll(left, 128 - STRIP * (k + 1), 1)
        return jnp.concatenate([tall_ref[k], jnp.where(half, from_right, from_left)], axis=1)

    later = extended(TERMINAL)
    center = extended(DIAGONAL) + (inv_step + 4.0)
    rhs = inv_step * later - hamiltonian(later) + coupling * extended(GUESS + 1)
    vs = basis(jnp.where(keep, rhs, 0.0), center, keep)
    for k in range(3):
        basis_ref[k] = vs[k]
    center_ref[...] = center
    guess_ref[...] = extended(GUESS)
    initial_ref[...] = inner(extended(INITIAL))
    mine = [middle(v, x, own) for v in vs]
    sums_ref[...] = row_of([(k, dot(mine[i], mine[j])) for k, (i, j) in enumerate(PAIRS)])


def second_kernel(grid, parts_ref, last_ref, center_ref, guess_ref, later_ref, basis_ref, inner_center, sums_ref):
    _, _, x, own = grid
    rows, wide = last_ref.shape[1:]
    keep = inside(rows, wide, -HALO, own, grid)
    row = gathered_products(parts_ref)
    coefs = coefficients([entry(row, k) for k in range(len(PAIRS))])
    later = combined(coefs, [last_ref[k] for k in range(3)])
    later_ref[...] = inner(later)
    center = center_ref[...]
    inner_center[...] = inner(center)
    rhs = inv_step * later - hamiltonian(later) + coupling * guess_ref[...]
    vs = basis(jnp.where(keep, rhs, 0.0), center, keep)
    for k in range(3):
        basis_ref[k] = inner(vs[k])
    mine = [middle(v, x, own) for v in vs]
    sums_ref[...] = row_of([(k, dot(mine[i], mine[j])) for k, (i, j) in enumerate(PAIRS)])


def third_kernel(grid, parts_ref, last_ref, center_ref, initial_ref, later_ref, value_ref, images_ref, sums_ref):
    _, _, x, own = grid
    rows, wide = last_ref.shape[1:]
    keep = inside(rows, wide, -INNER, own, grid)
    row = gathered_products(parts_ref)
    coefs = coefficients([entry(row, k) for k in range(len(PAIRS))])
    value = combined(coefs, [last_ref[k] for k in range(3)])
    value_ref[...] = middle(value, x, own)
    center = center_ref[...]
    firsts = basis(density_rhs(initial_ref[...], drift(value), keep), center, keep)
    mine = [middle(v, x, own) for v in firsts]
    values = [(6 * 8 + k, dot(mine[i], mine[j])) for k, (i, j) in enumerate(PAIRS)]
    speeds = drift(later_ref[...])
    images = []
    for v in firsts[:3]:
        chain = basis(density_rhs(v, speeds, keep), center, keep)
        images.append([middle(w, x, own) for w in chain])
    for i in range(3):
        for k in range(3):
            images_ref[3 * i + k] = images[i][k]
    for place, (a, b) in enumerate(MIXED):
        for k, (i, j) in enumerate(PAIRS):
            values.append((8 * place + k, dot(images[a][i], images[b][j])))
    sums_ref[...] = row_of(values)


def fourth_kernel(parts_ref, images_ref, value_ref, value_out, density_ref):
    x = value_out.shape[0]
    mine = pl.ds(pl.multiple_of(lax.axis_index(PART) * x, x), x)
    value_out[...] = value_ref[mine, :]
    row = gathered_products(parts_ref)
    first = coefficients([entry(row, 6 * 8 + k) for k in range(len(PAIRS))])
    products = []
    for k in range(len(PAIRS)):
        total = None
        for place, (a, b) in enumerate(MIXED):
            term = first[a] * first[b] * entry(row, 8 * place + k)
            term = term if a == b else 2.0 * term
            total = term if total is None else total + term
        products.append(total)
    second = coefficients(products)
    total = None
    for i in range(3):
        for k in range(3):
            term = (first[i] * second[k]) * images_ref[3 * i + k, mine, :]
            total = term if total is None else total + term
    density_ref[...] = total


def everywhere(row):
    axes = (*BAND, *GY)
    size = lax.axis_size(axes)
    copies = jnp.broadcast_to(row, (size, 1, 128))
    return lax.all_to_all(copies, axes, split_axis=0, concat_axis=0, tiled=True).reshape(size, 128)


def swapped(far, near, axis):
    peers = lax.axis_size(axis)
    pairs = [(i, i + 1) for i in range(1, peers - 1, 2)]
    return (
        lax.ppermute(far, axis, pairs + [(b, a) for a, b in pairs]),
        lax.all_gather(near, axis[-1], tiled=True),
    )


def call(kernel, out_shape, *args, results=pltpu.VMEM):
    vmem = pl.BlockSpec(memory_space=pltpu.VMEM)
    return pl.pallas_call(
        kernel,
        out_shape=[results(s, jnp.float32) for s in out_shape],
        in_specs=[vmem] * len(args),
        out_specs=[vmem] * len(out_shape),
        compiler_params=pltpu.CompilerParams(vmem_limit_bytes=VMEM_LIMIT),
    )(*[pltpu.with_memory_space_constraint(a, pltpu.VMEM) for a in args])


def shards(terminal, initial_density, density_guess, diagonal):
    x, own = terminal.shape
    band = x * lax.axis_size(PART)
    grid = (x * lax.axis_size(GX), own * lax.axis_size(GY), band, own)
    fields = pl.pallas_call(
        stack_kernel,
        out_shape=pltpu.VMEM((FIELDS, x, own), jnp.float32),
        in_specs=[pl.BlockSpec(memory_space=pltpu.HBM)] * 4,
        out_specs=pl.BlockSpec(memory_space=pltpu.VMEM),
        scratch_shapes=[pltpu.SemaphoreType.DMA((4,))],
    )(terminal, diagonal, density_guess, initial_density)
    whole = lax.all_gather(fields, PART)
    packed = (8 * (FIELDS + 2), own)
    far, near = call(row_kernel, [packed, packed], whole)
    rows = band + 2 * HALO
    tall, far, near = call(
        column_kernel,
        [(FIELDS, rows, own), (rows, 128), (rows, 128)],
        whole, *swapped(far, near, BAND),
    )
    wide = own + EDGE
    full, fewer = (rows, wide), (band + 2 * INNER, wide)
    basis1, center, guess, initial, sums = call(
        functools.partial(first_kernel, grid),
        [(3, *full), full, full, fewer, (1, 128)],
        tall, *swapped(far, near, GY),
    )
    later, basis0, center, sums = call(
        functools.partial(second_kernel, grid),
        [fewer, (3, *fewer), fewer, (1, 128)],
        everywhere(sums), basis1, center, guess,
    )
    value, images, sums = call(
        functools.partial(third_kernel, grid),
        [(band, own), (9, band, own), (1, 128)],
        everywhere(sums), basis0, center, initial, later,
    )
    return tuple(
        call(
            fourth_kernel, [(x, own)] * 2, everywhere(sums), images, value,
            results=jax.ShapeDtypeStruct,
        )
    )


def solution(mesh):
    torus = Mesh(mesh.devices.reshape(4, 2, 4, 8, 2), GX + GY)
    in_specs = (P(GX, GY), P(GX, GY), P(None, GX, GY), P(GX, GY))
    out_specs = (P(GX, GY), P(GX, GY))
    return jax.shard_map(
        shards, mesh=torus, in_specs=in_specs, out_specs=out_specs, check_vma=False
    )
```

```python
import functools

import jax
import jax.numpy as jnp
from jax import lax
from jax.experimental import pallas as pl
from jax.experimental.pallas import tpu as pltpu
from jax.sharding import Mesh
from jax.sharding import PartitionSpec as P

BAND = ("band_0", "band_1")
PART = "part"
GX = (*BAND, PART)
GY = ("gy_0", "gy_1")

inv_step = 0.5
coupling = 0.5

LOW = 0.6
HIGH = 10.5
S1 = 3.5
S2 = 5.5
S3 = 4.0
PAIRS = ((0, 0), (0, 1), (1, 1), (1, 2), (2, 2), (2, 3))
MIXED = ((0, 0), (1, 1), (2, 2), (0, 1), (0, 2), (1, 2))

HALF = 64
EDGE = 128
TERMINAL, DIAGONAL, GUESS, INITIAL = 0, 1, 2, 4
FIELDS = 5
SENT = FIELDS + 3
VMEM_LIMIT = 24 * 2**20
STRIP = 16
HALO = 16
INNER = 8


def before(v, dim):
    return pltpu.roll(v, 1, dim)


def after(v, dim):
    return pltpu.roll(v, v.shape[dim] - 1, dim)


def inside(rows, wide, first_row, own, grid):
    nx, ny, local_x, local_y = grid
    row = lax.broadcasted_iota(jnp.int32, (rows, wide), 0) + (lax.axis_index(BAND) * local_x + first_row)
    lane = lax.broadcasted_iota(jnp.int32, (rows, wide), 1)
    column = jnp.where(lane < own + HALF, lane, lane - wide) + lax.axis_index(GY) * local_y
    return (row >= 0) & (row < nx) & (column >= 0) & (column < ny)


def shifted(v, center, shift, keep):
    beside = (before(v, 0) + after(v, 0)) + (before(v, 1) + after(v, 1))
    return jnp.where(keep, (center - shift) * v - beside, 0.0)


def basis(v0, center, keep):
    v1 = shifted(v0, center, S1, keep)
    v2 = shifted(v1, center, S2, keep)
    return [v0, v1, v2, shifted(v2, center, S3, keep)]


def hamiltonian(u):
    ahead_x = after(u, 0) - u
    back_x = u - before(u, 0)
    ahead_y = after(u, 1) - u
    back_y = u - before(u, 1)
    return 0.5 * (
        jnp.maximum(back_x, 0.0) ** 2
        + jnp.minimum(ahead_x, 0.0) ** 2
        + jnp.maximum(back_y, 0.0) ** 2
        + jnp.minimum(ahead_y, 0.0) ** 2
    )


def drift(u):
    speed_x = u - after(u, 0)
    speed_y = u - after(u, 1)
    return (
        jnp.maximum(speed_x, 0.0),
        jnp.minimum(speed_x, 0.0),
        jnp.maximum(speed_y, 0.0),
        jnp.minimum(speed_y, 0.0),
    )


def density_rhs(m, speeds, keep):
    out_x, in_x, out_y, in_y = speeds
    flux_x = out_x * m + in_x * after(m, 0)
    flux_y = out_y * m + in_y * after(m, 1)
    div = (flux_x - before(flux_x, 0)) + (flux_y - before(flux_y, 1))
    return jnp.where(keep, inv_step * m - div, 0.0)


def dot(a, b):
    rows, wide = a.shape
    total = jnp.sum((a * b).reshape(rows // 8, 8, wide), axis=0)
    total = sum(total[:, k : k + 128] for k in range(128, wide, 128)) + total[:, :128]
    return jnp.sum(jnp.sum(total, axis=1, keepdims=True), axis=0, keepdims=True)


def row_of(values):
    lane = lax.broadcasted_iota(jnp.int32, (1, 128), 1)
    row = jnp.zeros((1, 128), jnp.float32)
    for place, value in values:
        row = jnp.where(lane == place, value, row)
    return row


def entry(row, place):
    lane = lax.broadcasted_iota(jnp.int32, row.shape, 1)
    return jnp.sum(jnp.where(lane == place, row, 0.0), axis=1, keepdims=True)


def form(matrix, vector):
    total = None
    for i, a in enumerate(vector):
        for j, b in enumerate(vector[: i + 1]):
            term = a * b * matrix[j][i]
            term = term if i == j else 2.0 * term
            total = term if total is None else total + term
    return total


def alpha_of(squared, energy):
    return jnp.clip(squared / jnp.maximum(energy, 1e-36), 0.999 / HIGH, 1.001 / LOW)


def beta_of(new, old):
    return jnp.clip(new / jnp.maximum(old, 1e-36), 0.0, 1.001 * HIGH / LOW)


def coefficients(products):
    g = dict(zip(PAIRS, products))
    g[0, 2] = g[1, 1] + (S1 - S2) * g[0, 1]
    gram = [[g[0, 0], g[0, 1], g[0, 2]], [None, g[1, 1], g[1, 2]], [None, None, g[2, 2]]]
    energy = [
        [g[0, 1] + S1 * g[0, 0], g[1, 1] + S1 * g[0, 1], g[1, 2] + S1 * g[0, 2]],
        [None, g[1, 2] + S2 * g[1, 1], g[2, 2] + S2 * g[1, 2]],
        [None, None, g[2, 3] + S3 * g[2, 2]],
    ]
    norm0 = g[0, 0]
    alpha0 = alpha_of(norm0, energy[0][0])
    resid1 = (1.0 - alpha0 * S1, -alpha0)
    norm1 = jnp.maximum(form(gram, resid1), 0.0)
    beta0 = beta_of(norm1, norm0)
    direct1 = (resid1[0] + beta0, resid1[1])
    alpha1 = alpha_of(norm1, form(energy, direct1))
    resid2 = (
        resid1[0] - alpha1 * (S1 * direct1[0]),
        resid1[1] - alpha1 * (direct1[0] + S2 * direct1[1]),
        -alpha1 * direct1[1],
    )
    norm2 = jnp.maximum(form(gram, resid2), 0.0)
    beta1 = beta_of(norm2, norm1)
    direct2 = (resid2[0] + beta1 * direct1[0], resid2[1] + beta1 * direct1[1], resid2[2])
    alpha2 = alpha_of(norm2, form(energy, direct2))
    return (
        alpha0 + alpha1 * direct1[0] + alpha2 * direct2[0],
        alpha1 * direct1[1] + alpha2 * direct2[1],
        alpha2 * direct2[2],
    )


def combined(coefs, vectors):
    total = coefs[0] * vectors[0]
    for c, v in zip(coefs[1:], vectors[1:]):
        total = total + c * v
    return total


def middle(v, x, own):
    return v[(v.shape[0] - x) // 2 : (v.shape[0] + x) // 2, :own]


def inner(v):
    return v[HALO - INNER : v.shape[0] - (HALO - INNER)]


def gathered_products(parts_ref):
    return jnp.sum(parts_ref[...], axis=0, keepdims=True)


def odd_index(axis, shape):
    place = lax.rem(lax.axis_index(axis), 2)
    return (lax.broadcasted_iota(jnp.int32, shape, 0) * 0 + place) == 1


def stack_kernel(terminal, diagonal, guess, initial, fields_ref, far_edge, near_edge, sems):
    copies = [
        pltpu.make_async_copy(terminal, fields_ref.at[TERMINAL], sems.at[0]),
        pltpu.make_async_copy(diagonal, fields_ref.at[DIAGONAL], sems.at[1]),
        pltpu.make_async_copy(guess, fields_ref.at[pl.ds(GUESS, 2)], sems.at[2]),
        pltpu.make_async_copy(initial, fields_ref.at[INITIAL], sems.at[3]),
    ]
    for copy in copies:
        copy.start()
    for copy in copies:
        copy.wait()
    _, x, own = fields_ref.shape
    shape = (x, 128)
    strip = lax.broadcasted_iota(jnp.int32, shape, 1) // STRIP
    firsts = lasts = jnp.zeros(shape, jnp.float32)
    for k in range(FIELDS):
        first, last = fields_ref[k, :, :128], fields_ref[k, :, own - 128 :]
        firsts = jnp.where(strip == k, pltpu.roll(first, STRIP * k, 1) if k else first, firsts)
        lasts = jnp.where(strip == k, pltpu.roll(last, STRIP * (k + 1), 1), lasts)
    odd = odd_index(GY, shape)
    far_edge[...] = jnp.where(odd, lasts, firsts)
    near_edge[...] = jnp.where(odd, firsts, lasts)


def edge_kernel(fields_ref, far_edge, near_edge, block_ref):
    _, x, own = fields_ref.shape
    odd = odd_index(GY, (x, EDGE))
    left = jnp.where(odd, near_edge[:x, :], far_edge[...])
    right = jnp.where(odd, far_edge[...], near_edge[x:, :])
    for k in range(FIELDS):
        block_ref[x * k : x * (k + 1), :] = fields_ref[k]
    edges = [right[:8], left[:8], right[8:], left[8:]]
    block_ref[x * FIELDS :, :] = jnp.concatenate(edges, axis=1)


def row_kernel(band_ref, far_ref, near_ref):
    parts, _, own = band_ref.shape
    shape = (8, own)
    row = lax.broadcasted_iota(jnp.int32, shape, 0)

    def halves(part):
        tiles = [band_ref[part, 8 * k : 8 * k + 8, :] for k in range(2 * FIELDS + 1)]
        return tiles[: 2 * FIELDS : 2], tiles[1 : 2 * FIELDS : 2], tiles[2 * FIELDS]

    first, second, edge = halves(0)
    top = first + [
        jnp.where(row < 5, second[TERMINAL], pltpu.roll(second[DIAGONAL], 5, 0)),
        jnp.where(row < 4, second[GUESS + 1], pltpu.roll(second[GUESS], 4, 0)),
        edge,
    ]
    first, second, edge = halves(parts - 1)
    bottom = second + [
        jnp.where(row >= 3, first[TERMINAL], pltpu.roll(first[DIAGONAL], 3, 0)),
        jnp.where(row >= 4, first[GUESS + 1], pltpu.roll(first[GUESS], 4, 0)),
        edge,
    ]
    odd = odd_index(BAND, shape)
    for k, (t, b) in enumerate(zip(top, bottom)):
        far_ref[8 * k : 8 * k + 8, :] = jnp.where(odd, b, t)
        near_ref[8 * k : 8 * k + 8, :] = jnp.where(odd, t, b)


def first_kernel(grid, band_ref, far_ref, near_ref, basis_ref, center_ref, guess_ref, initial_ref, sums_ref):
    _, _, x, own = grid
    wide = own + EDGE
    rows = x + 2 * HALO
    parts = band_ref.shape[0]
    keep = inside(rows, wide, -HALO, own, grid)
    odd = odd_index(BAND, (8, own))

    def tile(k, odd_from, odd_start, even_from, even_start):
        odd_tile = odd_from[8 * (odd_start + k) : 8 * (odd_start + k) + 8, :]
        return jnp.where(odd, odd_tile, even_from[8 * (even_start + k) : 8 * (even_start + k) + 8, :])

    above = [tile(k, near_ref, 0, far_ref, 0) for k in range(SENT)]
    below = [tile(k, far_ref, 0, near_ref, SENT) for k in range(SENT)]
    rest_above = {
        TERMINAL: above[FIELDS],
        DIAGONAL: pltpu.roll(above[FIELDS], 5, 0),
        GUESS + 1: above[FIELDS + 1],
        GUESS: pltpu.roll(above[FIELDS + 1], 4, 0),
    }
    rest_below = {
        TERMINAL: below[FIELDS],
        DIAGONAL: pltpu.roll(below[FIELDS], 3, 0),
        GUESS + 1: below[FIELDS + 1],
        GUESS: pltpu.roll(below[FIELDS + 1], 4, 0),
    }
    nothing = jnp.zeros((8, own), jnp.float32)
    blocks = [above[-1], *[band_ref[part, 2 * 8 * FIELDS :, :] for part in range(parts)], below[-1]]
    right, left = (
        jnp.concatenate([b[:, at : at + 128] for b in blocks for at in (start, start + 256)], axis=0)
        for start in (0, 128)
    )
    half = lax.broadcasted_iota(jnp.int32, (rows, EDGE), 1) < HALF

    def extended(k):
        whole = jnp.concatenate(
            [
                rest_above.get(k, nothing),
                above[k],
                *[band_ref[part, 16 * k : 16 * k + 16, :] for part in range(parts)],
                below[k],
                rest_below.get(k, nothing),
            ],
            axis=0,
        )
        from_right = pltpu.roll(right, 128 - STRIP * k, 1) if k else right
        from_left = pltpu.roll(left, 128 - STRIP * (k + 1), 1)
        return jnp.concatenate([whole, jnp.where(half, from_right, from_left)], axis=1)

    later = extended(TERMINAL)
    center = extended(DIAGONAL) + (inv_step + 4.0)
    rhs = inv_step * later - hamiltonian(later) + coupling * extended(GUESS + 1)
    vs = basis(jnp.where(keep, rhs, 0.0), center, keep)
    for k in range(3):
        basis_ref[k] = vs[k]
    center_ref[...] = center
    guess_ref[...] = extended(GUESS)
    initial_ref[...] = inner(extended(INITIAL))
    mine = [middle(v, x, own) for v in vs]
    sums_ref[...] = row_of([(k, dot(mine[i], mine[j])) for k, (i, j) in enumerate(PAIRS)])


def second_kernel(grid, parts_ref, last_ref, center_ref, guess_ref, later_ref, basis_ref, inner_center, sums_ref):
    _, _, x, own = grid
    rows, wide = last_ref.shape[1:]
    keep = inside(rows, wide, -HALO, own, grid)
    row = gathered_products(parts_ref)
    coefs = coefficients([entry(row, k) for k in range(len(PAIRS))])
    later = combined(coefs, [last_ref[k] for k in range(3)])
    later_ref[...] = inner(later)
    center = center_ref[...]
    inner_center[...] = inner(center)
    rhs = inv_step * later - hamiltonian(later) + coupling * guess_ref[...]
    vs = basis(jnp.where(keep, rhs, 0.0), center, keep)
    for k in range(3):
        basis_ref[k] = inner(vs[k])
    mine = [middle(v, x, own) for v in vs]
    sums_ref[...] = row_of([(k, dot(mine[i], mine[j])) for k, (i, j) in enumerate(PAIRS)])


def third_kernel(grid, parts_ref, last_ref, center_ref, initial_ref, later_ref, value_ref, images_ref, sums_ref):
    _, _, x, own = grid
    rows, wide = last_ref.shape[1:]
    keep = inside(rows, wide, -INNER, own, grid)
    row = gathered_products(parts_ref)
    coefs = coefficients([entry(row, k) for k in range(len(PAIRS))])
    value = combined(coefs, [last_ref[k] for k in range(3)])
    value_ref[...] = middle(value, x, own)
    center = center_ref[...]
    firsts = basis(density_rhs(initial_ref[...], drift(value), keep), center, keep)
    mine = [middle(v, x, own) for v in firsts]
    values = [(6 * 8 + k, dot(mine[i], mine[j])) for k, (i, j) in enumerate(PAIRS)]
    speeds = drift(later_ref[...])
    images = []
    for v in firsts[:3]:
        chain = basis(density_rhs(v, speeds, keep), center, keep)
        images.append([middle(w, x, own) for w in chain])
    for i in range(3):
        for k in range(3):
            images_ref[3 * i + k] = images[i][k]
    for place, (a, b) in enumerate(MIXED):
        for k, (i, j) in enumerate(PAIRS):
            values.append((8 * place + k, dot(images[a][i], images[b][j])))
    sums_ref[...] = row_of(values)


def fourth_kernel(parts_ref, images_ref, value_ref, value_out, density_ref):
    x = value_out.shape[0]
    mine = pl.ds(pl.multiple_of(lax.axis_index(PART) * x, x), x)
    value_out[...] = value_ref[mine, :]
    row = gathered_products(parts_ref)
    first = coefficients([entry(row, 6 * 8 + k) for k in range(len(PAIRS))])
    products = []
    for k in range(len(PAIRS)):
        total = None
        for place, (a, b) in enumerate(MIXED):
            term = first[a] * first[b] * entry(row, 8 * place + k)
            term = term if a == b else 2.0 * term
            total = term if total is None else total + term
        products.append(total)
    second = coefficients(products)
    total = None
    for i in range(3):
        for k in range(3):
            term = (first[i] * second[k]) * images_ref[3 * i + k, mine, :]
            total = term if total is None else total + term
    density_ref[...] = total


def everywhere(row):
    axes = (*BAND, *GY)
    size = lax.axis_size(axes)
    copies = jnp.broadcast_to(row, (size, 1, 128))
    return lax.all_to_all(copies, axes, split_axis=0, concat_axis=0, tiled=True).reshape(size, 128)


def swapped(far, near, axis):
    peers = lax.axis_size(axis)
    pairs = [(i, i + 1) for i in range(1, peers - 1, 2)]
    return (
        lax.ppermute(far, axis, pairs + [(b, a) for a, b in pairs]),
        lax.all_gather(near, axis[-1], tiled=True),
    )


def call(kernel, out_shape, *args, results=pltpu.VMEM):
    vmem = pl.BlockSpec(memory_space=pltpu.VMEM)
    return pl.pallas_call(
        kernel,
        out_shape=[results(s, jnp.float32) for s in out_shape],
        in_specs=[vmem] * len(args),
        out_specs=[vmem] * len(out_shape),
        compiler_params=pltpu.CompilerParams(vmem_limit_bytes=VMEM_LIMIT),
    )(*[pltpu.with_memory_space_constraint(a, pltpu.VMEM) for a in args])


def shards(terminal, initial_density, density_guess, diagonal):
    x, own = terminal.shape
    band = x * lax.axis_size(PART)
    grid = (x * lax.axis_size(GX), own * lax.axis_size(GY), band, own)
    fields, far, near = pl.pallas_call(
        stack_kernel,
        out_shape=[pltpu.VMEM(s, jnp.float32) for s in [(FIELDS, x, own), (x, EDGE), (x, EDGE)]],
        in_specs=[pl.BlockSpec(memory_space=pltpu.HBM)] * 4,
        out_specs=[pl.BlockSpec(memory_space=pltpu.VMEM)] * 3,
        scratch_shapes=[pltpu.SemaphoreType.DMA((4,))],
    )(terminal, diagonal, density_guess, initial_density)
    (block,) = call(edge_kernel, [(x * FIELDS + 8, own)], fields, *swapped(far, near, GY))
    whole = lax.all_gather(block, PART)
    packed = (8 * SENT, own)
    far, near = call(row_kernel, [packed, packed], whole)
    rows = band + 2 * HALO
    wide = own + EDGE
    full, fewer = (rows, wide), (band + 2 * INNER, wide)
    basis1, center, guess, initial, sums = call(
        functools.partial(first_kernel, grid),
        [(3, *full), full, full, fewer, (1, 128)],
        whole, *swapped(far, near, BAND),
    )
    later, basis0, center, sums = call(
        functools.partial(second_kernel, grid),
        [fewer, (3, *fewer), fewer, (1, 128)],
        everywhere(sums), basis1, center, guess,
    )
    value, images, sums = call(
        functools.partial(third_kernel, grid),
        [(band, own), (9, band, own), (1, 128)],
        everywhere(sums), basis0, center, initial, later,
    )
    return tuple(
        call(
            fourth_kernel, [(x, own)] * 2, everywhere(sums), images, value,
            results=jax.ShapeDtypeStruct,
        )
    )


def solution(mesh):
    torus = Mesh(mesh.devices.reshape(4, 2, 4, 8, 2), GX + GY)
    in_specs = (P(GX, GY), P(GX, GY), P(None, GX, GY), P(GX, GY))
    out_specs = (P(GX, GY), P(GX, GY))
    return jax.shard_map(
        shards, mesh=torus, in_specs=in_specs, out_specs=out_specs, check_vma=False
    )
```

```python
import functools

import jax
import jax.numpy as jnp
from jax import lax
from jax.experimental import pallas as pl
from jax.experimental.pallas import tpu as pltpu
from jax.sharding import Mesh
from jax.sharding import PartitionSpec as P

BAND = ("band_0", "band_1")
PART = "part"
GX = (*BAND, PART)
GY = ("gy_0", "gy_1")

inv_step = 0.5
coupling = 0.5

LOW = 0.6
HIGH = 10.5
S1 = 3.5
S2 = 5.5
S3 = 4.0
PAIRS = ((0, 0), (0, 1), (1, 1), (1, 2), (2, 2), (2, 3))
MIXED = ((0, 0), (1, 1), (2, 2), (0, 1), (0, 2), (1, 2))

HALF = 64
EDGE = 128
TERMINAL, DIAGONAL, GUESS, INITIAL = 0, 1, 2, 4
FIELDS = 5
SENT = FIELDS + 3
VMEM_LIMIT = 24 * 2**20
STRIP = 16
HALO = 16
INNER = 8


def before(v, dim):
    return pltpu.roll(v, 1, dim)


def after(v, dim):
    return pltpu.roll(v, v.shape[dim] - 1, dim)


def keeper(halo, x, own):
    band, column = lax.axis_index(BAND), lax.axis_index(GY)
    bands, columns = lax.axis_size(BAND), lax.axis_size(GY)
    top = jnp.where(band > 0, 1.0, 0.0)
    bottom = jnp.where(band < bands - 1, 1.0, 0.0)
    lane = lax.broadcasted_iota(jnp.int32, (8, EDGE), 1)
    edge = jnp.where(
        lane < HALF, jnp.where(column < columns - 1, 1.0, 0.0), jnp.where(column > 0, 1.0, 0.0)
    )

    def tiled(rows):
        return jnp.concatenate([edge] * (rows // 8), axis=0)

    ends = tiled(halo)

    def keep(v):
        first, last = v[:halo], v[halo + x :]
        inner_rows = v[halo : halo + x]
        main = [first[:, :own] * top, inner_rows[:, :own], last[:, :own] * bottom]
        side = [
            first[:, own:] * (ends * top),
            inner_rows[:, own:] * tiled(x),
            last[:, own:] * (ends * bottom),
        ]
        return jnp.concatenate([jnp.concatenate(p, axis=0) for p in (main, side)], axis=1)

    return keep


def shifted(v, center, shift, keep):
    beside = (before(v, 0) + after(v, 0)) + (before(v, 1) + after(v, 1))
    return keep((center - shift) * v - beside)


def basis(v0, center, keep):
    v1 = shifted(v0, center, S1, keep)
    v2 = shifted(v1, center, S2, keep)
    return [v0, v1, v2, shifted(v2, center, S3, keep)]


def hamiltonian(u):
    ahead_x = after(u, 0) - u
    back_x = u - before(u, 0)
    ahead_y = after(u, 1) - u
    back_y = u - before(u, 1)
    return 0.5 * (
        jnp.maximum(back_x, 0.0) ** 2
        + jnp.minimum(ahead_x, 0.0) ** 2
        + jnp.maximum(back_y, 0.0) ** 2
        + jnp.minimum(ahead_y, 0.0) ** 2
    )


def drift(u):
    speed_x = u - after(u, 0)
    speed_y = u - after(u, 1)
    return (
        jnp.maximum(speed_x, 0.0),
        jnp.minimum(speed_x, 0.0),
        jnp.maximum(speed_y, 0.0),
        jnp.minimum(speed_y, 0.0),
    )


def density_rhs(m, speeds, keep):
    out_x, in_x, out_y, in_y = speeds
    flux_x = out_x * m + in_x * after(m, 0)
    flux_y = out_y * m + in_y * after(m, 1)
    div = (flux_x - before(flux_x, 0)) + (flux_y - before(flux_y, 1))
    return keep(inv_step * m - div)


def dot(a, b):
    rows, wide = a.shape
    total = jnp.sum((a * b).reshape(rows // 8, 8, wide), axis=0)
    total = sum(total[:, k : k + 128] for k in range(128, wide, 128)) + total[:, :128]
    return jnp.sum(jnp.sum(total, axis=1, keepdims=True), axis=0, keepdims=True)


def row_of(values):
    lane = lax.broadcasted_iota(jnp.int32, (1, 128), 1)
    row = jnp.zeros((1, 128), jnp.float32)
    for place, value in values:
        row = jnp.where(lane == place, value, row)
    return row


def entry(row, place):
    lane = lax.broadcasted_iota(jnp.int32, row.shape, 1)
    return jnp.sum(jnp.where(lane == place, row, 0.0), axis=1, keepdims=True)


def form(matrix, vector):
    total = None
    for i, a in enumerate(vector):
        for j, b in enumerate(vector[: i + 1]):
            term = a * b * matrix[j][i]
            term = term if i == j else 2.0 * term
            total = term if total is None else total + term
    return total


def alpha_of(squared, energy):
    return jnp.clip(squared / jnp.maximum(energy, 1e-36), 0.999 / HIGH, 1.001 / LOW)


def beta_of(new, old):
    return jnp.clip(new / jnp.maximum(old, 1e-36), 0.0, 1.001 * HIGH / LOW)


def coefficients(products):
    g = dict(zip(PAIRS, products))
    g[0, 2] = g[1, 1] + (S1 - S2) * g[0, 1]
    gram = [[g[0, 0], g[0, 1], g[0, 2]], [None, g[1, 1], g[1, 2]], [None, None, g[2, 2]]]
    energy = [
        [g[0, 1] + S1 * g[0, 0], g[1, 1] + S1 * g[0, 1], g[1, 2] + S1 * g[0, 2]],
        [None, g[1, 2] + S2 * g[1, 1], g[2, 2] + S2 * g[1, 2]],
        [None, None, g[2, 3] + S3 * g[2, 2]],
    ]
    norm0 = g[0, 0]
    alpha0 = alpha_of(norm0, energy[0][0])
    resid1 = (1.0 - alpha0 * S1, -alpha0)
    norm1 = jnp.maximum(form(gram, resid1), 0.0)
    beta0 = beta_of(norm1, norm0)
    direct1 = (resid1[0] + beta0, resid1[1])
    alpha1 = alpha_of(norm1, form(energy, direct1))
    resid2 = (
        resid1[0] - alpha1 * (S1 * direct1[0]),
        resid1[1] - alpha1 * (direct1[0] + S2 * direct1[1]),
        -alpha1 * direct1[1],
    )
    norm2 = jnp.maximum(form(gram, resid2), 0.0)
    beta1 = beta_of(norm2, norm1)
    direct2 = (resid2[0] + beta1 * direct1[0], resid2[1] + beta1 * direct1[1], resid2[2])
    alpha2 = alpha_of(norm2, form(energy, direct2))
    return (
        alpha0 + alpha1 * direct1[0] + alpha2 * direct2[0],
        alpha1 * direct1[1] + alpha2 * direct2[1],
        alpha2 * direct2[2],
    )


def combined(coefs, vectors):
    total = coefs[0] * vectors[0]
    for c, v in zip(coefs[1:], vectors[1:]):
        total = total + c * v
    return total


def middle(v, x, own):
    return v[(v.shape[0] - x) // 2 : (v.shape[0] + x) // 2, :own]


def inner(v):
    return v[HALO - INNER : v.shape[0] - (HALO - INNER)]


def gathered_products(parts_ref):
    return jnp.sum(parts_ref[...], axis=0, keepdims=True)


def odd_index(axis, shape):
    place = lax.rem(lax.axis_index(axis), 2)
    return (lax.broadcasted_iota(jnp.int32, shape, 0) * 0 + place) == 1


def stack_kernel(terminal, diagonal, guess, initial, fields_ref, far_edge, near_edge, sems):
    copies = [
        pltpu.make_async_copy(terminal, fields_ref.at[TERMINAL], sems.at[0]),
        pltpu.make_async_copy(diagonal, fields_ref.at[DIAGONAL], sems.at[1]),
        pltpu.make_async_copy(guess, fields_ref.at[pl.ds(GUESS, 2)], sems.at[2]),
        pltpu.make_async_copy(initial, fields_ref.at[INITIAL], sems.at[3]),
    ]
    for copy in copies:
        copy.start()
    for copy in copies:
        copy.wait()
    _, x, own = fields_ref.shape
    shape = (x, 128)
    strip = lax.broadcasted_iota(jnp.int32, shape, 1) // STRIP
    firsts = lasts = jnp.zeros(shape, jnp.float32)
    for k in range(FIELDS):
        first, last = fields_ref[k, :, :128], fields_ref[k, :, own - 128 :]
        firsts = jnp.where(strip == k, pltpu.roll(first, STRIP * k, 1) if k else first, firsts)
        lasts = jnp.where(strip == k, pltpu.roll(last, STRIP * (k + 1), 1), lasts)
    odd = odd_index(GY, shape)
    far_edge[...] = jnp.where(odd, lasts, firsts)
    near_edge[...] = jnp.where(odd, firsts, lasts)


def edge_kernel(fields_ref, far_edge, near_edge, block_ref):
    _, x, own = fields_ref.shape
    odd = odd_index(GY, (x, EDGE))
    left = jnp.where(odd, near_edge[:x, :], far_edge[...])
    right = jnp.where(odd, far_edge[...], near_edge[x:, :])
    for k in range(FIELDS):
        block_ref[x * k : x * (k + 1), :] = fields_ref[k]
    edges = [right[:8], left[:8], right[8:], left[8:]]
    block_ref[x * FIELDS :, :] = jnp.concatenate(edges, axis=1)


def row_kernel(band_ref, far_ref, near_ref):
    parts, _, own = band_ref.shape
    shape = (8, own)
    row = lax.broadcasted_iota(jnp.int32, shape, 0)

    def halves(part):
        tiles = [band_ref[part, 8 * k : 8 * k + 8, :] for k in range(2 * FIELDS + 1)]
        return tiles[: 2 * FIELDS : 2], tiles[1 : 2 * FIELDS : 2], tiles[2 * FIELDS]

    first, second, edge = halves(0)
    top = first + [
        jnp.where(row < 5, second[TERMINAL], pltpu.roll(second[DIAGONAL], 5, 0)),
        jnp.where(row < 4, second[GUESS + 1], pltpu.roll(second[GUESS], 4, 0)),
        edge,
    ]
    first, second, edge = halves(parts - 1)
    bottom = second + [
        jnp.where(row >= 3, first[TERMINAL], pltpu.roll(first[DIAGONAL], 3, 0)),
        jnp.where(row >= 4, first[GUESS + 1], pltpu.roll(first[GUESS], 4, 0)),
        edge,
    ]
    odd = odd_index(BAND, shape)
    for k, (t, b) in enumerate(zip(top, bottom)):
        far_ref[8 * k : 8 * k + 8, :] = jnp.where(odd, b, t)
        near_ref[8 * k : 8 * k + 8, :] = jnp.where(odd, t, b)


def first_kernel(grid, band_ref, far_ref, near_ref, basis_ref, center_ref, guess_ref, initial_ref, sums_ref):
    _, _, x, own = grid
    wide = own + EDGE
    rows = x + 2 * HALO
    parts = band_ref.shape[0]
    keep = keeper(HALO, x, own)
    odd = odd_index(BAND, (8, own))

    def tile(k, odd_from, odd_start, even_from, even_start):
        odd_tile = odd_from[8 * (odd_start + k) : 8 * (odd_start + k) + 8, :]
        return jnp.where(odd, odd_tile, even_from[8 * (even_start + k) : 8 * (even_start + k) + 8, :])

    above = [tile(k, near_ref, 0, far_ref, 0) for k in range(SENT)]
    below = [tile(k, far_ref, 0, near_ref, SENT) for k in range(SENT)]
    rest_above = {
        TERMINAL: above[FIELDS],
        DIAGONAL: pltpu.roll(above[FIELDS], 5, 0),
        GUESS + 1: above[FIELDS + 1],
        GUESS: pltpu.roll(above[FIELDS + 1], 4, 0),
    }
    rest_below = {
        TERMINAL: below[FIELDS],
        DIAGONAL: pltpu.roll(below[FIELDS], 3, 0),
        GUESS + 1: below[FIELDS + 1],
        GUESS: pltpu.roll(below[FIELDS + 1], 4, 0),
    }
    nothing = jnp.zeros((8, own), jnp.float32)
    blocks = [above[-1], *[band_ref[part, 2 * 8 * FIELDS :, :] for part in range(parts)], below[-1]]
    right, left = (
        jnp.concatenate([b[:, at : at + 128] for b in blocks for at in (start, start + 256)], axis=0)
        for start in (0, 128)
    )
    half = lax.broadcasted_iota(jnp.int32, (rows, EDGE), 1) < HALF

    def extended(k):
        whole = jnp.concatenate(
            [
                rest_above.get(k, nothing),
                above[k],
                *[band_ref[part, 16 * k : 16 * k + 16, :] for part in range(parts)],
                below[k],
                rest_below.get(k, nothing),
            ],
            axis=0,
        )
        from_right = pltpu.roll(right, 128 - STRIP * k, 1) if k else right
        from_left = pltpu.roll(left, 128 - STRIP * (k + 1), 1)
        return jnp.concatenate([whole, jnp.where(half, from_right, from_left)], axis=1)

    later = extended(TERMINAL)
    center = extended(DIAGONAL) + (inv_step + 4.0)
    rhs = inv_step * later - hamiltonian(later) + coupling * extended(GUESS + 1)
    vs = basis(keep(rhs), center, keep)
    for k in range(3):
        basis_ref[k] = vs[k]
    center_ref[...] = center
    guess_ref[...] = extended(GUESS)
    initial_ref[...] = inner(extended(INITIAL))
    mine = [middle(v, x, own) for v in vs]
    sums_ref[...] = row_of([(k, dot(mine[i], mine[j])) for k, (i, j) in enumerate(PAIRS)])


def second_kernel(grid, parts_ref, last_ref, center_ref, guess_ref, later_ref, basis_ref, inner_center, sums_ref):
    _, _, x, own = grid
    rows, wide = last_ref.shape[1:]
    keep = keeper(HALO, x, own)
    row = gathered_products(parts_ref)
    coefs = coefficients([entry(row, k) for k in range(len(PAIRS))])
    later = combined(coefs, [last_ref[k] for k in range(3)])
    later_ref[...] = inner(later)
    center = center_ref[...]
    inner_center[...] = inner(center)
    rhs = inv_step * later - hamiltonian(later) + coupling * guess_ref[...]
    vs = basis(keep(rhs), center, keep)
    for k in range(3):
        basis_ref[k] = inner(vs[k])
    mine = [middle(v, x, own) for v in vs]
    sums_ref[...] = row_of([(k, dot(mine[i], mine[j])) for k, (i, j) in enumerate(PAIRS)])


def third_kernel(grid, parts_ref, last_ref, center_ref, initial_ref, later_ref, value_ref, images_ref, sums_ref):
    _, _, x, own = grid
    rows, wide = last_ref.shape[1:]
    keep = keeper(INNER, x, own)
    row = gathered_products(parts_ref)
    coefs = coefficients([entry(row, k) for k in range(len(PAIRS))])
    value = combined(coefs, [last_ref[k] for k in range(3)])
    value_ref[...] = middle(value, x, own)
    center = center_ref[...]
    firsts = basis(density_rhs(initial_ref[...], drift(value), keep), center, keep)
    mine = [middle(v, x, own) for v in firsts]
    values = [(6 * 8 + k, dot(mine[i], mine[j])) for k, (i, j) in enumerate(PAIRS)]
    speeds = drift(later_ref[...])
    images = []
    for v in firsts[:3]:
        chain = basis(density_rhs(v, speeds, keep), center, keep)
        images.append([middle(w, x, own) for w in chain])
    for i in range(3):
        for k in range(3):
            images_ref[3 * i + k] = images[i][k]
    for place, (a, b) in enumerate(MIXED):
        for k, (i, j) in enumerate(PAIRS):
            values.append((8 * place + k, dot(images[a][i], images[b][j])))
    sums_ref[...] = row_of(values)


def fourth_kernel(parts_ref, images_ref, value_ref, value_out, density_ref):
    x = value_out.shape[0]
    mine = pl.ds(pl.multiple_of(lax.axis_index(PART) * x, x), x)
    value_out[...] = value_ref[mine, :]
    row = gathered_products(parts_ref)
    first = coefficients([entry(row, 6 * 8 + k) for k in range(len(PAIRS))])
    products = []
    for k in range(len(PAIRS)):
        total = None
        for place, (a, b) in enumerate(MIXED):
            term = first[a] * first[b] * entry(row, 8 * place + k)
            term = term if a == b else 2.0 * term
            total = term if total is None else total + term
        products.append(total)
    second = coefficients(products)
    total = None
    for i in range(3):
        for k in range(3):
            term = (first[i] * second[k]) * images_ref[3 * i + k, mine, :]
            total = term if total is None else total + term
    density_ref[...] = total


def everywhere(row):
    axes = (*BAND, *GY)
    size = lax.axis_size(axes)
    copies = jnp.broadcast_to(row, (size, 1, 128))
    return lax.all_to_all(copies, axes, split_axis=0, concat_axis=0, tiled=True).reshape(size, 128)


def swapped(far, near, axis):
    peers = lax.axis_size(axis)
    pairs = [(i, i + 1) for i in range(1, peers - 1, 2)]
    return (
        lax.ppermute(far, axis, pairs + [(b, a) for a, b in pairs]),
        lax.all_gather(near, axis[-1], tiled=True),
    )


def call(kernel, out_shape, *args, results=pltpu.VMEM):
    vmem = pl.BlockSpec(memory_space=pltpu.VMEM)
    return pl.pallas_call(
        kernel,
        out_shape=[results(s, jnp.float32) for s in out_shape],
        in_specs=[vmem] * len(args),
        out_specs=[vmem] * len(out_shape),
        compiler_params=pltpu.CompilerParams(vmem_limit_bytes=VMEM_LIMIT),
    )(*[pltpu.with_memory_space_constraint(a, pltpu.VMEM) for a in args])


def shards(terminal, initial_density, density_guess, diagonal):
    x, own = terminal.shape
    band = x * lax.axis_size(PART)
    grid = (x * lax.axis_size(GX), own * lax.axis_size(GY), band, own)
    fields, far, near = pl.pallas_call(
        stack_kernel,
        out_shape=[pltpu.VMEM(s, jnp.float32) for s in [(FIELDS, x, own), (x, EDGE), (x, EDGE)]],
        in_specs=[pl.BlockSpec(memory_space=pltpu.HBM)] * 4,
        out_specs=[pl.BlockSpec(memory_space=pltpu.VMEM)] * 3,
        scratch_shapes=[pltpu.SemaphoreType.DMA((4,))],
    )(terminal, diagonal, density_guess, initial_density)
    (block,) = call(edge_kernel, [(x * FIELDS + 8, own)], fields, *swapped(far, near, GY))
    whole = lax.all_gather(block, PART)
    packed = (8 * SENT, own)
    far, near = call(row_kernel, [packed, packed], whole)
    rows = band + 2 * HALO
    wide = own + EDGE
    full, fewer = (rows, wide), (band + 2 * INNER, wide)
    basis1, center, guess, initial, sums = call(
        functools.partial(first_kernel, grid),
        [(3, *full), full, full, fewer, (1, 128)],
        whole, *swapped(far, near, BAND),
    )
    later, basis0, center, sums = call(
        functools.partial(second_kernel, grid),
        [fewer, (3, *fewer), fewer, (1, 128)],
        everywhere(sums), basis1, center, guess,
    )
    value, images, sums = call(
        functools.partial(third_kernel, grid),
        [(band, own), (9, band, own), (1, 128)],
        everywhere(sums), basis0, center, initial, later,
    )
    return tuple(
        call(
            fourth_kernel, [(x, own)] * 2, everywhere(sums), images, value,
            results=jax.ShapeDtypeStruct,
        )
    )


def solution(mesh):
    torus = Mesh(mesh.devices.reshape(4, 2, 4, 8, 2), GX + GY)
    in_specs = (P(GX, GY), P(GX, GY), P(None, GX, GY), P(GX, GY))
    out_specs = (P(GX, GY), P(GX, GY))
    return jax.shard_map(
        shards, mesh=torus, in_specs=in_specs, out_specs=out_specs, check_vma=False
    )
```

```python
import functools

import jax
import jax.numpy as jnp
from jax import lax
from jax.experimental import pallas as pl
from jax.experimental.pallas import tpu as pltpu
from jax.sharding import Mesh
from jax.sharding import PartitionSpec as P

BAND = ("band_0", "band_1")
PART = "part"
GX = (*BAND, PART)
GY = ("gy_0", "gy_1")

inv_step = 0.5
coupling = 0.5

LOW = 0.6
HIGH = 10.5
S1 = 3.5
S2 = 5.5
S3 = 4.0
PAIRS = ((0, 0), (0, 1), (1, 1), (1, 2), (2, 2), (2, 3))
MIXED = ((0, 0), (1, 1), (2, 2), (0, 1), (0, 2), (1, 2))

HALF = 64
EDGE = 128
TERMINAL, DIAGONAL, GUESS, INITIAL = 0, 1, 2, 4
FIELDS = 5
SENT = FIELDS + 3
VMEM_LIMIT = 24 * 2**20
STRIP = 16
HALO = 16
INNER = 8


def before(v, dim):
    return pltpu.roll(v, 1, dim)


def after(v, dim):
    return pltpu.roll(v, v.shape[dim] - 1, dim)


def keeper(halo, x, own):
    band, column = lax.axis_index(BAND), lax.axis_index(GY)
    bands, columns = lax.axis_size(BAND), lax.axis_size(GY)
    top = jnp.where(band > 0, 1.0, 0.0)
    bottom = jnp.where(band < bands - 1, 1.0, 0.0)
    lane = lax.broadcasted_iota(jnp.int32, (8, EDGE), 1)
    edge = jnp.where(
        lane < HALF, jnp.where(column < columns - 1, 1.0, 0.0), jnp.where(column > 0, 1.0, 0.0)
    )

    def tiled(rows):
        return jnp.concatenate([edge] * (rows // 8), axis=0)

    ends = tiled(halo)

    def keep(v):
        first, last = v[:halo], v[halo + x :]
        inner_rows = v[halo : halo + x]
        main = [first[:, :own] * top, inner_rows[:, :own], last[:, :own] * bottom]
        side = [
            first[:, own:] * (ends * top),
            inner_rows[:, own:] * tiled(x),
            last[:, own:] * (ends * bottom),
        ]
        return jnp.concatenate([jnp.concatenate(p, axis=0) for p in (main, side)], axis=1)

    return keep


def shifted(v, center, shift, keep):
    beside = (before(v, 0) + after(v, 0)) + (before(v, 1) + after(v, 1))
    return keep((center - shift) * v - beside)


def basis(v0, center, keep):
    v1 = shifted(v0, center, S1, keep)
    v2 = shifted(v1, center, S2, keep)
    return [v0, v1, v2, shifted(v2, center, S3, keep)]


def hamiltonian(u):
    ahead_x = after(u, 0) - u
    back_x = u - before(u, 0)
    ahead_y = after(u, 1) - u
    back_y = u - before(u, 1)
    return 0.5 * (
        jnp.maximum(back_x, 0.0) ** 2
        + jnp.minimum(ahead_x, 0.0) ** 2
        + jnp.maximum(back_y, 0.0) ** 2
        + jnp.minimum(ahead_y, 0.0) ** 2
    )


def drift(u):
    speed_x = u - after(u, 0)
    speed_y = u - after(u, 1)
    return (
        jnp.maximum(speed_x, 0.0),
        jnp.minimum(speed_x, 0.0),
        jnp.maximum(speed_y, 0.0),
        jnp.minimum(speed_y, 0.0),
    )


def density_rhs(m, speeds, keep):
    out_x, in_x, out_y, in_y = speeds
    flux_x = out_x * m + in_x * after(m, 0)
    flux_y = out_y * m + in_y * after(m, 1)
    div = (flux_x - before(flux_x, 0)) + (flux_y - before(flux_y, 1))
    return keep(inv_step * m - div)


def dot(a, b):
    rows, wide = a.shape
    total = jnp.sum((a * b).reshape(rows // 8, 8, wide), axis=0)
    total = sum(total[:, k : k + 128] for k in range(128, wide, 128)) + total[:, :128]
    return jnp.sum(jnp.sum(total, axis=1, keepdims=True), axis=0, keepdims=True)


def row_of(values):
    lane = lax.broadcasted_iota(jnp.int32, (1, 128), 1)
    row = jnp.zeros((1, 128), jnp.float32)
    for place, value in values:
        row = jnp.where(lane == place, value, row)
    return row


def entry(row, place):
    lane = lax.broadcasted_iota(jnp.int32, row.shape, 1)
    return jnp.sum(jnp.where(lane == place, row, 0.0), axis=1, keepdims=True)


def form(matrix, vector):
    total = None
    for i, a in enumerate(vector):
        for j, b in enumerate(vector[: i + 1]):
            term = a * b * matrix[j][i]
            term = term if i == j else 2.0 * term
            total = term if total is None else total + term
    return total


def alpha_of(squared, energy):
    return jnp.clip(squared / jnp.maximum(energy, 1e-36), 0.999 / HIGH, 1.001 / LOW)


def beta_of(new, old):
    return jnp.clip(new / jnp.maximum(old, 1e-36), 0.0, 1.001 * HIGH / LOW)


def coefficients(products):
    g = dict(zip(PAIRS, products))
    g[0, 2] = g[1, 1] + (S1 - S2) * g[0, 1]
    gram = [[g[0, 0], g[0, 1], g[0, 2]], [None, g[1, 1], g[1, 2]], [None, None, g[2, 2]]]
    energy = [
        [g[0, 1] + S1 * g[0, 0], g[1, 1] + S1 * g[0, 1], g[1, 2] + S1 * g[0, 2]],
        [None, g[1, 2] + S2 * g[1, 1], g[2, 2] + S2 * g[1, 2]],
        [None, None, g[2, 3] + S3 * g[2, 2]],
    ]
    norm0 = g[0, 0]
    alpha0 = alpha_of(norm0, energy[0][0])
    resid1 = (1.0 - alpha0 * S1, -alpha0)
    norm1 = jnp.maximum(form(gram, resid1), 0.0)
    beta0 = beta_of(norm1, norm0)
    direct1 = (resid1[0] + beta0, resid1[1])
    alpha1 = alpha_of(norm1, form(energy, direct1))
    resid2 = (
        resid1[0] - alpha1 * (S1 * direct1[0]),
        resid1[1] - alpha1 * (direct1[0] + S2 * direct1[1]),
        -alpha1 * direct1[1],
    )
    norm2 = jnp.maximum(form(gram, resid2), 0.0)
    beta1 = beta_of(norm2, norm1)
    direct2 = (resid2[0] + beta1 * direct1[0], resid2[1] + beta1 * direct1[1], resid2[2])
    alpha2 = alpha_of(norm2, form(energy, direct2))
    return (
        alpha0 + alpha1 * direct1[0] + alpha2 * direct2[0],
        alpha1 * direct1[1] + alpha2 * direct2[1],
        alpha2 * direct2[2],
    )


def combined(coefs, vectors):
    total = coefs[0] * vectors[0]
    for c, v in zip(coefs[1:], vectors[1:]):
        total = total + c * v
    return total


def middle(v, x, own):
    return v[(v.shape[0] - x) // 2 : (v.shape[0] + x) // 2, :own]


def inner(v):
    return v[HALO - INNER : v.shape[0] - (HALO - INNER)]


def gathered_products(parts_ref):
    return jnp.sum(parts_ref[...], axis=0, keepdims=True)


def odd_index(axis, shape):
    place = lax.rem(lax.axis_index(axis), 2)
    return (lax.broadcasted_iota(jnp.int32, shape, 0) * 0 + place) == 1


def stack_kernel(terminal, diagonal, guess, initial, fields_ref, far_edge, near_edge, sems):
    copies = [
        pltpu.make_async_copy(terminal, fields_ref.at[TERMINAL], sems.at[0]),
        pltpu.make_async_copy(diagonal, fields_ref.at[DIAGONAL], sems.at[1]),
        pltpu.make_async_copy(guess, fields_ref.at[pl.ds(GUESS, 2)], sems.at[2]),
        pltpu.make_async_copy(initial, fields_ref.at[INITIAL], sems.at[3]),
    ]
    for copy in copies:
        copy.start()
    for copy in copies:
        copy.wait()
    _, x, own = fields_ref.shape
    shape = (x, 128)
    strip = lax.broadcasted_iota(jnp.int32, shape, 1) // STRIP
    firsts = lasts = jnp.zeros(shape, jnp.float32)
    for k in range(FIELDS):
        first, last = fields_ref[k, :, :128], fields_ref[k, :, own - 128 :]
        firsts = jnp.where(strip == k, pltpu.roll(first, STRIP * k, 1) if k else first, firsts)
        lasts = jnp.where(strip == k, pltpu.roll(last, STRIP * (k + 1), 1), lasts)
    odd = odd_index(GY, shape)
    far_edge[...] = jnp.where(odd, lasts, firsts)
    near_edge[...] = jnp.where(odd, firsts, lasts)


def edge_kernel(fields_ref, far_edge, near_edge, block_ref):
    _, x, own = fields_ref.shape
    odd = odd_index(GY, (x, EDGE))
    left = jnp.where(odd, near_edge[:x, :], far_edge[...])
    right = jnp.where(odd, far_edge[...], near_edge[x:, :])
    edges = jnp.concatenate([right[:8], left[:8], right[8:], left[8:]], axis=1)
    for part in range(block_ref.shape[0]):
        for k in range(FIELDS):
            block_ref[part, x * k : x * (k + 1), :] = fields_ref[k]
        block_ref[part, x * FIELDS :, :] = edges


def row_kernel(band_ref, far_ref, near_ref):
    parts, _, own = band_ref.shape
    shape = (8, own)
    row = lax.broadcasted_iota(jnp.int32, shape, 0)

    def halves(part):
        tiles = [band_ref[part, 8 * k : 8 * k + 8, :] for k in range(2 * FIELDS + 1)]
        return tiles[: 2 * FIELDS : 2], tiles[1 : 2 * FIELDS : 2], tiles[2 * FIELDS]

    first, second, edge = halves(0)
    top = first + [
        jnp.where(row < 5, second[TERMINAL], pltpu.roll(second[DIAGONAL], 5, 0)),
        jnp.where(row < 4, second[GUESS + 1], pltpu.roll(second[GUESS], 4, 0)),
        edge,
    ]
    first, second, edge = halves(parts - 1)
    bottom = second + [
        jnp.where(row >= 3, first[TERMINAL], pltpu.roll(first[DIAGONAL], 3, 0)),
        jnp.where(row >= 4, first[GUESS + 1], pltpu.roll(first[GUESS], 4, 0)),
        edge,
    ]
    odd = odd_index(BAND, shape)
    for k, (t, b) in enumerate(zip(top, bottom)):
        far_ref[8 * k : 8 * k + 8, :] = jnp.where(odd, b, t)
        near_ref[8 * k : 8 * k + 8, :] = jnp.where(odd, t, b)


def first_kernel(grid, band_ref, far_ref, near_ref, basis_ref, center_ref, guess_ref, initial_ref, sums_ref):
    _, _, x, own = grid
    wide = own + EDGE
    rows = x + 2 * HALO
    parts = band_ref.shape[0]
    keep = keeper(HALO, x, own)
    odd = odd_index(BAND, (8, own))

    def tile(k, odd_from, odd_start, even_from, even_start):
        odd_tile = odd_from[8 * (odd_start + k) : 8 * (odd_start + k) + 8, :]
        return jnp.where(odd, odd_tile, even_from[8 * (even_start + k) : 8 * (even_start + k) + 8, :])

    above = [tile(k, near_ref, 0, far_ref, 0) for k in range(SENT)]
    below = [tile(k, far_ref, 0, near_ref, SENT) for k in range(SENT)]
    rest_above = {
        TERMINAL: above[FIELDS],
        DIAGONAL: pltpu.roll(above[FIELDS], 5, 0),
        GUESS + 1: above[FIELDS + 1],
        GUESS: pltpu.roll(above[FIELDS + 1], 4, 0),
    }
    rest_below = {
        TERMINAL: below[FIELDS],
        DIAGONAL: pltpu.roll(below[FIELDS], 3, 0),
        GUESS + 1: below[FIELDS + 1],
        GUESS: pltpu.roll(below[FIELDS + 1], 4, 0),
    }
    nothing = jnp.zeros((8, own), jnp.float32)
    blocks = [above[-1], *[band_ref[part, 2 * 8 * FIELDS :, :] for part in range(parts)], below[-1]]
    right, left = (
        jnp.concatenate([b[:, at : at + 128] for b in blocks for at in (start, start + 256)], axis=0)
        for start in (0, 128)
    )
    half = lax.broadcasted_iota(jnp.int32, (rows, EDGE), 1) < HALF

    def extended(k):
        whole = jnp.concatenate(
            [
                rest_above.get(k, nothing),
                above[k],
                *[band_ref[part, 16 * k : 16 * k + 16, :] for part in range(parts)],
                below[k],
                rest_below.get(k, nothing),
            ],
            axis=0,
        )
        from_right = pltpu.roll(right, 128 - STRIP * k, 1) if k else right
        from_left = pltpu.roll(left, 128 - STRIP * (k + 1), 1)
        return jnp.concatenate([whole, jnp.where(half, from_right, from_left)], axis=1)

    later = extended(TERMINAL)
    center = extended(DIAGONAL) + (inv_step + 4.0)
    rhs = inv_step * later - hamiltonian(later) + coupling * extended(GUESS + 1)
    vs = basis(keep(rhs), center, keep)
    for k in range(3):
        basis_ref[k] = vs[k]
    center_ref[...] = center
    guess_ref[...] = extended(GUESS)
    initial_ref[...] = inner(extended(INITIAL))
    mine = [middle(v, x, own) for v in vs]
    sums_ref[...] = row_of([(k, dot(mine[i], mine[j])) for k, (i, j) in enumerate(PAIRS)])


def second_kernel(grid, parts_ref, last_ref, center_ref, guess_ref, later_ref, basis_ref, inner_center, sums_ref):
    _, _, x, own = grid
    rows, wide = last_ref.shape[1:]
    keep = keeper(HALO, x, own)
    row = gathered_products(parts_ref)
    coefs = coefficients([entry(row, k) for k in range(len(PAIRS))])
    later = combined(coefs, [last_ref[k] for k in range(3)])
    later_ref[...] = inner(later)
    center = center_ref[...]
    inner_center[...] = inner(center)
    rhs = inv_step * later - hamiltonian(later) + coupling * guess_ref[...]
    vs = basis(keep(rhs), center, keep)
    for k in range(3):
        basis_ref[k] = inner(vs[k])
    mine = [middle(v, x, own) for v in vs]
    sums_ref[...] = row_of([(k, dot(mine[i], mine[j])) for k, (i, j) in enumerate(PAIRS)])


def third_kernel(grid, parts_ref, last_ref, center_ref, initial_ref, later_ref, value_ref, images_ref, sums_ref):
    _, _, x, own = grid
    rows, wide = last_ref.shape[1:]
    keep = keeper(INNER, x, own)
    row = gathered_products(parts_ref)
    coefs = coefficients([entry(row, k) for k in range(len(PAIRS))])
    value = combined(coefs, [last_ref[k] for k in range(3)])
    value_ref[...] = middle(value, x, own)
    center = center_ref[...]
    firsts = basis(density_rhs(initial_ref[...], drift(value), keep), center, keep)
    mine = [middle(v, x, own) for v in firsts]
    values = [(6 * 8 + k, dot(mine[i], mine[j])) for k, (i, j) in enumerate(PAIRS)]
    speeds = drift(later_ref[...])
    images = []
    for v in firsts[:3]:
        chain = basis(density_rhs(v, speeds, keep), center, keep)
        images.append([middle(w, x, own) for w in chain])
    for i in range(3):
        for k in range(3):
            images_ref[3 * i + k] = images[i][k]
    for place, (a, b) in enumerate(MIXED):
        for k, (i, j) in enumerate(PAIRS):
            values.append((8 * place + k, dot(images[a][i], images[b][j])))
    sums_ref[...] = row_of(values)


def fourth_kernel(parts_ref, images_ref, value_ref, value_out, density_ref):
    x = value_out.shape[0]
    mine = pl.ds(pl.multiple_of(lax.axis_index(PART) * x, x), x)
    value_out[...] = value_ref[mine, :]
    row = gathered_products(parts_ref)
    first = coefficients([entry(row, 6 * 8 + k) for k in range(len(PAIRS))])
    products = []
    for k in range(len(PAIRS)):
        total = None
        for place, (a, b) in enumerate(MIXED):
            term = first[a] * first[b] * entry(row, 8 * place + k)
            term = term if a == b else 2.0 * term
            total = term if total is None else total + term
        products.append(total)
    second = coefficients(products)
    total = None
    for i in range(3):
        for k in range(3):
            term = (first[i] * second[k]) * images_ref[3 * i + k, mine, :]
            total = term if total is None else total + term
    density_ref[...] = total


def everywhere(row):
    axes = (*BAND, *GY)
    size = lax.axis_size(axes)
    copies = jnp.broadcast_to(row, (size, 1, 128))
    return lax.all_to_all(copies, axes, split_axis=0, concat_axis=0, tiled=True).reshape(size, 128)


def swapped(far, near, axis):
    peers = lax.axis_size(axis)
    pairs = [(i, i + 1) for i in range(1, peers - 1, 2)]
    return (
        lax.ppermute(far, axis, pairs + [(b, a) for a, b in pairs]),
        lax.all_gather(near, axis[-1], tiled=True),
    )


def call(kernel, out_shape, *args, results=pltpu.VMEM):
    vmem = pl.BlockSpec(memory_space=pltpu.VMEM)
    return pl.pallas_call(
        kernel,
        out_shape=[results(s, jnp.float32) for s in out_shape],
        in_specs=[vmem] * len(args),
        out_specs=[vmem] * len(out_shape),
        compiler_params=pltpu.CompilerParams(vmem_limit_bytes=VMEM_LIMIT),
    )(*[pltpu.with_memory_space_constraint(a, pltpu.VMEM) for a in args])


def shards(terminal, initial_density, density_guess, diagonal):
    x, own = terminal.shape
    band = x * lax.axis_size(PART)
    grid = (x * lax.axis_size(GX), own * lax.axis_size(GY), band, own)
    fields, far, near = pl.pallas_call(
        stack_kernel,
        out_shape=[pltpu.VMEM(s, jnp.float32) for s in [(FIELDS, x, own), (x, EDGE), (x, EDGE)]],
        in_specs=[pl.BlockSpec(memory_space=pltpu.HBM)] * 4,
        out_specs=[pl.BlockSpec(memory_space=pltpu.VMEM)] * 3,
        scratch_shapes=[pltpu.SemaphoreType.DMA((4,))],
    )(terminal, diagonal, density_guess, initial_density)
    copies = (lax.axis_size(PART), x * FIELDS + 8, own)
    (blocks,) = call(edge_kernel, [copies], fields, *swapped(far, near, GY))
    whole = lax.all_to_all(blocks, PART, split_axis=0, concat_axis=0, tiled=True)
    packed = (8 * SENT, own)
    far, near = call(row_kernel, [packed, packed], whole)
    rows = band + 2 * HALO
    wide = own + EDGE
    full, fewer = (rows, wide), (band + 2 * INNER, wide)
    basis1, center, guess, initial, sums = call(
        functools.partial(first_kernel, grid),
        [(3, *full), full, full, fewer, (1, 128)],
        whole, *swapped(far, near, BAND),
    )
    later, basis0, center, sums = call(
        functools.partial(second_kernel, grid),
        [fewer, (3, *fewer), fewer, (1, 128)],
        everywhere(sums), basis1, center, guess,
    )
    value, images, sums = call(
        functools.partial(third_kernel, grid),
        [(band, own), (9, band, own), (1, 128)],
        everywhere(sums), basis0, center, initial, later,
    )
    return tuple(
        call(
            fourth_kernel, [(x, own)] * 2, everywhere(sums), images, value,
            results=jax.ShapeDtypeStruct,
        )
    )


def solution(mesh):
    torus = Mesh(mesh.devices.reshape(4, 2, 4, 8, 2), GX + GY)
    in_specs = (P(GX, GY), P(GX, GY), P(None, GX, GY), P(GX, GY))
    out_specs = (P(GX, GY), P(GX, GY))
    return jax.shard_map(
        shards, mesh=torus, in_specs=in_specs, out_specs=out_specs, check_vma=False
    )
```

```python
import functools

import jax
import jax.numpy as jnp
from jax import lax
from jax.experimental import pallas as pl
from jax.experimental.pallas import tpu as pltpu
from jax.sharding import Mesh
from jax.sharding import PartitionSpec as P

BAND = ("band_0", "band_1")
PART = "part"
GX = (*BAND, PART)
GY = ("gy_0", "gy_1")

inv_step = 0.5
coupling = 0.5

LOW = 0.6
HIGH = 10.5
S1 = 3.5
S2 = 5.5
S3 = 4.0
PAIRS = ((0, 0), (0, 1), (1, 1), (1, 2), (2, 2), (2, 3))
MIXED = ((0, 0), (1, 1), (2, 2), (0, 1), (0, 2), (1, 2))

HALF = 64
EDGE = 128
TERMINAL, DIAGONAL, GUESS, INITIAL = 0, 1, 2, 4
FIELDS = 5
SENT = FIELDS + 3
VMEM_LIMIT = 24 * 2**20
STRIP = 16
HALO = 16
INNER = 8


def before(v, dim):
    return pltpu.roll(v, 1, dim)


def after(v, dim):
    return pltpu.roll(v, v.shape[dim] - 1, dim)


def keeper(halo, x, own):
    band, column = lax.axis_index(BAND), lax.axis_index(GY)
    bands, columns = lax.axis_size(BAND), lax.axis_size(GY)
    top = jnp.where(band > 0, 1.0, 0.0)
    bottom = jnp.where(band < bands - 1, 1.0, 0.0)
    lane = lax.broadcasted_iota(jnp.int32, (8, EDGE), 1)
    edge = jnp.where(
        lane < HALF, jnp.where(column < columns - 1, 1.0, 0.0), jnp.where(column > 0, 1.0, 0.0)
    )

    def tiled(rows):
        return jnp.concatenate([edge] * (rows // 8), axis=0)

    ends = tiled(halo)

    def keep(v):
        first, last = v[:halo], v[halo + x :]
        inner_rows = v[halo : halo + x]
        main = [first[:, :own] * top, inner_rows[:, :own], last[:, :own] * bottom]
        side = [
            first[:, own:] * (ends * top),
            inner_rows[:, own:] * tiled(x),
            last[:, own:] * (ends * bottom),
        ]
        return jnp.concatenate([jnp.concatenate(p, axis=0) for p in (main, side)], axis=1)

    return keep


def shifted(v, center, shift, keep):
    beside = (before(v, 0) + after(v, 0)) + (before(v, 1) + after(v, 1))
    return keep((center - shift) * v - beside)


def basis(v0, center, keep):
    v1 = shifted(v0, center, S1, keep)
    v2 = shifted(v1, center, S2, keep)
    return [v0, v1, v2, shifted(v2, center, S3, keep)]


def hamiltonian(u):
    ahead_x = after(u, 0) - u
    back_x = u - before(u, 0)
    ahead_y = after(u, 1) - u
    back_y = u - before(u, 1)
    return 0.5 * (
        jnp.maximum(back_x, 0.0) ** 2
        + jnp.minimum(ahead_x, 0.0) ** 2
        + jnp.maximum(back_y, 0.0) ** 2
        + jnp.minimum(ahead_y, 0.0) ** 2
    )


def drift(u):
    speed_x = u - after(u, 0)
    speed_y = u - after(u, 1)
    return (
        jnp.maximum(speed_x, 0.0),
        jnp.minimum(speed_x, 0.0),
        jnp.maximum(speed_y, 0.0),
        jnp.minimum(speed_y, 0.0),
    )


def density_rhs(m, speeds, keep):
    out_x, in_x, out_y, in_y = speeds
    flux_x = out_x * m + in_x * after(m, 0)
    flux_y = out_y * m + in_y * after(m, 1)
    div = (flux_x - before(flux_x, 0)) + (flux_y - before(flux_y, 1))
    return keep(inv_step * m - div)


def dot(a, b):
    rows, wide = a.shape
    total = jnp.sum((a * b).reshape(rows // 8, 8, wide), axis=0)
    total = sum(total[:, k : k + 128] for k in range(128, wide, 128)) + total[:, :128]
    return jnp.sum(jnp.sum(total, axis=1, keepdims=True), axis=0, keepdims=True)


def row_of(values):
    lane = lax.broadcasted_iota(jnp.int32, (1, 128), 1)
    row = jnp.zeros((1, 128), jnp.float32)
    for place, value in values:
        row = jnp.where(lane == place, value, row)
    return row


def entry(row, place):
    lane = lax.broadcasted_iota(jnp.int32, row.shape, 1)
    return jnp.sum(jnp.where(lane == place, row, 0.0), axis=1, keepdims=True)


def form(matrix, vector):
    total = None
    for i, a in enumerate(vector):
        for j, b in enumerate(vector[: i + 1]):
            term = a * b * matrix[j][i]
            term = term if i == j else 2.0 * term
            total = term if total is None else total + term
    return total


def alpha_of(squared, energy):
    return jnp.clip(squared / jnp.maximum(energy, 1e-36), 0.999 / HIGH, 1.001 / LOW)


def beta_of(new, old):
    return jnp.clip(new / jnp.maximum(old, 1e-36), 0.0, 1.001 * HIGH / LOW)


def coefficients(products):
    g = dict(zip(PAIRS, products))
    g[0, 2] = g[1, 1] + (S1 - S2) * g[0, 1]
    gram = [[g[0, 0], g[0, 1], g[0, 2]], [None, g[1, 1], g[1, 2]], [None, None, g[2, 2]]]
    energy = [
        [g[0, 1] + S1 * g[0, 0], g[1, 1] + S1 * g[0, 1], g[1, 2] + S1 * g[0, 2]],
        [None, g[1, 2] + S2 * g[1, 1], g[2, 2] + S2 * g[1, 2]],
        [None, None, g[2, 3] + S3 * g[2, 2]],
    ]
    norm0 = g[0, 0]
    alpha0 = alpha_of(norm0, energy[0][0])
    resid1 = (1.0 - alpha0 * S1, -alpha0)
    norm1 = jnp.maximum(form(gram, resid1), 0.0)
    beta0 = beta_of(norm1, norm0)
    direct1 = (resid1[0] + beta0, resid1[1])
    alpha1 = alpha_of(norm1, form(energy, direct1))
    resid2 = (
        resid1[0] - alpha1 * (S1 * direct1[0]),
        resid1[1] - alpha1 * (direct1[0] + S2 * direct1[1]),
        -alpha1 * direct1[1],
    )
    norm2 = jnp.maximum(form(gram, resid2), 0.0)
    beta1 = beta_of(norm2, norm1)
    direct2 = (resid2[0] + beta1 * direct1[0], resid2[1] + beta1 * direct1[1], resid2[2])
    alpha2 = alpha_of(norm2, form(energy, direct2))
    return (
        alpha0 + alpha1 * direct1[0] + alpha2 * direct2[0],
        alpha1 * direct1[1] + alpha2 * direct2[1],
        alpha2 * direct2[2],
    )


def combined(coefs, vectors):
    total = coefs[0] * vectors[0]
    for c, v in zip(coefs[1:], vectors[1:]):
        total = total + c * v
    return total


def middle(v, x, own):
    return v[(v.shape[0] - x) // 2 : (v.shape[0] + x) // 2, :own]


def inner(v):
    return v[HALO - INNER : v.shape[0] - (HALO - INNER)]


def gathered_products(parts_ref):
    return jnp.sum(parts_ref[...], axis=0, keepdims=True)


def odd_index(axis, shape):
    place = lax.rem(lax.axis_index(axis), 2)
    return (lax.broadcasted_iota(jnp.int32, shape, 0) * 0 + place) == 1


def stack_kernel(terminal, diagonal, guess, initial, fields_ref, far_edge, near_edge, sems):
    copies = [
        pltpu.make_async_copy(terminal, fields_ref.at[TERMINAL], sems.at[0]),
        pltpu.make_async_copy(diagonal, fields_ref.at[DIAGONAL], sems.at[1]),
        pltpu.make_async_copy(guess, fields_ref.at[pl.ds(GUESS, 2)], sems.at[2]),
        pltpu.make_async_copy(initial, fields_ref.at[INITIAL], sems.at[3]),
    ]
    for copy in copies:
        copy.start()
    for copy in copies:
        copy.wait()
    _, x, own = fields_ref.shape
    shape = (x, 128)
    strip = lax.broadcasted_iota(jnp.int32, shape, 1) // STRIP
    firsts = lasts = jnp.zeros(shape, jnp.float32)
    for k in range(FIELDS):
        first, last = fields_ref[k, :, :128], fields_ref[k, :, own - 128 :]
        firsts = jnp.where(strip == k, pltpu.roll(first, STRIP * k, 1) if k else first, firsts)
        lasts = jnp.where(strip == k, pltpu.roll(last, STRIP * (k + 1), 1), lasts)
    odd = odd_index(GY, shape)
    far_edge[...] = jnp.where(odd, lasts, firsts)
    near_edge[...] = jnp.where(odd, firsts, lasts)


def edge_kernel(fields_ref, far_edge, near_edge, block_ref):
    _, x, own = fields_ref.shape
    odd = odd_index(GY, (x, EDGE))
    left = jnp.where(odd, near_edge[:x, :], far_edge[...])
    right = jnp.where(odd, far_edge[...], near_edge[x:, :])
    for k in range(FIELDS):
        block_ref[2 * k] = fields_ref[k, :8, :]
        block_ref[2 * k + 1] = fields_ref[k, 8:, :]
    edges = [right[:8], left[:8], right[8:], left[8:]]
    block_ref[2 * FIELDS] = jnp.concatenate(edges, axis=1)


def row_kernel(band_ref, far_ref, near_ref):
    parts, _, own = band_ref.shape
    shape = (8, own)
    row = lax.broadcasted_iota(jnp.int32, shape, 0)

    def halves(part):
        tiles = [band_ref[part, 8 * k : 8 * k + 8, :] for k in range(2 * FIELDS + 1)]
        return tiles[: 2 * FIELDS : 2], tiles[1 : 2 * FIELDS : 2], tiles[2 * FIELDS]

    first, second, edge = halves(0)
    top = first + [
        jnp.where(row < 5, second[TERMINAL], pltpu.roll(second[DIAGONAL], 5, 0)),
        jnp.where(row < 4, second[GUESS + 1], pltpu.roll(second[GUESS], 4, 0)),
        edge,
    ]
    first, second, edge = halves(parts - 1)
    bottom = second + [
        jnp.where(row >= 3, first[TERMINAL], pltpu.roll(first[DIAGONAL], 3, 0)),
        jnp.where(row >= 4, first[GUESS + 1], pltpu.roll(first[GUESS], 4, 0)),
        edge,
    ]
    odd = odd_index(BAND, shape)
    for k, (t, b) in enumerate(zip(top, bottom)):
        far_ref[8 * k : 8 * k + 8, :] = jnp.where(odd, b, t)
        near_ref[8 * k : 8 * k + 8, :] = jnp.where(odd, t, b)


def first_kernel(grid, band_ref, far_ref, near_ref, basis_ref, center_ref, guess_ref, initial_ref, sums_ref):
    _, _, x, own = grid
    wide = own + EDGE
    rows = x + 2 * HALO
    parts = band_ref.shape[0]
    keep = keeper(HALO, x, own)
    odd = odd_index(BAND, (8, own))

    def tile(k, odd_from, odd_start, even_from, even_start):
        odd_tile = odd_from[8 * (odd_start + k) : 8 * (odd_start + k) + 8, :]
        return jnp.where(odd, odd_tile, even_from[8 * (even_start + k) : 8 * (even_start + k) + 8, :])

    above = [tile(k, near_ref, 0, far_ref, 0) for k in range(SENT)]
    below = [tile(k, far_ref, 0, near_ref, SENT) for k in range(SENT)]
    rest_above = {
        TERMINAL: above[FIELDS],
        DIAGONAL: pltpu.roll(above[FIELDS], 5, 0),
        GUESS + 1: above[FIELDS + 1],
        GUESS: pltpu.roll(above[FIELDS + 1], 4, 0),
    }
    rest_below = {
        TERMINAL: below[FIELDS],
        DIAGONAL: pltpu.roll(below[FIELDS], 3, 0),
        GUESS + 1: below[FIELDS + 1],
        GUESS: pltpu.roll(below[FIELDS + 1], 4, 0),
    }
    nothing = jnp.zeros((8, own), jnp.float32)
    blocks = [above[-1], *[band_ref[part, 2 * 8 * FIELDS :, :] for part in range(parts)], below[-1]]
    right, left = (
        jnp.concatenate([b[:, at : at + 128] for b in blocks for at in (start, start + 256)], axis=0)
        for start in (0, 128)
    )
    half = lax.broadcasted_iota(jnp.int32, (rows, EDGE), 1) < HALF

    def extended(k):
        whole = jnp.concatenate(
            [
                rest_above.get(k, nothing),
                above[k],
                *[band_ref[part, 16 * k : 16 * k + 16, :] for part in range(parts)],
                below[k],
                rest_below.get(k, nothing),
            ],
            axis=0,
        )
        from_right = pltpu.roll(right, 128 - STRIP * k, 1) if k else right
        from_left = pltpu.roll(left, 128 - STRIP * (k + 1), 1)
        return jnp.concatenate([whole, jnp.where(half, from_right, from_left)], axis=1)

    later = extended(TERMINAL)
    center = extended(DIAGONAL) + (inv_step + 4.0)
    rhs = inv_step * later - hamiltonian(later) + coupling * extended(GUESS + 1)
    vs = basis(keep(rhs), center, keep)
    for k in range(3):
        basis_ref[k] = vs[k]
    center_ref[...] = center
    guess_ref[...] = extended(GUESS)
    initial_ref[...] = inner(extended(INITIAL))
    mine = [middle(v, x, own) for v in vs]
    sums_ref[...] = row_of([(k, dot(mine[i], mine[j])) for k, (i, j) in enumerate(PAIRS)])


def second_kernel(grid, parts_ref, last_ref, center_ref, guess_ref, later_ref, basis_ref, inner_center, sums_ref):
    _, _, x, own = grid
    rows, wide = last_ref.shape[1:]
    keep = keeper(HALO, x, own)
    row = gathered_products(parts_ref)
    coefs = coefficients([entry(row, k) for k in range(len(PAIRS))])
    later = combined(coefs, [last_ref[k] for k in range(3)])
    later_ref[...] = inner(later)
    center = center_ref[...]
    inner_center[...] = inner(center)
    rhs = inv_step * later - hamiltonian(later) + coupling * guess_ref[...]
    vs = basis(keep(rhs), center, keep)
    for k in range(3):
        basis_ref[k] = inner(vs[k])
    mine = [middle(v, x, own) for v in vs]
    sums_ref[...] = row_of([(k, dot(mine[i], mine[j])) for k, (i, j) in enumerate(PAIRS)])


def third_kernel(grid, parts_ref, last_ref, center_ref, initial_ref, later_ref, value_ref, images_ref, sums_ref):
    _, _, x, own = grid
    rows, wide = last_ref.shape[1:]
    keep = keeper(INNER, x, own)
    row = gathered_products(parts_ref)
    coefs = coefficients([entry(row, k) for k in range(len(PAIRS))])
    value = combined(coefs, [last_ref[k] for k in range(3)])
    value_ref[...] = middle(value, x, own)
    center = center_ref[...]
    firsts = basis(density_rhs(initial_ref[...], drift(value), keep), center, keep)
    mine = [middle(v, x, own) for v in firsts]
    values = [(6 * 8 + k, dot(mine[i], mine[j])) for k, (i, j) in enumerate(PAIRS)]
    speeds = drift(later_ref[...])
    images = []
    for v in firsts[:3]:
        chain = basis(density_rhs(v, speeds, keep), center, keep)
        images.append([middle(w, x, own) for w in chain])
    for i in range(3):
        for k in range(3):
            images_ref[3 * i + k] = images[i][k]
    for place, (a, b) in enumerate(MIXED):
        for k, (i, j) in enumerate(PAIRS):
            values.append((8 * place + k, dot(images[a][i], images[b][j])))
    sums_ref[...] = row_of(values)


def fourth_kernel(parts_ref, images_ref, value_ref, value_out, density_ref):
    x = value_out.shape[0]
    mine = pl.ds(pl.multiple_of(lax.axis_index(PART) * x, x), x)
    value_out[...] = value_ref[mine, :]
    row = gathered_products(parts_ref)
    first = coefficients([entry(row, 6 * 8 + k) for k in range(len(PAIRS))])
    products = []
    for k in range(len(PAIRS)):
        total = None
        for place, (a, b) in enumerate(MIXED):
            term = first[a] * first[b] * entry(row, 8 * place + k)
            term = term if a == b else 2.0 * term
            total = term if total is None else total + term
        products.append(total)
    second = coefficients(products)
    total = None
    for i in range(3):
        for k in range(3):
            term = (first[i] * second[k]) * images_ref[3 * i + k, mine, :]
            total = term if total is None else total + term
    density_ref[...] = total


def everywhere(row):
    axes = (*BAND, *GY)
    size = lax.axis_size(axes)
    copies = jnp.broadcast_to(row, (size, 1, 128))
    return lax.all_to_all(copies, axes, split_axis=0, concat_axis=0, tiled=True).reshape(size, 128)


def swapped(far, near, axis):
    peers = lax.axis_size(axis)
    pairs = [(i, i + 1) for i in range(1, peers - 1, 2)]
    return (
        lax.ppermute(far, axis, pairs + [(b, a) for a, b in pairs]),
        lax.all_gather(near, axis[-1], tiled=True),
    )


def call(kernel, out_shape, *args, results=pltpu.VMEM):
    vmem = pl.BlockSpec(memory_space=pltpu.VMEM)
    return pl.pallas_call(
        kernel,
        out_shape=[results(s, jnp.float32) for s in out_shape],
        in_specs=[vmem] * len(args),
        out_specs=[vmem] * len(out_shape),
        compiler_params=pltpu.CompilerParams(vmem_limit_bytes=VMEM_LIMIT),
    )(*[pltpu.with_memory_space_constraint(a, pltpu.VMEM) for a in args])


def shards(terminal, initial_density, density_guess, diagonal):
    x, own = terminal.shape
    band = x * lax.axis_size(PART)
    grid = (x * lax.axis_size(GX), own * lax.axis_size(GY), band, own)
    fields, far, near = pl.pallas_call(
        stack_kernel,
        out_shape=[pltpu.VMEM(s, jnp.float32) for s in [(FIELDS, x, own), (x, EDGE), (x, EDGE)]],
        in_specs=[pl.BlockSpec(memory_space=pltpu.HBM)] * 4,
        out_specs=[pl.BlockSpec(memory_space=pltpu.VMEM)] * 3,
        scratch_shapes=[pltpu.SemaphoreType.DMA((4,))],
    )(terminal, diagonal, density_guess, initial_density)
    (block,) = call(edge_kernel, [(2 * FIELDS + 1, 8, own)], fields, *swapped(far, near, GY))
    whole = lax.all_gather(block, PART).reshape(-1, x * FIELDS + 8, own)
    packed = (8 * SENT, own)
    far, near = call(row_kernel, [packed, packed], whole)
    rows = band + 2 * HALO
    wide = own + EDGE
    full, fewer = (rows, wide), (band + 2 * INNER, wide)
    basis1, center, guess, initial, sums = call(
        functools.partial(first_kernel, grid),
        [(3, *full), full, full, fewer, (1, 128)],
        whole, *swapped(far, near, BAND),
    )
    later, basis0, center, sums = call(
        functools.partial(second_kernel, grid),
        [fewer, (3, *fewer), fewer, (1, 128)],
        everywhere(sums), basis1, center, guess,
    )
    value, images, sums = call(
        functools.partial(third_kernel, grid),
        [(band, own), (9, band, own), (1, 128)],
        everywhere(sums), basis0, center, initial, later,
    )
    return tuple(
        call(
            fourth_kernel, [(x, own)] * 2, everywhere(sums), images, value,
            results=jax.ShapeDtypeStruct,
        )
    )


def solution(mesh):
    torus = Mesh(mesh.devices.reshape(4, 2, 4, 8, 2), GX + GY)
    in_specs = (P(GX, GY), P(GX, GY), P(None, GX, GY), P(GX, GY))
    out_specs = (P(GX, GY), P(GX, GY))
    return jax.shard_map(
        shards, mesh=torus, in_specs=in_specs, out_specs=out_specs, check_vma=False
    )
```

```python
import functools

import jax
import jax.numpy as jnp
from jax import lax
from jax.experimental import pallas as pl
from jax.experimental.pallas import tpu as pltpu
from jax.sharding import Mesh
from jax.sharding import PartitionSpec as P

BAND = ("band_0", "band_1")
PART = "part"
GX = (*BAND, PART)
GY = ("gy_0", "gy_1")

inv_step = 0.5
coupling = 0.5

LOW = 0.6
HIGH = 10.5
S1 = 3.5
S2 = 5.5
S3 = 4.0
PAIRS = ((0, 0), (0, 1), (1, 1), (1, 2), (2, 2), (2, 3))
MIXED = ((0, 0), (1, 1), (2, 2), (0, 1), (0, 2), (1, 2))

HALF = 64
EDGE = 128
TERMINAL, DIAGONAL, GUESS, INITIAL = 0, 1, 2, 4
FIELDS = 5
SENT = FIELDS + 3
VMEM_LIMIT = 24 * 2**20
STRIP = 16
HALO = 16
INNER = 8


def before(v, dim):
    return pltpu.roll(v, 1, dim)


def after(v, dim):
    return pltpu.roll(v, v.shape[dim] - 1, dim)


def keeper(halo, x, own):
    band, column = lax.axis_index(BAND), lax.axis_index(GY)
    bands, columns = lax.axis_size(BAND), lax.axis_size(GY)
    top = jnp.where(band > 0, 1.0, 0.0)
    bottom = jnp.where(band < bands - 1, 1.0, 0.0)
    lane = lax.broadcasted_iota(jnp.int32, (8, EDGE), 1)
    edge = jnp.where(
        lane < HALF, jnp.where(column < columns - 1, 1.0, 0.0), jnp.where(column > 0, 1.0, 0.0)
    )

    def tiled(rows):
        return jnp.concatenate([edge] * (rows // 8), axis=0)

    ends = tiled(halo)

    def keep(v):
        first, last = v[:halo], v[halo + x :]
        inner_rows = v[halo : halo + x]
        main = [first[:, :own] * top, inner_rows[:, :own], last[:, :own] * bottom]
        side = [
            first[:, own:] * (ends * top),
            inner_rows[:, own:] * tiled(x),
            last[:, own:] * (ends * bottom),
        ]
        return jnp.concatenate([jnp.concatenate(p, axis=0) for p in (main, side)], axis=1)

    return keep


def shifted(v, center, shift, keep):
    beside = (before(v, 0) + after(v, 0)) + (before(v, 1) + after(v, 1))
    return keep((center - shift) * v - beside)


def basis(v0, center, keep):
    v1 = shifted(v0, center, S1, keep)
    v2 = shifted(v1, center, S2, keep)
    return [v0, v1, v2, shifted(v2, center, S3, keep)]


def hamiltonian(u):
    total = None
    for dim in (0, 1):
        ahead = after(u, dim) - u
        term = before(jnp.maximum(ahead, 0.0) ** 2, dim) + jnp.minimum(ahead, 0.0) ** 2
        total = term if total is None else total + term
    return 0.5 * total


def drift(u):
    speed_x = u - after(u, 0)
    speed_y = u - after(u, 1)
    return (
        jnp.maximum(speed_x, 0.0),
        jnp.minimum(speed_x, 0.0),
        jnp.maximum(speed_y, 0.0),
        jnp.minimum(speed_y, 0.0),
    )


def density_rhs(m, speeds, keep):
    out_x, in_x, out_y, in_y = speeds
    flux_x = out_x * m + in_x * after(m, 0)
    flux_y = out_y * m + in_y * after(m, 1)
    div = (flux_x - before(flux_x, 0)) + (flux_y - before(flux_y, 1))
    return keep(inv_step * m - div)


def dot(a, b):
    rows, wide = a.shape
    total = jnp.sum((a * b).reshape(rows // 8, 8, wide), axis=0)
    total = sum(total[:, k : k + 128] for k in range(128, wide, 128)) + total[:, :128]
    return jnp.sum(total, axis=1, keepdims=True)


def row_of(values):
    lane = lax.broadcasted_iota(jnp.int32, (8, 128), 1)
    rows = jnp.zeros((8, 128), jnp.float32)
    for place, value in values:
        rows = jnp.where(lane == place, value, rows)
    return jnp.sum(rows, axis=0, keepdims=True)


def entry(row, place):
    lane = lax.broadcasted_iota(jnp.int32, row.shape, 1)
    return jnp.sum(jnp.where(lane == place, row, 0.0), axis=1, keepdims=True)


def form(matrix, vector):
    total = None
    for i, a in enumerate(vector):
        for j, b in enumerate(vector[: i + 1]):
            term = a * b * matrix[j][i]
            term = term if i == j else 2.0 * term
            total = term if total is None else total + term
    return total


def alpha_of(squared, energy):
    return jnp.clip(squared / jnp.maximum(energy, 1e-36), 0.999 / HIGH, 1.001 / LOW)


def beta_of(new, old):
    return jnp.clip(new / jnp.maximum(old, 1e-36), 0.0, 1.001 * HIGH / LOW)


def coefficients(products):
    g = dict(zip(PAIRS, products))
    g[0, 2] = g[1, 1] + (S1 - S2) * g[0, 1]
    gram = [[g[0, 0], g[0, 1], g[0, 2]], [None, g[1, 1], g[1, 2]], [None, None, g[2, 2]]]
    energy = [
        [g[0, 1] + S1 * g[0, 0], g[1, 1] + S1 * g[0, 1], g[1, 2] + S1 * g[0, 2]],
        [None, g[1, 2] + S2 * g[1, 1], g[2, 2] + S2 * g[1, 2]],
        [None, None, g[2, 3] + S3 * g[2, 2]],
    ]
    norm0 = g[0, 0]
    alpha0 = alpha_of(norm0, energy[0][0])
    resid1 = (1.0 - alpha0 * S1, -alpha0)
    norm1 = jnp.maximum(form(gram, resid1), 0.0)
    beta0 = beta_of(norm1, norm0)
    direct1 = (resid1[0] + beta0, resid1[1])
    alpha1 = alpha_of(norm1, form(energy, direct1))
    resid2 = (
        resid1[0] - alpha1 * (S1 * direct1[0]),
        resid1[1] - alpha1 * (direct1[0] + S2 * direct1[1]),
        -alpha1 * direct1[1],
    )
    norm2 = jnp.maximum(form(gram, resid2), 0.0)
    beta1 = beta_of(norm2, norm1)
    direct2 = (resid2[0] + beta1 * direct1[0], resid2[1] + beta1 * direct1[1], resid2[2])
    alpha2 = alpha_of(norm2, form(energy, direct2))
    return (
        alpha0 + alpha1 * direct1[0] + alpha2 * direct2[0],
        alpha1 * direct1[1] + alpha2 * direct2[1],
        alpha2 * direct2[2],
    )


def combined(coefs, vectors):
    total = coefs[0] * vectors[0]
    for c, v in zip(coefs[1:], vectors[1:]):
        total = total + c * v
    return total


def middle(v, x, own):
    return v[(v.shape[0] - x) // 2 : (v.shape[0] + x) // 2, :own]


def inner(v):
    return v[HALO - INNER : v.shape[0] - (HALO - INNER)]


def gathered_products(parts_ref):
    return jnp.sum(parts_ref[...], axis=0, keepdims=True)


def odd_index(axis, shape):
    place = lax.rem(lax.axis_index(axis), 2)
    return (lax.broadcasted_iota(jnp.int32, shape, 0) * 0 + place) == 1


def stack_kernel(terminal, diagonal, guess, initial, fields_ref, far_edge, near_edge, sems):
    copies = [
        pltpu.make_async_copy(terminal, fields_ref.at[TERMINAL], sems.at[0]),
        pltpu.make_async_copy(diagonal, fields_ref.at[DIAGONAL], sems.at[1]),
        pltpu.make_async_copy(guess, fields_ref.at[pl.ds(GUESS, 2)], sems.at[2]),
        pltpu.make_async_copy(initial, fields_ref.at[INITIAL], sems.at[3]),
    ]
    for copy in copies:
        copy.start()
    for copy in copies:
        copy.wait()
    _, x, own = fields_ref.shape
    shape = (x, 128)
    strip = lax.broadcasted_iota(jnp.int32, shape, 1) // STRIP
    firsts = lasts = jnp.zeros(shape, jnp.float32)
    for k in range(FIELDS):
        first, last = fields_ref[k, :, :128], fields_ref[k, :, own - 128 :]
        firsts = jnp.where(strip == k, pltpu.roll(first, STRIP * k, 1) if k else first, firsts)
        lasts = jnp.where(strip == k, pltpu.roll(last, STRIP * (k + 1), 1), lasts)
    odd = odd_index(GY, shape)
    far_edge[...] = jnp.where(odd, lasts, firsts)
    near_edge[...] = jnp.where(odd, firsts, lasts)


def edge_kernel(fields_ref, far_edge, near_edge, block_ref):
    _, x, own = fields_ref.shape
    odd = odd_index(GY, (x, EDGE))
    left = jnp.where(odd, near_edge[:x, :], far_edge[...])
    right = jnp.where(odd, far_edge[...], near_edge[x:, :])
    for k in range(FIELDS):
        block_ref[x * k : x * (k + 1), :] = fields_ref[k]
    edges = [right[:8], left[:8], right[8:], left[8:]]
    block_ref[x * FIELDS :, :] = jnp.concatenate(edges, axis=1)


def row_kernel(band_ref, far_ref, near_ref):
    parts, _, own = band_ref.shape
    shape = (8, own)
    row = lax.broadcasted_iota(jnp.int32, shape, 0)

    def halves(part):
        tiles = [band_ref[part, 8 * k : 8 * k + 8, :] for k in range(2 * FIELDS + 1)]
        return tiles[: 2 * FIELDS : 2], tiles[1 : 2 * FIELDS : 2], tiles[2 * FIELDS]

    first, second, edge = halves(0)
    top = first + [
        jnp.where(row < 5, second[TERMINAL], pltpu.roll(second[DIAGONAL], 5, 0)),
        jnp.where(row < 4, second[GUESS + 1], pltpu.roll(second[GUESS], 4, 0)),
        edge,
    ]
    first, second, edge = halves(parts - 1)
    bottom = second + [
        jnp.where(row >= 3, first[TERMINAL], pltpu.roll(first[DIAGONAL], 3, 0)),
        jnp.where(row >= 4, first[GUESS + 1], pltpu.roll(first[GUESS], 4, 0)),
        edge,
    ]
    odd = odd_index(BAND, shape)
    for k, (t, b) in enumerate(zip(top, bottom)):
        far_ref[8 * k : 8 * k + 8, :] = jnp.where(odd, b, t)
        near_ref[8 * k : 8 * k + 8, :] = jnp.where(odd, t, b)


def first_kernel(grid, band_ref, far_ref, near_ref, basis_ref, center_ref, guess_ref, initial_ref, sums_ref):
    _, _, x, own = grid
    wide = own + EDGE
    rows = x + 2 * HALO
    parts = band_ref.shape[0]
    keep = keeper(HALO, x, own)
    odd = odd_index(BAND, (8, own))

    def tile(k, odd_from, odd_start, even_from, even_start):
        odd_tile = odd_from[8 * (odd_start + k) : 8 * (odd_start + k) + 8, :]
        return jnp.where(odd, odd_tile, even_from[8 * (even_start + k) : 8 * (even_start + k) + 8, :])

    above = [tile(k, near_ref, 0, far_ref, 0) for k in range(SENT)]
    below = [tile(k, far_ref, 0, near_ref, SENT) for k in range(SENT)]
    rest_above = {
        TERMINAL: above[FIELDS],
        DIAGONAL: pltpu.roll(above[FIELDS], 5, 0),
        GUESS + 1: above[FIELDS + 1],
        GUESS: pltpu.roll(above[FIELDS + 1], 4, 0),
    }
    rest_below = {
        TERMINAL: below[FIELDS],
        DIAGONAL: pltpu.roll(below[FIELDS], 3, 0),
        GUESS + 1: below[FIELDS + 1],
        GUESS: pltpu.roll(below[FIELDS + 1], 4, 0),
    }
    nothing = jnp.zeros((8, own), jnp.float32)
    blocks = [above[-1], *[band_ref[part, 2 * 8 * FIELDS :, :] for part in range(parts)], below[-1]]
    right, left = (
        jnp.concatenate([b[:, at : at + 128] for b in blocks for at in (start, start + 256)], axis=0)
        for start in (0, 128)
    )
    half = lax.broadcasted_iota(jnp.int32, (rows, EDGE), 1) < HALF

    def extended(k):
        whole = jnp.concatenate(
            [
                rest_above.get(k, nothing),
                above[k],
                *[band_ref[part, 16 * k : 16 * k + 16, :] for part in range(parts)],
                below[k],
                rest_below.get(k, nothing),
            ],
            axis=0,
        )
        from_right = pltpu.roll(right, 128 - STRIP * k, 1) if k else right
        from_left = pltpu.roll(left, 128 - STRIP * (k + 1), 1)
        return jnp.concatenate([whole, jnp.where(half, from_right, from_left)], axis=1)

    later = extended(TERMINAL)
    center = extended(DIAGONAL) + (inv_step + 4.0)
    rhs = inv_step * later - hamiltonian(later) + coupling * extended(GUESS + 1)
    vs = basis(keep(rhs), center, keep)
    for k in range(3):
        basis_ref[k] = vs[k]
    center_ref[...] = center
    guess_ref[...] = extended(GUESS)
    initial_ref[...] = inner(extended(INITIAL))
    mine = [middle(v, x, own) for v in vs]
    sums_ref[...] = row_of([(k, dot(mine[i], mine[j])) for k, (i, j) in enumerate(PAIRS)])


def second_kernel(grid, parts_ref, last_ref, center_ref, guess_ref, later_ref, basis_ref, inner_center, sums_ref):
    _, _, x, own = grid
    rows, wide = last_ref.shape[1:]
    keep = keeper(HALO, x, own)
    row = gathered_products(parts_ref)
    coefs = coefficients([entry(row, k) for k in range(len(PAIRS))])
    later = combined(coefs, [last_ref[k] for k in range(3)])
    later_ref[...] = inner(later)
    center = center_ref[...]
    inner_center[...] = inner(center)
    rhs = inv_step * later - hamiltonian(later) + coupling * guess_ref[...]
    vs = basis(keep(rhs), center, keep)
    for k in range(3):
        basis_ref[k] = inner(vs[k])
    mine = [middle(v, x, own) for v in vs]
    sums_ref[...] = row_of([(k, dot(mine[i], mine[j])) for k, (i, j) in enumerate(PAIRS)])


def third_kernel(grid, parts_ref, last_ref, center_ref, initial_ref, later_ref, value_ref, images_ref, sums_ref):
    _, _, x, own = grid
    rows, wide = last_ref.shape[1:]
    keep = keeper(INNER, x, own)
    row = gathered_products(parts_ref)
    coefs = coefficients([entry(row, k) for k in range(len(PAIRS))])
    value = combined(coefs, [last_ref[k] for k in range(3)])
    value_ref[...] = middle(value, x, own)
    center = center_ref[...]
    firsts = basis(density_rhs(initial_ref[...], drift(value), keep), center, keep)
    mine = [middle(v, x, own) for v in firsts]
    values = [(6 * 8 + k, dot(mine[i], mine[j])) for k, (i, j) in enumerate(PAIRS)]
    speeds = drift(later_ref[...])
    images = []
    for v in firsts[:3]:
        chain = basis(density_rhs(v, speeds, keep), center, keep)
        images.append([middle(w, x, own) for w in chain])
    for i in range(3):
        for k in range(3):
            images_ref[3 * i + k] = images[i][k]
    for place, (a, b) in enumerate(MIXED):
        for k, (i, j) in enumerate(PAIRS):
            values.append((8 * place + k, dot(images[a][i], images[b][j])))
    sums_ref[...] = row_of(values)


def fourth_kernel(parts_ref, images_ref, value_ref, value_out, density_ref):
    x = value_out.shape[0]
    mine = pl.ds(pl.multiple_of(lax.axis_index(PART) * x, x), x)
    value_out[...] = value_ref[mine, :]
    row = gathered_products(parts_ref)
    first = coefficients([entry(row, 6 * 8 + k) for k in range(len(PAIRS))])
    products = []
    for k in range(len(PAIRS)):
        total = None
        for place, (a, b) in enumerate(MIXED):
            term = first[a] * first[b] * entry(row, 8 * place + k)
            term = term if a == b else 2.0 * term
            total = term if total is None else total + term
        products.append(total)
    second = coefficients(products)
    total = None
    for i in range(3):
        for k in range(3):
            term = (first[i] * second[k]) * images_ref[3 * i + k, mine, :]
            total = term if total is None else total + term
    density_ref[...] = total


def everywhere(row):
    axes = (*BAND, *GY)
    size = lax.axis_size(axes)
    copies = jnp.broadcast_to(row, (size, 1, 128))
    return lax.all_to_all(copies, axes, split_axis=0, concat_axis=0, tiled=True).reshape(size, 128)


def swapped(far, near, axis):
    peers = lax.axis_size(axis)
    pairs = [(i, i + 1) for i in range(1, peers - 1, 2)]
    return (
        lax.ppermute(far, axis, pairs + [(b, a) for a, b in pairs]),
        lax.all_gather(near, axis[-1], tiled=True),
    )


def call(kernel, out_shape, *args, results=pltpu.VMEM):
    vmem = pl.BlockSpec(memory_space=pltpu.VMEM)
    return pl.pallas_call(
        kernel,
        out_shape=[results(s, jnp.float32) for s in out_shape],
        in_specs=[vmem] * len(args),
        out_specs=[vmem] * len(out_shape),
        compiler_params=pltpu.CompilerParams(vmem_limit_bytes=VMEM_LIMIT),
    )(*[pltpu.with_memory_space_constraint(a, pltpu.VMEM) for a in args])


def shards(terminal, initial_density, density_guess, diagonal):
    x, own = terminal.shape
    band = x * lax.axis_size(PART)
    grid = (x * lax.axis_size(GX), own * lax.axis_size(GY), band, own)
    fields, far, near = pl.pallas_call(
        stack_kernel,
        out_shape=[pltpu.VMEM(s, jnp.float32) for s in [(FIELDS, x, own), (x, EDGE), (x, EDGE)]],
        in_specs=[pl.BlockSpec(memory_space=pltpu.HBM)] * 4,
        out_specs=[pl.BlockSpec(memory_space=pltpu.VMEM)] * 3,
        scratch_shapes=[pltpu.SemaphoreType.DMA((4,))],
    )(terminal, diagonal, density_guess, initial_density)
    (block,) = call(edge_kernel, [(x * FIELDS + 8, own)], fields, *swapped(far, near, GY))
    whole = lax.all_gather(block, PART)
    packed = (8 * SENT, own)
    far, near = call(row_kernel, [packed, packed], whole)
    rows = band + 2 * HALO
    wide = own + EDGE
    full, fewer = (rows, wide), (band + 2 * INNER, wide)
    basis1, center, guess, initial, sums = call(
        functools.partial(first_kernel, grid),
        [(3, *full), full, full, fewer, (1, 128)],
        whole, *swapped(far, near, BAND),
    )
    later, basis0, center, sums = call(
        functools.partial(second_kernel, grid),
        [fewer, (3, *fewer), fewer, (1, 128)],
        everywhere(sums), basis1, center, guess,
    )
    value, images, sums = call(
        functools.partial(third_kernel, grid),
        [(band, own), (9, band, own), (1, 128)],
        everywhere(sums), basis0, center, initial, later,
    )
    return tuple(
        call(
            fourth_kernel, [(x, own)] * 2, everywhere(sums), images, value,
            results=jax.ShapeDtypeStruct,
        )
    )


def solution(mesh):
    torus = Mesh(mesh.devices.reshape(4, 2, 4, 8, 2), GX + GY)
    in_specs = (P(GX, GY), P(GX, GY), P(None, GX, GY), P(GX, GY))
    out_specs = (P(GX, GY), P(GX, GY))
    return jax.shard_map(
        shards, mesh=torus, in_specs=in_specs, out_specs=out_specs, check_vma=False
    )
```

```python
import functools

import jax
import jax.numpy as jnp
from jax import lax
from jax.experimental import pallas as pl
from jax.experimental.pallas import tpu as pltpu
from jax.sharding import Mesh
from jax.sharding import PartitionSpec as P

BAND = ("band_0", "band_1")
PART = "part"
GX = (*BAND, PART)
GY = ("gy_0", "gy_1")

inv_step = 0.5
coupling = 0.5

LOW = 0.6
HIGH = 10.5
S1 = 3.5
S2 = 5.5
S3 = 4.0
PAIRS = ((0, 0), (0, 1), (1, 1), (1, 2), (2, 2), (2, 3))
MIXED = ((0, 0), (1, 1), (2, 2), (0, 1), (0, 2), (1, 2))

HALF = 64
EDGE = 128
TERMINAL, DIAGONAL, GUESS, INITIAL = 0, 1, 2, 4
FIELDS = 5
VMEM_LIMIT = 24 * 2**20
STRIP = 16
HALO = 16
INNER = 8


def before(v, dim):
    return pltpu.roll(v, 1, dim)


def after(v, dim):
    return pltpu.roll(v, v.shape[dim] - 1, dim)


def keeper(halo, x, own):
    band, column = lax.axis_index(BAND), lax.axis_index(GY)
    bands, columns = lax.axis_size(BAND), lax.axis_size(GY)
    top = jnp.where(band > 0, 1.0, 0.0)
    bottom = jnp.where(band < bands - 1, 1.0, 0.0)
    lane = lax.broadcasted_iota(jnp.int32, (8, EDGE), 1)
    edge = jnp.where(
        lane < HALF, jnp.where(column < columns - 1, 1.0, 0.0), jnp.where(column > 0, 1.0, 0.0)
    )

    def tiled(rows):
        return jnp.concatenate([edge] * (rows // 8), axis=0)

    ends = tiled(halo)

    def keep(v):
        first, last = v[:halo], v[halo + x :]
        inner_rows = v[halo : halo + x]
        main = [first[:, :own] * top, inner_rows[:, :own], last[:, :own] * bottom]
        side = [
            first[:, own:] * (ends * top),
            inner_rows[:, own:] * tiled(x),
            last[:, own:] * (ends * bottom),
        ]
        return jnp.concatenate([jnp.concatenate(p, axis=0) for p in (main, side)], axis=1)

    return keep


def shifted(v, center, shift, keep):
    beside = (before(v, 0) + after(v, 0)) + (before(v, 1) + after(v, 1))
    return keep((center - shift) * v - beside)


def basis(v0, center, keep):
    v1 = shifted(v0, center, S1, keep)
    v2 = shifted(v1, center, S2, keep)
    return [v0, v1, v2, shifted(v2, center, S3, keep)]


def hamiltonian(u):
    total = None
    for dim in (0, 1):
        ahead = after(u, dim) - u
        term = before(jnp.maximum(ahead, 0.0) ** 2, dim) + jnp.minimum(ahead, 0.0) ** 2
        total = term if total is None else total + term
    return 0.5 * total


def drift(u):
    speed_x = u - after(u, 0)
    speed_y = u - after(u, 1)
    return (
        jnp.maximum(speed_x, 0.0),
        jnp.minimum(speed_x, 0.0),
        jnp.maximum(speed_y, 0.0),
        jnp.minimum(speed_y, 0.0),
    )


def density_rhs(m, speeds, keep):
    out_x, in_x, out_y, in_y = speeds
    flux_x = out_x * m + in_x * after(m, 0)
    flux_y = out_y * m + in_y * after(m, 1)
    div = (flux_x - before(flux_x, 0)) + (flux_y - before(flux_y, 1))
    return keep(inv_step * m - div)


def dot(a, b):
    rows, wide = a.shape
    total = jnp.sum((a * b).reshape(rows // 8, 8, wide), axis=0)
    total = sum(total[:, k : k + 128] for k in range(128, wide, 128)) + total[:, :128]
    return jnp.sum(total, axis=1, keepdims=True)


def row_of(values):
    lane = lax.broadcasted_iota(jnp.int32, (8, 128), 1)
    rows = jnp.zeros((8, 128), jnp.float32)
    for place, value in values:
        rows = jnp.where(lane == place, value, rows)
    return jnp.sum(rows, axis=0, keepdims=True)


def entry(row, place):
    lane = lax.broadcasted_iota(jnp.int32, row.shape, 1)
    return jnp.sum(jnp.where(lane == place, row, 0.0), axis=1, keepdims=True)


def form(matrix, vector):
    total = None
    for i, a in enumerate(vector):
        for j, b in enumerate(vector[: i + 1]):
            term = a * b * matrix[j][i]
            term = term if i == j else 2.0 * term
            total = term if total is None else total + term
    return total


def alpha_of(squared, energy):
    return jnp.clip(squared / jnp.maximum(energy, 1e-36), 0.999 / HIGH, 1.001 / LOW)


def beta_of(new, old):
    return jnp.clip(new / jnp.maximum(old, 1e-36), 0.0, 1.001 * HIGH / LOW)


def coefficients(products):
    g = dict(zip(PAIRS, products))
    g[0, 2] = g[1, 1] + (S1 - S2) * g[0, 1]
    gram = [[g[0, 0], g[0, 1], g[0, 2]], [None, g[1, 1], g[1, 2]], [None, None, g[2, 2]]]
    energy = [
        [g[0, 1] + S1 * g[0, 0], g[1, 1] + S1 * g[0, 1], g[1, 2] + S1 * g[0, 2]],
        [None, g[1, 2] + S2 * g[1, 1], g[2, 2] + S2 * g[1, 2]],
        [None, None, g[2, 3] + S3 * g[2, 2]],
    ]
    norm0 = g[0, 0]
    alpha0 = alpha_of(norm0, energy[0][0])
    resid1 = (1.0 - alpha0 * S1, -alpha0)
    norm1 = jnp.maximum(form(gram, resid1), 0.0)
    beta0 = beta_of(norm1, norm0)
    direct1 = (resid1[0] + beta0, resid1[1])
    alpha1 = alpha_of(norm1, form(energy, direct1))
    resid2 = (
        resid1[0] - alpha1 * (S1 * direct1[0]),
        resid1[1] - alpha1 * (direct1[0] + S2 * direct1[1]),
        -alpha1 * direct1[1],
    )
    norm2 = jnp.maximum(form(gram, resid2), 0.0)
    beta1 = beta_of(norm2, norm1)
    direct2 = (resid2[0] + beta1 * direct1[0], resid2[1] + beta1 * direct1[1], resid2[2])
    alpha2 = alpha_of(norm2, form(energy, direct2))
    return (
        alpha0 + alpha1 * direct1[0] + alpha2 * direct2[0],
        alpha1 * direct1[1] + alpha2 * direct2[1],
        alpha2 * direct2[2],
    )


def combined(coefs, vectors):
    total = coefs[0] * vectors[0]
    for c, v in zip(coefs[1:], vectors[1:]):
        total = total + c * v
    return total


def middle(v, x, own):
    return v[(v.shape[0] - x) // 2 : (v.shape[0] + x) // 2, :own]


def inner(v):
    return v[HALO - INNER : v.shape[0] - (HALO - INNER)]


def gathered_products(parts_ref):
    return jnp.sum(parts_ref[...], axis=0, keepdims=True)


def odd_index(axis, shape):
    place = lax.rem(lax.axis_index(axis), 2)
    return (lax.broadcasted_iota(jnp.int32, shape, 0) * 0 + place) == 1


def stack_kernel(terminal, diagonal, guess, initial, fields_ref, sems):
    copies = [
        pltpu.make_async_copy(terminal, fields_ref.at[TERMINAL], sems.at[0]),
        pltpu.make_async_copy(diagonal, fields_ref.at[DIAGONAL], sems.at[1]),
        pltpu.make_async_copy(guess, fields_ref.at[pl.ds(GUESS, 2)], sems.at[2]),
        pltpu.make_async_copy(initial, fields_ref.at[INITIAL], sems.at[3]),
    ]
    for copy in copies:
        copy.start()
    for copy in copies:
        copy.wait()


def row_kernel(band_ref, far_ref, near_ref):
    parts, _, _, own = band_ref.shape
    shape = (8, own)
    row = lax.broadcasted_iota(jnp.int32, shape, 0)
    first, second = ([band_ref[0, k, half] for k in range(FIELDS)] for half in (pl.ds(0, 8), pl.ds(8, 8)))
    top = first + [
        jnp.where(row < 5, second[TERMINAL], pltpu.roll(second[DIAGONAL], 5, 0)),
        jnp.where(row < 4, second[GUESS + 1], pltpu.roll(second[GUESS], 4, 0)),
    ]
    first, second = ([band_ref[parts - 1, k, half] for k in range(FIELDS)] for half in (pl.ds(0, 8), pl.ds(8, 8)))
    bottom = second + [
        jnp.where(row >= 3, first[TERMINAL], pltpu.roll(first[DIAGONAL], 3, 0)),
        jnp.where(row >= 4, first[GUESS + 1], pltpu.roll(first[GUESS], 4, 0)),
    ]
    odd = odd_index(BAND, shape)
    for k, (t, b) in enumerate(zip(top, bottom)):
        far_ref[8 * k : 8 * k + 8, :] = jnp.where(odd, b, t)
        near_ref[8 * k : 8 * k + 8, :] = jnp.where(odd, t, b)


def column_kernel(band_ref, far_ref, near_ref, tall_ref, far_edge, near_edge):
    parts, _, x, own = band_ref.shape
    odd = odd_index(BAND, (8, own))

    sent = FIELDS + 2

    def tile(k, odd_from, odd_start, even_from, even_start):
        odd_tile = odd_from[8 * (odd_start + k) : 8 * (odd_start + k) + 8, :]
        return jnp.where(odd, odd_tile, even_from[8 * (even_start + k) : 8 * (even_start + k) + 8, :])

    above = [tile(k, near_ref, 0, far_ref, 0) for k in range(sent)]
    below = [tile(k, far_ref, 0, near_ref, sent) for k in range(sent)]
    rest_above = {
        TERMINAL: above[FIELDS],
        DIAGONAL: pltpu.roll(above[FIELDS], 5, 0),
        GUESS + 1: above[FIELDS + 1],
        GUESS: pltpu.roll(above[FIELDS + 1], 4, 0),
    }
    rest_below = {
        TERMINAL: below[FIELDS],
        DIAGONAL: pltpu.roll(below[FIELDS], 3, 0),
        GUESS + 1: below[FIELDS + 1],
        GUESS: pltpu.roll(below[FIELDS + 1], 4, 0),
    }
    nothing = jnp.zeros((8, own), jnp.float32)
    shape = (parts * x + 2 * HALO, 128)
    strip = lax.broadcasted_iota(jnp.int32, shape, 1) // STRIP
    firsts = lasts = jnp.zeros(shape, jnp.float32)
    for k in range(FIELDS):
        blocks = [band_ref[part, k] for part in range(parts)]
        whole = jnp.concatenate(
            [rest_above.get(k, nothing), above[k], *blocks, below[k], rest_below.get(k, nothing)], axis=0
        )
        tall_ref[k] = whole
        first, last = whole[:, :128], whole[:, own - 128 :]
        firsts = jnp.where(strip == k, pltpu.roll(first, STRIP * k, 1) if k else first, firsts)
        lasts = jnp.where(strip == k, pltpu.roll(last, STRIP * (k + 1), 1), lasts)
    odd = odd_index(GY, shape)
    far_edge[...] = jnp.where(odd, lasts, firsts)
    near_edge[...] = jnp.where(odd, firsts, lasts)


def first_kernel(grid, tall_ref, far_edge, near_edge, basis_ref, center_ref, guess_ref, initial_ref, sums_ref):
    _, _, x, own = grid
    wide = own + EDGE
    rows = tall_ref.shape[1]
    keep = keeper(HALO, x, own)
    odd = odd_index(GY, (rows, EDGE))
    left = jnp.where(odd, near_edge[:rows, :], far_edge[...])
    right = jnp.where(odd, far_edge[...], near_edge[rows:, :])
    half = lax.broadcasted_iota(jnp.int32, (rows, EDGE), 1) < HALF

    def extended(k):
        from_right = pltpu.roll(right, 128 - STRIP * k, 1) if k else right
        from_left = pltpu.roll(left, 128 - STRIP * (k + 1), 1)
        return jnp.concatenate([tall_ref[k], jnp.where(half, from_right, from_left)], axis=1)

    later = extended(TERMINAL)
    center = extended(DIAGONAL) + (inv_step + 4.0)
    rhs = inv_step * later - hamiltonian(later) + coupling * extended(GUESS + 1)
    vs = basis(keep(rhs), center, keep)
    for k in range(3):
        basis_ref[k] = vs[k]
    center_ref[...] = center
    guess_ref[...] = extended(GUESS)
    initial_ref[...] = inner(extended(INITIAL))
    mine = [middle(v, x, own) for v in vs]
    sums_ref[...] = row_of([(k, dot(mine[i], mine[j])) for k, (i, j) in enumerate(PAIRS)])


def second_kernel(grid, parts_ref, last_ref, center_ref, guess_ref, later_ref, basis_ref, inner_center, sums_ref):
    _, _, x, own = grid
    rows, wide = last_ref.shape[1:]
    keep = keeper(HALO, x, own)
    row = gathered_products(parts_ref)
    coefs = coefficients([entry(row, k) for k in range(len(PAIRS))])
    later = combined(coefs, [last_ref[k] for k in range(3)])
    later_ref[...] = inner(later)
    center = center_ref[...]
    inner_center[...] = inner(center)
    rhs = inv_step * later - hamiltonian(later) + coupling * guess_ref[...]
    vs = basis(keep(rhs), center, keep)
    for k in range(3):
        basis_ref[k] = inner(vs[k])
    mine = [middle(v, x, own) for v in vs]
    sums_ref[...] = row_of([(k, dot(mine[i], mine[j])) for k, (i, j) in enumerate(PAIRS)])


def third_kernel(grid, parts_ref, last_ref, center_ref, initial_ref, later_ref, value_ref, images_ref, sums_ref):
    _, _, x, own = grid
    rows, wide = last_ref.shape[1:]
    keep = keeper(INNER, x, own)
    row = gathered_products(parts_ref)
    coefs = coefficients([entry(row, k) for k in range(len(PAIRS))])
    value = combined(coefs, [last_ref[k] for k in range(3)])
    value_ref[...] = middle(value, x, own)
    center = center_ref[...]
    firsts = basis(density_rhs(initial_ref[...], drift(value), keep), center, keep)
    mine = [middle(v, x, own) for v in firsts]
    values = [(6 * 8 + k, dot(mine[i], mine[j])) for k, (i, j) in enumerate(PAIRS)]
    speeds = drift(later_ref[...])
    images = []
    for v in firsts[:3]:
        chain = basis(density_rhs(v, speeds, keep), center, keep)
        images.append([middle(w, x, own) for w in chain])
    for i in range(3):
        for k in range(3):
            images_ref[3 * i + k] = images[i][k]
    for place, (a, b) in enumerate(MIXED):
        for k, (i, j) in enumerate(PAIRS):
            values.append((8 * place + k, dot(images[a][i], images[b][j])))
    sums_ref[...] = row_of(values)


def fourth_kernel(parts_ref, images_ref, value_ref, value_out, density_ref):
    x = value_out.shape[0]
    mine = pl.ds(pl.multiple_of(lax.axis_index(PART) * x, x), x)
    value_out[...] = value_ref[mine, :]
    row = gathered_products(parts_ref)
    first = coefficients([entry(row, 6 * 8 + k) for k in range(len(PAIRS))])
    products = []
    for k in range(len(PAIRS)):
        total = None
        for place, (a, b) in enumerate(MIXED):
            term = first[a] * first[b] * entry(row, 8 * place + k)
            term = term if a == b else 2.0 * term
            total = term if total is None else total + term
        products.append(total)
    second = coefficients(products)
    total = None
    for i in range(3):
        for k in range(3):
            term = (first[i] * second[k]) * images_ref[3 * i + k, mine, :]
            total = term if total is None else total + term
    density_ref[...] = total


def everywhere(row):
    axes = (*BAND, *GY)
    size = lax.axis_size(axes)
    copies = jnp.broadcast_to(row, (size, 1, 128))
    return lax.all_to_all(copies, axes, split_axis=0, concat_axis=0, tiled=True).reshape(size, 128)


def swapped(far, near, axis):
    peers = lax.axis_size(axis)
    pairs = [(i, i + 1) for i in range(1, peers - 1, 2)]
    return (
        lax.ppermute(far, axis, pairs + [(b, a) for a, b in pairs]),
        lax.all_gather(near, axis[-1], tiled=True),
    )


def call(kernel, out_shape, *args, results=pltpu.VMEM):
    vmem = pl.BlockSpec(memory_space=pltpu.VMEM)
    return pl.pallas_call(
        kernel,
        out_shape=[results(s, jnp.float32) for s in out_shape],
        in_specs=[vmem] * len(args),
        out_specs=[vmem] * len(out_shape),
        compiler_params=pltpu.CompilerParams(vmem_limit_bytes=VMEM_LIMIT),
    )(*[pltpu.with_memory_space_constraint(a, pltpu.VMEM) for a in args])


def shards(terminal, initial_density, density_guess, diagonal):
    x, own = terminal.shape
    band = x * lax.axis_size(PART)
    grid = (x * lax.axis_size(GX), own * lax.axis_size(GY), band, own)
    fields = pl.pallas_call(
        stack_kernel,
        out_shape=pltpu.VMEM((FIELDS, x, own), jnp.float32),
        in_specs=[pl.BlockSpec(memory_space=pltpu.HBM)] * 4,
        out_specs=pl.BlockSpec(memory_space=pltpu.VMEM),
        scratch_shapes=[pltpu.SemaphoreType.DMA((4,))],
    )(terminal, diagonal, density_guess, initial_density)
    whole = lax.all_gather(fields, PART)
    packed = (8 * (FIELDS + 2), own)
    far, near = call(row_kernel, [packed, packed], whole)
    rows = band + 2 * HALO
    tall, far, near = call(
        column_kernel,
        [(FIELDS, rows, own), (rows, 128), (rows, 128)],
        whole, *swapped(far, near, BAND),
    )
    wide = own + EDGE
    full, fewer = (rows, wide), (band + 2 * INNER, wide)
    basis1, center, guess, initial, sums = call(
        functools.partial(first_kernel, grid),
        [(3, *full), full, full, fewer, (1, 128)],
        tall, *swapped(far, near, GY),
    )
    later, basis0, center, sums = call(
        functools.partial(second_kernel, grid),
        [fewer, (3, *fewer), fewer, (1, 128)],
        everywhere(sums), basis1, center, guess,
    )
    value, images, sums = call(
        functools.partial(third_kernel, grid),
        [(band, own), (9, band, own), (1, 128)],
        everywhere(sums), basis0, center, initial, later,
    )
    return tuple(
        call(
            fourth_kernel, [(x, own)] * 2, everywhere(sums), images, value,
            results=jax.ShapeDtypeStruct,
        )
    )


def solution(mesh):
    torus = Mesh(mesh.devices.reshape(4, 2, 4, 8, 2), GX + GY)
    in_specs = (P(GX, GY), P(GX, GY), P(None, GX, GY), P(GX, GY))
    out_specs = (P(GX, GY), P(GX, GY))
    return jax.shard_map(
        shards, mesh=torus, in_specs=in_specs, out_specs=out_specs, check_vma=False
    )
```

```python
import functools

import jax
import jax.numpy as jnp
from jax import lax
from jax.experimental import pallas as pl
from jax.experimental.pallas import tpu as pltpu
from jax.sharding import Mesh
from jax.sharding import PartitionSpec as P

BAND = ("band_0", "band_1")
PART = "part"
GX = (*BAND, PART)
GY = ("gy_0", "gy_1")

inv_step = 0.5
coupling = 0.5

LOW = 0.6
HIGH = 10.5
S1 = 3.5
S2 = 5.5
S3 = 4.0
PAIRS = ((0, 0), (0, 1), (1, 1), (1, 2), (2, 2), (2, 3))
MIXED = ((0, 0), (1, 1), (2, 2), (0, 1), (0, 2), (1, 2))

HALF = 64
EDGE = 128
TERMINAL, DIAGONAL, GUESS, INITIAL = 0, 1, 2, 4
FIELDS = 5
SENT = FIELDS + 3
VMEM_LIMIT = 24 * 2**20
STRIP = 16
HALO = 16
INNER = 8


def before(v, dim):
    return pltpu.roll(v, 1, dim)


def after(v, dim):
    return pltpu.roll(v, v.shape[dim] - 1, dim)


def keeper(halo, x, own):
    band, column = lax.axis_index(BAND), lax.axis_index(GY)
    bands, columns = lax.axis_size(BAND), lax.axis_size(GY)
    top = jnp.where(band > 0, 1.0, 0.0)
    bottom = jnp.where(band < bands - 1, 1.0, 0.0)
    lane = lax.broadcasted_iota(jnp.int32, (8, EDGE), 1)
    edge = jnp.where(
        lane < HALF, jnp.where(column < columns - 1, 1.0, 0.0), jnp.where(column > 0, 1.0, 0.0)
    )

    def tiled(rows):
        return jnp.concatenate([edge] * (rows // 8), axis=0)

    ends = tiled(halo)

    def keep(v):
        first, last = v[:halo], v[halo + x :]
        inner_rows = v[halo : halo + x]
        main = [first[:, :own] * top, inner_rows[:, :own], last[:, :own] * bottom]
        side = [
            first[:, own:] * (ends * top),
            inner_rows[:, own:] * tiled(x),
            last[:, own:] * (ends * bottom),
        ]
        return jnp.concatenate([jnp.concatenate(p, axis=0) for p in (main, side)], axis=1)

    return keep


def shifted(v, center, shift, keep):
    beside = (before(v, 0) + after(v, 0)) + (before(v, 1) + after(v, 1))
    return keep((center - shift) * v - beside)


def basis(v0, center, keep):
    v1 = shifted(v0, center, S1, keep)
    v2 = shifted(v1, center, S2, keep)
    return [v0, v1, v2, shifted(v2, center, S3, keep)]


def hamiltonian(u):
    total = None
    for dim in (0, 1):
        ahead = after(u, dim) - u
        term = before(jnp.maximum(ahead, 0.0) ** 2, dim) + jnp.minimum(ahead, 0.0) ** 2
        total = term if total is None else total + term
    return 0.5 * total


def drift(u):
    speed_x = u - after(u, 0)
    speed_y = u - after(u, 1)
    return (
        jnp.maximum(speed_x, 0.0),
        jnp.minimum(speed_x, 0.0),
        jnp.maximum(speed_y, 0.0),
        jnp.minimum(speed_y, 0.0),
    )


def density_rhs(m, speeds, keep):
    out_x, in_x, out_y, in_y = speeds
    flux_x = out_x * m + in_x * after(m, 0)
    flux_y = out_y * m + in_y * after(m, 1)
    div = (flux_x - before(flux_x, 0)) + (flux_y - before(flux_y, 1))
    return keep(inv_step * m - div)


def dot(a, b):
    rows, wide = a.shape
    total = jnp.sum((a * b).reshape(rows // 8, 8, wide), axis=0)
    total = sum(total[:, k : k + 128] for k in range(128, wide, 128)) + total[:, :128]
    return jnp.sum(total, axis=1, keepdims=True)


def row_of(values):
    lane = lax.broadcasted_iota(jnp.int32, (8, 128), 1)
    rows = jnp.zeros((8, 128), jnp.float32)
    for place, value in values:
        rows = jnp.where(lane == place, value, rows)
    return jnp.sum(rows, axis=0, keepdims=True)


def entry(row, place):
    lane = lax.broadcasted_iota(jnp.int32, row.shape, 1)
    return jnp.sum(jnp.where(lane == place, row, 0.0), axis=1, keepdims=True)


def form(matrix, vector):
    total = None
    for i, a in enumerate(vector):
        for j, b in enumerate(vector[: i + 1]):
            term = a * b * matrix[j][i]
            term = term if i == j else 2.0 * term
            total = term if total is None else total + term
    return total


def alpha_of(squared, energy):
    return jnp.clip(squared / jnp.maximum(energy, 1e-36), 0.999 / HIGH, 1.001 / LOW)


def beta_of(new, old):
    return jnp.clip(new / jnp.maximum(old, 1e-36), 0.0, 1.001 * HIGH / LOW)


def coefficients(products):
    g = dict(zip(PAIRS, products))
    g[0, 2] = g[1, 1] + (S1 - S2) * g[0, 1]
    gram = [[g[0, 0], g[0, 1], g[0, 2]], [None, g[1, 1], g[1, 2]], [None, None, g[2, 2]]]
    energy = [
        [g[0, 1] + S1 * g[0, 0], g[1, 1] + S1 * g[0, 1], g[1, 2] + S1 * g[0, 2]],
        [None, g[1, 2] + S2 * g[1, 1], g[2, 2] + S2 * g[1, 2]],
        [None, None, g[2, 3] + S3 * g[2, 2]],
    ]
    norm0 = g[0, 0]
    alpha0 = alpha_of(norm0, energy[0][0])
    resid1 = (1.0 - alpha0 * S1, -alpha0)
    norm1 = jnp.maximum(form(gram, resid1), 0.0)
    beta0 = beta_of(norm1, norm0)
    direct1 = (resid1[0] + beta0, resid1[1])
    alpha1 = alpha_of(norm1, form(energy, direct1))
    resid2 = (
        resid1[0] - alpha1 * (S1 * direct1[0]),
        resid1[1] - alpha1 * (direct1[0] + S2 * direct1[1]),
        -alpha1 * direct1[1],
    )
    norm2 = jnp.maximum(form(gram, resid2), 0.0)
    beta1 = beta_of(norm2, norm1)
    direct2 = (resid2[0] + beta1 * direct1[0], resid2[1] + beta1 * direct1[1], resid2[2])
    alpha2 = alpha_of(norm2, form(energy, direct2))
    return (
        alpha0 + alpha1 * direct1[0] + alpha2 * direct2[0],
        alpha1 * direct1[1] + alpha2 * direct2[1],
        alpha2 * direct2[2],
    )


def combined(coefs, vectors):
    total = coefs[0] * vectors[0]
    for c, v in zip(coefs[1:], vectors[1:]):
        total = total + c * v
    return total


def middle(v, x, own):
    return v[(v.shape[0] - x) // 2 : (v.shape[0] + x) // 2, :own]


def inner(v):
    return v[HALO - INNER : v.shape[0] - (HALO - INNER)]


def gathered_products(parts_ref):
    return jnp.sum(parts_ref[...], axis=0, keepdims=True)


def odd_index(axis, shape):
    place = lax.rem(lax.axis_index(axis), 2)
    return (lax.broadcasted_iota(jnp.int32, shape, 0) * 0 + place) == 1


def stack_kernel(terminal, diagonal, guess, initial, fields_ref, far_edge, near_edge, sems):
    copies = [
        pltpu.make_async_copy(terminal, fields_ref.at[TERMINAL], sems.at[0]),
        pltpu.make_async_copy(diagonal, fields_ref.at[DIAGONAL], sems.at[1]),
        pltpu.make_async_copy(guess, fields_ref.at[pl.ds(GUESS, 2)], sems.at[2]),
        pltpu.make_async_copy(initial, fields_ref.at[INITIAL], sems.at[3]),
    ]
    for copy in copies:
        copy.start()
    for copy in copies:
        copy.wait()
    _, x, own = fields_ref.shape
    shape = (x, 128)
    strip = lax.broadcasted_iota(jnp.int32, shape, 1) // STRIP
    firsts = lasts = jnp.zeros(shape, jnp.float32)
    for k in range(FIELDS):
        first, last = fields_ref[k, :, :128], fields_ref[k, :, own - 128 :]
        firsts = jnp.where(strip == k, pltpu.roll(first, STRIP * k, 1) if k else first, firsts)
        lasts = jnp.where(strip == k, pltpu.roll(last, STRIP * (k + 1), 1), lasts)
    odd = odd_index(GY, shape)
    far_edge[...] = jnp.where(odd, lasts, firsts)
    near_edge[...] = jnp.where(odd, firsts, lasts)


def edge_kernel(fields_ref, far_edge, near_edge, block_ref):
    _, x, own = fields_ref.shape
    odd = odd_index(GY, (x, EDGE))
    left = jnp.where(odd, near_edge[:x, :], far_edge[...])
    right = jnp.where(odd, far_edge[...], near_edge[x:, :])
    for k in range(FIELDS):
        block_ref[x * k : x * (k + 1), :] = fields_ref[k]
    edges = [right[:8], left[:8], right[8:], left[8:]]
    block_ref[x * FIELDS :, :] = jnp.concatenate(edges, axis=1)


def row_kernel(band_ref, far_ref, near_ref):
    parts, _, own = band_ref.shape
    shape = (8, own)
    row = lax.broadcasted_iota(jnp.int32, shape, 0)

    def halves(part):
        tiles = [band_ref[part, 8 * k : 8 * k + 8, :] for k in range(2 * FIELDS + 1)]
        return tiles[: 2 * FIELDS : 2], tiles[1 : 2 * FIELDS : 2], tiles[2 * FIELDS]

    first, second, edge = halves(0)
    top = first + [
        jnp.where(row < 5, second[TERMINAL], pltpu.roll(second[DIAGONAL], 5, 0)),
        jnp.where(row < 4, second[GUESS + 1], pltpu.roll(second[GUESS], 4, 0)),
        edge,
    ]
    first, second, edge = halves(parts - 1)
    bottom = second + [
        jnp.where(row >= 3, first[TERMINAL], pltpu.roll(first[DIAGONAL], 3, 0)),
        jnp.where(row >= 4, first[GUESS + 1], pltpu.roll(first[GUESS], 4, 0)),
        edge,
    ]
    odd = odd_index(BAND, shape)
    for k, (t, b) in enumerate(zip(top, bottom)):
        far_ref[8 * k : 8 * k + 8, :] = jnp.where(odd, b, t)
        near_ref[8 * k : 8 * k + 8, :] = jnp.where(odd, t, b)


def first_kernel(grid, band_ref, far_ref, near_ref, basis_ref, center_ref, guess_ref, initial_ref, sums_ref):
    _, _, x, own = grid
    wide = own + EDGE
    rows = x + 2 * HALO
    parts = band_ref.shape[0]
    keep = keeper(HALO, x, own)
    odd = odd_index(BAND, (8, own))

    def tile(k, odd_from, odd_start, even_from, even_start):
        odd_tile = odd_from[8 * (odd_start + k) : 8 * (odd_start + k) + 8, :]
        return jnp.where(odd, odd_tile, even_from[8 * (even_start + k) : 8 * (even_start + k) + 8, :])

    above = [tile(k, near_ref, 0, far_ref, 0) for k in range(SENT)]
    below = [tile(k, far_ref, 0, near_ref, SENT) for k in range(SENT)]
    rest_above = {
        TERMINAL: above[FIELDS],
        DIAGONAL: pltpu.roll(above[FIELDS], 5, 0),
        GUESS + 1: above[FIELDS + 1],
        GUESS: pltpu.roll(above[FIELDS + 1], 4, 0),
    }
    rest_below = {
        TERMINAL: below[FIELDS],
        DIAGONAL: pltpu.roll(below[FIELDS], 3, 0),
        GUESS + 1: below[FIELDS + 1],
        GUESS: pltpu.roll(below[FIELDS + 1], 4, 0),
    }
    nothing = jnp.zeros((8, own), jnp.float32)
    blocks = [above[-1], *[band_ref[part, 2 * 8 * FIELDS :, :] for part in range(parts)], below[-1]]
    right, left = (
        jnp.concatenate([b[:, at : at + 128] for b in blocks for at in (start, start + 256)], axis=0)
        for start in (0, 128)
    )
    half = lax.broadcasted_iota(jnp.int32, (rows, EDGE), 1) < HALF

    def extended(k):
        whole = jnp.concatenate(
            [
                rest_above.get(k, nothing),
                above[k],
                *[band_ref[part, 16 * k : 16 * k + 16, :] for part in range(parts)],
                below[k],
                rest_below.get(k, nothing),
            ],
            axis=0,
        )
        from_right = pltpu.roll(right, 128 - STRIP * k, 1) if k else right
        from_left = pltpu.roll(left, 128 - STRIP * (k + 1), 1)
        return jnp.concatenate([whole, jnp.where(half, from_right, from_left)], axis=1)

    later = extended(TERMINAL)
    center = extended(DIAGONAL) + (inv_step + 4.0)
    rhs = inv_step * later - hamiltonian(later) + coupling * extended(GUESS + 1)
    vs = basis(keep(rhs), center, keep)
    for k in range(3):
        basis_ref[k] = vs[k]
    center_ref[...] = center
    guess_ref[...] = extended(GUESS)
    initial_ref[...] = inner(extended(INITIAL))
    mine = [middle(v, x, own) for v in vs]
    sums_ref[...] = row_of([(k, dot(mine[i], mine[j])) for k, (i, j) in enumerate(PAIRS)])


def second_kernel(grid, parts_ref, last_ref, center_ref, guess_ref, later_ref, basis_ref, inner_center, sums_ref):
    _, _, x, own = grid
    rows, wide = last_ref.shape[1:]
    keep = keeper(HALO, x, own)
    row = gathered_products(parts_ref)
    coefs = coefficients([entry(row, k) for k in range(len(PAIRS))])
    later = combined(coefs, [last_ref[k] for k in range(3)])
    later_ref[...] = inner(later)
    center = center_ref[...]
    inner_center[...] = inner(center)
    rhs = inv_step * later - hamiltonian(later) + coupling * guess_ref[...]
    vs = basis(keep(rhs), center, keep)
    for k in range(3):
        basis_ref[k] = inner(vs[k])
    mine = [middle(v, x, own) for v in vs]
    sums_ref[...] = row_of([(k, dot(mine[i], mine[j])) for k, (i, j) in enumerate(PAIRS)])


def third_kernel(grid, parts_ref, last_ref, center_ref, initial_ref, later_ref, value_ref, images_ref, sums_ref):
    _, _, x, own = grid
    rows, wide = last_ref.shape[1:]
    keep = keeper(INNER, x, own)
    row = gathered_products(parts_ref)
    coefs = coefficients([entry(row, k) for k in range(len(PAIRS))])
    value = combined(coefs, [last_ref[k] for k in range(3)])
    value_ref[...] = middle(value, x, own)
    center = center_ref[...]
    firsts = basis(density_rhs(initial_ref[...], drift(value), keep), center, keep)
    mine = [middle(v, x, own) for v in firsts]
    values = [(6 * 8 + k, dot(mine[i], mine[j])) for k, (i, j) in enumerate(PAIRS)]
    speeds = drift(later_ref[...])
    images = []
    for v in firsts[:3]:
        chain = basis(density_rhs(v, speeds, keep), center, keep)
        images.append([middle(w, x, own) for w in chain])
    for i in range(3):
        for k in range(3):
            images_ref[3 * i + k] = images[i][k]
    for place, (a, b) in enumerate(MIXED):
        for k, (i, j) in enumerate(PAIRS):
            values.append((8 * place + k, dot(images[a][i], images[b][j])))
    sums_ref[...] = row_of(values)


def fourth_kernel(parts_ref, images_ref, value_ref, value_out, density_ref):
    x = value_out.shape[0]
    mine = pl.ds(pl.multiple_of(lax.axis_index(PART) * x, x), x)
    value_out[...] = value_ref[mine, :]
    row = gathered_products(parts_ref)
    first = coefficients([entry(row, 6 * 8 + k) for k in range(len(PAIRS))])
    products = []
    for k in range(len(PAIRS)):
        total = None
        for place, (a, b) in enumerate(MIXED):
            term = first[a] * first[b] * entry(row, 8 * place + k)
            term = term if a == b else 2.0 * term
            total = term if total is None else total + term
        products.append(total)
    second = coefficients(products)
    total = None
    for i in range(3):
        for k in range(3):
            term = (first[i] * second[k]) * images_ref[3 * i + k, mine, :]
            total = term if total is None else total + term
    density_ref[...] = total


def everywhere(row):
    axes = (*BAND, *GY)
    size = lax.axis_size(axes)
    copies = jnp.broadcast_to(row, (size, 1, 128))
    return lax.all_to_all(copies, axes, split_axis=0, concat_axis=0, tiled=True).reshape(size, 128)


def swapped(far, near, axis):
    peers = lax.axis_size(axis)
    pairs = [(i, i + 1) for i in range(1, peers - 1, 2)]
    gathered = lax.all_gather(near, axis[-1], tiled=True)
    if axis == GY:
        far, gathered = lax.optimization_barrier((far, gathered))
    return lax.ppermute(far, axis, pairs + [(b, a) for a, b in pairs]), gathered


def call(kernel, out_shape, *args, results=pltpu.VMEM):
    vmem = pl.BlockSpec(memory_space=pltpu.VMEM)
    return pl.pallas_call(
        kernel,
        out_shape=[results(s, jnp.float32) for s in out_shape],
        in_specs=[vmem] * len(args),
        out_specs=[vmem] * len(out_shape),
        compiler_params=pltpu.CompilerParams(vmem_limit_bytes=VMEM_LIMIT),
    )(*[pltpu.with_memory_space_constraint(a, pltpu.VMEM) for a in args])


def shards(terminal, initial_density, density_guess, diagonal):
    x, own = terminal.shape
    band = x * lax.axis_size(PART)
    grid = (x * lax.axis_size(GX), own * lax.axis_size(GY), band, own)
    fields, far, near = pl.pallas_call(
        stack_kernel,
        out_shape=[pltpu.VMEM(s, jnp.float32) for s in [(FIELDS, x, own), (x, EDGE), (x, EDGE)]],
        in_specs=[pl.BlockSpec(memory_space=pltpu.HBM)] * 4,
        out_specs=[pl.BlockSpec(memory_space=pltpu.VMEM)] * 3,
        scratch_shapes=[pltpu.SemaphoreType.DMA((4,))],
    )(terminal, diagonal, density_guess, initial_density)
    (block,) = call(edge_kernel, [(x * FIELDS + 8, own)], fields, *swapped(far, near, GY))
    whole = lax.all_gather(block, PART)
    packed = (8 * SENT, own)
    far, near = call(row_kernel, [packed, packed], whole)
    rows = band + 2 * HALO
    wide = own + EDGE
    full, fewer = (rows, wide), (band + 2 * INNER, wide)
    basis1, center, guess, initial, sums = call(
        functools.partial(first_kernel, grid),
        [(3, *full), full, full, fewer, (1, 128)],
        whole, *swapped(far, near, BAND),
    )
    later, basis0, center, sums = call(
        functools.partial(second_kernel, grid),
        [fewer, (3, *fewer), fewer, (1, 128)],
        everywhere(sums), basis1, center, guess,
    )
    value, images, sums = call(
        functools.partial(third_kernel, grid),
        [(band, own), (9, band, own), (1, 128)],
        everywhere(sums), basis0, center, initial, later,
    )
    return tuple(
        call(
            fourth_kernel, [(x, own)] * 2, everywhere(sums), images, value,
            results=jax.ShapeDtypeStruct,
        )
    )


def solution(mesh):
    torus = Mesh(mesh.devices.reshape(4, 2, 4, 8, 2), GX + GY)
    in_specs = (P(GX, GY), P(GX, GY), P(None, GX, GY), P(GX, GY))
    out_specs = (P(GX, GY), P(GX, GY))
    return jax.shard_map(
        shards, mesh=torus, in_specs=in_specs, out_specs=out_specs, check_vma=False
    )
```

```python
import functools

import jax
import jax.numpy as jnp
from jax import lax
from jax.experimental import pallas as pl
from jax.experimental.pallas import tpu as pltpu
from jax.sharding import Mesh
from jax.sharding import PartitionSpec as P

BAND = ("band_0", "band_1")
PART = "part"
GX = (*BAND, PART)
GY = ("gy_0", "gy_1")

inv_step = 0.5
coupling = 0.5

LOW = 0.6
HIGH = 10.5
S1 = 2.0
S2 = 6.0
S3 = 4.0
PAIRS = ((0, 0), (0, 1), (1, 1), (1, 2), (2, 2), (2, 3))
MIXED = ((0, 0), (1, 1), (2, 2), (0, 1), (0, 2), (1, 2))

HALF = 64
EDGE = 128
TERMINAL, DIAGONAL, GUESS, INITIAL = 0, 1, 2, 4
FIELDS = 5
SENT = FIELDS + 3
VMEM_LIMIT = 24 * 2**20
STRIP = 16
HALO = 16
INNER = 8


def before(v, dim):
    return pltpu.roll(v, 1, dim)


def after(v, dim):
    return pltpu.roll(v, v.shape[dim] - 1, dim)


def keeper(halo, x, own):
    band, column = lax.axis_index(BAND), lax.axis_index(GY)
    bands, columns = lax.axis_size(BAND), lax.axis_size(GY)
    top = jnp.where(band > 0, 1.0, 0.0)
    bottom = jnp.where(band < bands - 1, 1.0, 0.0)
    lane = lax.broadcasted_iota(jnp.int32, (8, EDGE), 1)
    edge = jnp.where(
        lane < HALF, jnp.where(column < columns - 1, 1.0, 0.0), jnp.where(column > 0, 1.0, 0.0)
    )

    def tiled(rows):
        return jnp.concatenate([edge] * (rows // 8), axis=0)

    ends = tiled(halo)

    def keep(v):
        first, last = v[:halo], v[halo + x :]
        inner_rows = v[halo : halo + x]
        main = [first[:, :own] * top, inner_rows[:, :own], last[:, :own] * bottom]
        side = [
            first[:, own:] * (ends * top),
            inner_rows[:, own:] * tiled(x),
            last[:, own:] * (ends * bottom),
        ]
        return jnp.concatenate([jnp.concatenate(p, axis=0) for p in (main, side)], axis=1)

    return keep


def shifted(v, center, shift, keep):
    beside = (before(v, 0) + after(v, 0)) + (before(v, 1) + after(v, 1))
    return keep((center - shift) * v - beside)


def basis(v0, center, keep):
    v1 = shifted(v0, center, S1, keep)
    v2 = shifted(v1, center, S2, keep)
    return [v0, v1, v2, shifted(v2, center, S3, keep)]


def hamiltonian(u):
    total = None
    for dim in (0, 1):
        ahead = after(u, dim) - u
        term = before(jnp.maximum(ahead, 0.0) ** 2, dim) + jnp.minimum(ahead, 0.0) ** 2
        total = term if total is None else total + term
    return 0.5 * total


def drift(u):
    speed_x = u - after(u, 0)
    speed_y = u - after(u, 1)
    return (
        jnp.maximum(speed_x, 0.0),
        jnp.minimum(speed_x, 0.0),
        jnp.maximum(speed_y, 0.0),
        jnp.minimum(speed_y, 0.0),
    )


def density_rhs(m, speeds, keep):
    out_x, in_x, out_y, in_y = speeds
    flux_x = out_x * m + in_x * after(m, 0)
    flux_y = out_y * m + in_y * after(m, 1)
    div = (flux_x - before(flux_x, 0)) + (flux_y - before(flux_y, 1))
    return keep(inv_step * m - div)


def dot(a, b):
    rows, wide = a.shape
    total = jnp.sum((a * b).reshape(rows // 8, 8, wide), axis=0)
    total = sum(total[:, k : k + 128] for k in range(128, wide, 128)) + total[:, :128]
    return jnp.sum(total, axis=1, keepdims=True)


def row_of(values):
    lane = lax.broadcasted_iota(jnp.int32, (8, 128), 1)
    rows = jnp.zeros((8, 128), jnp.float32)
    for place, value in values:
        rows = jnp.where(lane == place, value, rows)
    return jnp.sum(rows, axis=0, keepdims=True)


def entry(row, place):
    lane = lax.broadcasted_iota(jnp.int32, row.shape, 1)
    return jnp.sum(jnp.where(lane == place, row, 0.0), axis=1, keepdims=True)


def form(matrix, vector):
    total = None
    for i, a in enumerate(vector):
        for j, b in enumerate(vector[: i + 1]):
            term = a * b * matrix[j][i]
            term = term if i == j else 2.0 * term
            total = term if total is None else total + term
    return total


def alpha_of(squared, energy):
    return jnp.clip(squared / jnp.maximum(energy, 1e-36), 0.999 / HIGH, 1.001 / LOW)


def beta_of(new, old):
    return jnp.clip(new / jnp.maximum(old, 1e-36), 0.0, 1.001 * HIGH / LOW)


def coefficients(products):
    g = dict(zip(PAIRS, products))
    g[0, 2] = g[1, 1] + (S1 - S2) * g[0, 1]
    gram = [[g[0, 0], g[0, 1], g[0, 2]], [None, g[1, 1], g[1, 2]], [None, None, g[2, 2]]]
    energy = [
        [g[0, 1] + S1 * g[0, 0], g[1, 1] + S1 * g[0, 1], g[1, 2] + S1 * g[0, 2]],
        [None, g[1, 2] + S2 * g[1, 1], g[2, 2] + S2 * g[1, 2]],
        [None, None, g[2, 3] + S3 * g[2, 2]],
    ]
    norm0 = g[0, 0]
    alpha0 = alpha_of(norm0, energy[0][0])
    resid1 = (1.0 - alpha0 * S1, -alpha0)
    norm1 = jnp.maximum(form(gram, resid1), 0.0)
    beta0 = beta_of(norm1, norm0)
    direct1 = (resid1[0] + beta0, resid1[1])
    alpha1 = alpha_of(norm1, form(energy, direct1))
    resid2 = (
        resid1[0] - alpha1 * (S1 * direct1[0]),
        resid1[1] - alpha1 * (direct1[0] + S2 * direct1[1]),
        -alpha1 * direct1[1],
    )
    norm2 = jnp.maximum(form(gram, resid2), 0.0)
    beta1 = beta_of(norm2, norm1)
    direct2 = (resid2[0] + beta1 * direct1[0], resid2[1] + beta1 * direct1[1], resid2[2])
    alpha2 = alpha_of(norm2, form(energy, direct2))
    return (
        alpha0 + alpha1 * direct1[0] + alpha2 * direct2[0],
        alpha1 * direct1[1] + alpha2 * direct2[1],
        alpha2 * direct2[2],
    )


def combined(coefs, vectors):
    total = coefs[0] * vectors[0]
    for c, v in zip(coefs[1:], vectors[1:]):
        total = total + c * v
    return total


def middle(v, x, own):
    return v[(v.shape[0] - x) // 2 : (v.shape[0] + x) // 2, :own]


def inner(v):
    return v[HALO - INNER : v.shape[0] - (HALO - INNER)]


def gathered_products(parts_ref):
    return jnp.sum(parts_ref[...], axis=0, keepdims=True)


def odd_index(axis, shape):
    place = lax.rem(lax.axis_index(axis), 2)
    return (lax.broadcasted_iota(jnp.int32, shape, 0) * 0 + place) == 1


def stack_kernel(terminal, diagonal, guess, initial, fields_ref, far_edge, near_edge, sems):
    copies = [
        pltpu.make_async_copy(terminal, fields_ref.at[TERMINAL], sems.at[0]),
        pltpu.make_async_copy(diagonal, fields_ref.at[DIAGONAL], sems.at[1]),
        pltpu.make_async_copy(guess, fields_ref.at[pl.ds(GUESS, 2)], sems.at[2]),
        pltpu.make_async_copy(initial, fields_ref.at[INITIAL], sems.at[3]),
    ]
    for copy in copies:
        copy.start()
    for copy in copies:
        copy.wait()
    _, x, own = fields_ref.shape
    shape = (x, 128)
    strip = lax.broadcasted_iota(jnp.int32, shape, 1) // STRIP
    firsts = lasts = jnp.zeros(shape, jnp.float32)
    for k in range(FIELDS):
        first, last = fields_ref[k, :, :128], fields_ref[k, :, own - 128 :]
        firsts = jnp.where(strip == k, pltpu.roll(first, STRIP * k, 1) if k else first, firsts)
        lasts = jnp.where(strip == k, pltpu.roll(last, STRIP * (k + 1), 1), lasts)
    odd = odd_index(GY, shape)
    far_edge[...] = jnp.where(odd, lasts, firsts)
    near_edge[...] = jnp.where(odd, firsts, lasts)


def edge_kernel(fields_ref, far_edge, near_edge, block_ref):
    _, x, own = fields_ref.shape
    odd = odd_index(GY, (x, EDGE))
    left = jnp.where(odd, near_edge[:x, :], far_edge[...])
    right = jnp.where(odd, far_edge[...], near_edge[x:, :])
    for k in range(FIELDS):
        block_ref[x * k : x * (k + 1), :] = fields_ref[k]
    edges = [right[:8], left[:8], right[8:], left[8:]]
    block_ref[x * FIELDS :, :] = jnp.concatenate(edges, axis=1)


def row_kernel(band_ref, far_ref, near_ref):
    parts, _, own = band_ref.shape
    shape = (8, own)
    row = lax.broadcasted_iota(jnp.int32, shape, 0)

    def halves(part):
        tiles = [band_ref[part, 8 * k : 8 * k + 8, :] for k in range(2 * FIELDS + 1)]
        return tiles[: 2 * FIELDS : 2], tiles[1 : 2 * FIELDS : 2], tiles[2 * FIELDS]

    first, second, edge = halves(0)
    top = first + [
        jnp.where(row < 5, second[TERMINAL], pltpu.roll(second[DIAGONAL], 5, 0)),
        jnp.where(row < 4, second[GUESS + 1], pltpu.roll(second[GUESS], 4, 0)),
        edge,
    ]
    first, second, edge = halves(parts - 1)
    bottom = second + [
        jnp.where(row >= 3, first[TERMINAL], pltpu.roll(first[DIAGONAL], 3, 0)),
        jnp.where(row >= 4, first[GUESS + 1], pltpu.roll(first[GUESS], 4, 0)),
        edge,
    ]
    odd = odd_index(BAND, shape)
    for k, (t, b) in enumerate(zip(top, bottom)):
        far_ref[8 * k : 8 * k + 8, :] = jnp.where(odd, b, t)
        near_ref[8 * k : 8 * k + 8, :] = jnp.where(odd, t, b)


def first_kernel(grid, band_ref, far_ref, near_ref, basis_ref, center_ref, guess_ref, initial_ref, sums_ref):
    _, _, x, own = grid
    wide = own + EDGE
    rows = x + 2 * HALO
    parts = band_ref.shape[0]
    keep = keeper(HALO, x, own)
    odd = odd_index(BAND, (8, own))

    def tile(k, odd_from, odd_start, even_from, even_start):
        odd_tile = odd_from[8 * (odd_start + k) : 8 * (odd_start + k) + 8, :]
        return jnp.where(odd, odd_tile, even_from[8 * (even_start + k) : 8 * (even_start + k) + 8, :])

    above = [tile(k, near_ref, 0, far_ref, 0) for k in range(SENT)]
    below = [tile(k, far_ref, 0, near_ref, SENT) for k in range(SENT)]
    rest_above = {
        TERMINAL: above[FIELDS],
        DIAGONAL: pltpu.roll(above[FIELDS], 5, 0),
        GUESS + 1: above[FIELDS + 1],
        GUESS: pltpu.roll(above[FIELDS + 1], 4, 0),
    }
    rest_below = {
        TERMINAL: below[FIELDS],
        DIAGONAL: pltpu.roll(below[FIELDS], 3, 0),
        GUESS + 1: below[FIELDS + 1],
        GUESS: pltpu.roll(below[FIELDS + 1], 4, 0),
    }
    nothing = jnp.zeros((8, own), jnp.float32)
    blocks = [above[-1], *[band_ref[part, 2 * 8 * FIELDS :, :] for part in range(parts)], below[-1]]
    right, left = (
        jnp.concatenate([b[:, at : at + 128] for b in blocks for at in (start, start + 256)], axis=0)
        for start in (0, 128)
    )
    half = lax.broadcasted_iota(jnp.int32, (rows, EDGE), 1) < HALF

    def extended(k):
        whole = jnp.concatenate(
            [
                rest_above.get(k, nothing),
                above[k],
                *[band_ref[part, 16 * k : 16 * k + 16, :] for part in range(parts)],
                below[k],
                rest_below.get(k, nothing),
            ],
            axis=0,
        )
        from_right = pltpu.roll(right, 128 - STRIP * k, 1) if k else right
        from_left = pltpu.roll(left, 128 - STRIP * (k + 1), 1)
        return jnp.concatenate([whole, jnp.where(half, from_right, from_left)], axis=1)

    later = extended(TERMINAL)
    center = extended(DIAGONAL) + (inv_step + 4.0)
    rhs = inv_step * later - hamiltonian(later) + coupling * extended(GUESS + 1)
    vs = basis(keep(rhs), center, keep)
    for k in range(3):
        basis_ref[k] = vs[k]
    center_ref[...] = center
    guess_ref[...] = extended(GUESS)
    initial_ref[...] = inner(extended(INITIAL))
    mine = [middle(v, x, own) for v in vs]
    sums_ref[...] = row_of([(k, dot(mine[i], mine[j])) for k, (i, j) in enumerate(PAIRS)])


def second_kernel(grid, parts_ref, last_ref, center_ref, guess_ref, later_ref, basis_ref, inner_center, sums_ref):
    _, _, x, own = grid
    rows, wide = last_ref.shape[1:]
    keep = keeper(HALO, x, own)
    row = gathered_products(parts_ref)
    coefs = coefficients([entry(row, k) for k in range(len(PAIRS))])
    later = combined(coefs, [last_ref[k] for k in range(3)])
    later_ref[...] = inner(later)
    center = center_ref[...]
    inner_center[...] = inner(center)
    rhs = inv_step * later - hamiltonian(later) + coupling * guess_ref[...]
    vs = basis(keep(rhs), center, keep)
    for k in range(3):
        basis_ref[k] = inner(vs[k])
    mine = [middle(v, x, own) for v in vs]
    sums_ref[...] = row_of([(k, dot(mine[i], mine[j])) for k, (i, j) in enumerate(PAIRS)])


def third_kernel(grid, parts_ref, last_ref, center_ref, initial_ref, later_ref, value_ref, images_ref, sums_ref):
    _, _, x, own = grid
    rows, wide = last_ref.shape[1:]
    keep = keeper(INNER, x, own)
    row = gathered_products(parts_ref)
    coefs = coefficients([entry(row, k) for k in range(len(PAIRS))])
    value = combined(coefs, [last_ref[k] for k in range(3)])
    value_ref[...] = middle(value, x, own)
    center = center_ref[...]
    firsts = basis(density_rhs(initial_ref[...], drift(value), keep), center, keep)
    mine = [middle(v, x, own) for v in firsts]
    values = [(6 * 8 + k, dot(mine[i], mine[j])) for k, (i, j) in enumerate(PAIRS)]
    speeds = drift(later_ref[...])
    images = []
    for v in firsts[:3]:
        chain = basis(density_rhs(v, speeds, keep), center, keep)
        images.append([middle(w, x, own) for w in chain])
    for i in range(3):
        for k in range(3):
            images_ref[3 * i + k] = images[i][k]
    for place, (a, b) in enumerate(MIXED):
        for k, (i, j) in enumerate(PAIRS):
            values.append((8 * place + k, dot(images[a][i], images[b][j])))
    sums_ref[...] = row_of(values)


def fourth_kernel(parts_ref, images_ref, value_ref, value_out, density_ref):
    x = value_out.shape[0]
    mine = pl.ds(pl.multiple_of(lax.axis_index(PART) * x, x), x)
    value_out[...] = value_ref[mine, :]
    row = gathered_products(parts_ref)
    first = coefficients([entry(row, 6 * 8 + k) for k in range(len(PAIRS))])
    products = []
    for k in range(len(PAIRS)):
        total = None
        for place, (a, b) in enumerate(MIXED):
            term = first[a] * first[b] * entry(row, 8 * place + k)
            term = term if a == b else 2.0 * term
            total = term if total is None else total + term
        products.append(total)
    second = coefficients(products)
    total = None
    for i in range(3):
        for k in range(3):
            term = (first[i] * second[k]) * images_ref[3 * i + k, mine, :]
            total = term if total is None else total + term
    density_ref[...] = total


def everywhere(row):
    axes = (*BAND, *GY)
    size = lax.axis_size(axes)
    copies = jnp.broadcast_to(row, (size, 1, 128))
    return lax.all_to_all(copies, axes, split_axis=0, concat_axis=0, tiled=True).reshape(size, 128)


def swapped(far, near, axis):
    peers = lax.axis_size(axis)
    pairs = [(i, i + 1) for i in range(1, peers - 1, 2)]
    return (
        lax.ppermute(far, axis, pairs + [(b, a) for a, b in pairs]),
        lax.all_gather(near, axis[-1], tiled=True),
    )


def call(kernel, out_shape, *args, results=pltpu.VMEM):
    vmem = pl.BlockSpec(memory_space=pltpu.VMEM)
    return pl.pallas_call(
        kernel,
        out_shape=[results(s, jnp.float32) for s in out_shape],
        in_specs=[vmem] * len(args),
        out_specs=[vmem] * len(out_shape),
        compiler_params=pltpu.CompilerParams(vmem_limit_bytes=VMEM_LIMIT),
    )(*[pltpu.with_memory_space_constraint(a, pltpu.VMEM) for a in args])


def shards(terminal, initial_density, density_guess, diagonal):
    x, own = terminal.shape
    band = x * lax.axis_size(PART)
    grid = (x * lax.axis_size(GX), own * lax.axis_size(GY), band, own)
    fields, far, near = pl.pallas_call(
        stack_kernel,
        out_shape=[pltpu.VMEM(s, jnp.float32) for s in [(FIELDS, x, own), (x, EDGE), (x, EDGE)]],
        in_specs=[pl.BlockSpec(memory_space=pltpu.HBM)] * 4,
        out_specs=[pl.BlockSpec(memory_space=pltpu.VMEM)] * 3,
        scratch_shapes=[pltpu.SemaphoreType.DMA((4,))],
    )(terminal, diagonal, density_guess, initial_density)
    (block,) = call(edge_kernel, [(x * FIELDS + 8, own)], fields, *swapped(far, near, GY))
    whole = lax.all_gather(block, PART)
    packed = (8 * SENT, own)
    far, near = call(row_kernel, [packed, packed], whole)
    rows = band + 2 * HALO
    wide = own + EDGE
    full, fewer = (rows, wide), (band + 2 * INNER, wide)
    basis1, center, guess, initial, sums = call(
        functools.partial(first_kernel, grid),
        [(3, *full), full, full, fewer, (1, 128)],
        whole, *swapped(far, near, BAND),
    )
    later, basis0, center, sums = call(
        functools.partial(second_kernel, grid),
        [fewer, (3, *fewer), fewer, (1, 128)],
        everywhere(sums), basis1, center, guess,
    )
    value, images, sums = call(
        functools.partial(third_kernel, grid),
        [(band, own), (9, band, own), (1, 128)],
        everywhere(sums), basis0, center, initial, later,
    )
    return tuple(
        call(
            fourth_kernel, [(x, own)] * 2, everywhere(sums), images, value,
            results=jax.ShapeDtypeStruct,
        )
    )


def solution(mesh):
    torus = Mesh(mesh.devices.reshape(4, 2, 4, 8, 2), GX + GY)
    in_specs = (P(GX, GY), P(GX, GY), P(None, GX, GY), P(GX, GY))
    out_specs = (P(GX, GY), P(GX, GY))
    return jax.shard_map(
        shards, mesh=torus, in_specs=in_specs, out_specs=out_specs, check_vma=False
    )
```
